8 devices in a mesh: dp: 1 (over z), y: 2 (over y), x: 4 (over x, core).
Axes of the slice: x: 2, y: 2, z: 1, core: 2. Of those that a mesh axis runs over, the one named last changes fastest.
Arguments:
- hidden: bfloat16 [256, 2560], P('dp', 'x')
- positions: int32 [256], P('dp')
- k_cache: bfloat16 [2, 256, 256, 8, 128], P(None, ('dp', 'x'), None, 'y')
- v_cache: bfloat16 [2, 256, 256, 8, 128], P(None, ('dp', 'x'), None, 'y')
- g_attn: bfloat16 [2, 2560], P(None, 'x')
- g_mlp: bfloat16 [2, 2560], P(None, 'x')
- q_gain: bfloat16 [2, 128], replicated
- k_gain: bfloat16 [2, 128], replicated
- w_q: bfloat16 [2, 2560, 4096], P(None, 'x', 'y')
- w_k: bfloat16 [2, 2560, 1024], P(None, 'x', 'y')
- w_v: bfloat16 [2, 2560, 1024], P(None, 'x', 'y')
- w_o: bfloat16 [2, 4096, 2560], P(None, 'y', 'x')
- w_gate: bfloat16 [2, 2560, 9728], P(None, 'x', 'y')
- w_up: bfloat16 [2, 2560, 9728], P(None, 'x', 'y')
- w_down: bfloat16 [2, 9728, 2560], P(None, 'y', 'x')
Outputs:
- output 1: bfloat16 [256, 2560], P('dp', 'x')
- output 2: bfloat16 [2, 256, 256, 8, 128], P(None, ('dp', 'x'), None, 'y')
- output 3: bfloat16 [2, 256, 256, 8, 128], P(None, ('dp', 'x'), None, 'y')
All inputs are finite; a program needn't handle non-finite values.
Results may differ from the reference program's by a relative error of at most 0.02.
Values are sent between devices in bfloat16 or wider.
A program may use at most 1 GiB of HBM per device.

```python
import jax
import jax.numpy as jnp
from jax import lax

LAYERS = 2
BATCH = 256
CACHE_LEN = 256
MODEL_DIM = 2560
Q_HEADS = 32
KV_HEADS = 8
FFN_DIM = 9728
HEAD_DIM = 128
NORM_EPS = 1e-6
ROPE_BASE = 1000000.0


def rms_scale(hidden, norm_gain):
    hidden_f32 = hidden.astype(jnp.float32)
    mean_sq = jnp.mean(hidden_f32 * hidden_f32, axis=-1, keepdims=True)
    return hidden_f32 * lax.rsqrt(mean_sq + NORM_EPS) * norm_gain.astype(jnp.float32)


def rope_tables(positions):
    half_dim = HEAD_DIM // 2
    inv_freq = jnp.power(ROPE_BASE, -2.0 * jnp.arange(half_dim, dtype=jnp.float32) / HEAD_DIM)
    angles = positions.astype(jnp.float32)[:, None] * inv_freq[None, :]
    return jnp.cos(angles), jnp.sin(angles)


def apply_rope(heads_f32, cos_tab, sin_tab):
    half_dim = HEAD_DIM // 2
    first_half = heads_f32[..., :half_dim]
    second_half = heads_f32[..., half_dim:]
    cos_b = cos_tab[:, None, :]
    sin_b = sin_tab[:, None, :]
    return jnp.concatenate([first_half * cos_b - second_half * sin_b, second_half * cos_b + first_half * sin_b], axis=-1)


def decoder_layer(hidden, positions, layer_params):
    k_cache, v_cache, g_attn, g_mlp, q_gain, k_gain, w_q, w_k, w_v, w_o, w_gate, w_up, w_down = layer_params
    batch_rows = hidden.shape[0]
    group_size = Q_HEADS // KV_HEADS
    normed = rms_scale(hidden, g_attn).astype(jnp.bfloat16)
    q_proj = jnp.dot(normed, w_q, preferred_element_type=jnp.float32).astype(jnp.bfloat16).reshape(batch_rows, Q_HEADS, HEAD_DIM)
    k_proj = jnp.dot(normed, w_k, preferred_element_type=jnp.float32).astype(jnp.bfloat16).reshape(batch_rows, KV_HEADS, HEAD_DIM)
    v_proj = jnp.dot(normed, w_v, preferred_element_type=jnp.float32).astype(jnp.bfloat16).reshape(batch_rows, KV_HEADS, HEAD_DIM)
    cos_tab, sin_tab = rope_tables(positions)
    q_rot = apply_rope(rms_scale(q_proj, q_gain), cos_tab, sin_tab).astype(jnp.bfloat16)
    k_rot = apply_rope(rms_scale(k_proj, k_gain), cos_tab, sin_tab).astype(jnp.bfloat16)
    slot_ids = jnp.arange(CACHE_LEN, dtype=jnp.int32)[None, :]
    slot_hit = (slot_ids == positions[:, None])[:, :, None, None]
    k_new = jnp.where(slot_hit, k_rot[:, None], k_cache)
    v_new = jnp.where(slot_hit, v_proj[:, None], v_cache)
    q_grouped = q_rot.reshape(batch_rows, KV_HEADS, group_size, HEAD_DIM)
    scores = jnp.einsum('bkge,blke->bkgl', q_grouped.astype(jnp.float32), k_new.astype(jnp.float32)) * (HEAD_DIM ** -0.5)
    valid_slot = (slot_ids <= positions[:, None])[:, None, None, :]
    scores = jnp.where(valid_slot, scores, -1e30)
    att_probs = jax.nn.softmax(scores, axis=-1).astype(jnp.bfloat16)
    attn_heads = jnp.einsum('bkgl,blke->bkge', att_probs.astype(jnp.float32), v_new.astype(jnp.float32)).astype(jnp.bfloat16)
    attn_out = jnp.dot(attn_heads.reshape(batch_rows, Q_HEADS * HEAD_DIM), w_o, preferred_element_type=jnp.float32).astype(jnp.bfloat16)
    mid_hidden = (hidden.astype(jnp.float32) + attn_out.astype(jnp.float32)).astype(jnp.bfloat16)
    normed_mlp = rms_scale(mid_hidden, g_mlp).astype(jnp.bfloat16)
    gate_val = jnp.dot(normed_mlp, w_gate, preferred_element_type=jnp.float32).astype(jnp.bfloat16)
    up_val = jnp.dot(normed_mlp, w_up, preferred_element_type=jnp.float32).astype(jnp.bfloat16)
    act_val = (jax.nn.silu(gate_val.astype(jnp.float32)) * up_val.astype(jnp.float32)).astype(jnp.bfloat16)
    mlp_out = jnp.dot(act_val, w_down, preferred_element_type=jnp.float32).astype(jnp.bfloat16)
    new_hidden = (mid_hidden.astype(jnp.float32) + mlp_out.astype(jnp.float32)).astype(jnp.bfloat16)
    return new_hidden, k_new, v_new


def setup_inputs(seed: int = 0, part: int = 0) -> dict:
    part_keys = jax.random.split(jax.random.fold_in(jax.random.key(seed), part), 5)
    weight_keys = jax.random.split(jax.random.key(seed + 7919), 11)
    q_width = Q_HEADS * HEAD_DIM
    kv_width = KV_HEADS * HEAD_DIM
    cache_shape = (LAYERS, BATCH, CACHE_LEN, KV_HEADS, HEAD_DIM)
    row_scale = jnp.exp(0.4 * jax.random.normal(part_keys[0], (BATCH, 1), jnp.float32))
    hidden = (jax.random.normal(part_keys[1], (BATCH, MODEL_DIM), jnp.float32) * row_scale).astype(jnp.bfloat16)
    raw_pos = jax.random.randint(part_keys[2], (BATCH,), 0, CACHE_LEN, jnp.int32)
    row_ids = jnp.arange(BATCH, dtype=jnp.int32)
    positions = jnp.where(row_ids == 0, CACHE_LEN - 1, jnp.where(row_ids == 1, 0, raw_pos)).astype(jnp.int32)
    k_cache = jax.random.normal(part_keys[3], cache_shape, jnp.float32).astype(jnp.bfloat16)
    v_cache = jax.random.normal(part_keys[4], cache_shape, jnp.float32).astype(jnp.bfloat16)
    g_attn = (1.0 + 0.25 * jax.random.normal(weight_keys[0], (LAYERS, MODEL_DIM), jnp.float32)).astype(jnp.bfloat16)
    g_mlp = (1.0 + 0.25 * jax.random.normal(weight_keys[1], (LAYERS, MODEL_DIM), jnp.float32)).astype(jnp.bfloat16)
    q_gain = (1.6 + 0.3 * jax.random.normal(weight_keys[2], (LAYERS, HEAD_DIM), jnp.float32)).astype(jnp.bfloat16)
    k_gain = (4.0 * jax.random.normal(weight_keys[3], (LAYERS, HEAD_DIM), jnp.float32)).astype(jnp.bfloat16)
    w_q = (jax.random.normal(weight_keys[4], (LAYERS, MODEL_DIM, q_width), jnp.float32) * MODEL_DIM ** -0.5).astype(jnp.bfloat16)
    w_k = (jax.random.normal(weight_keys[5], (LAYERS, MODEL_DIM, kv_width), jnp.float32) * MODEL_DIM ** -0.5).astype(jnp.bfloat16)
    w_v = (jax.random.normal(weight_keys[6], (LAYERS, MODEL_DIM, kv_width), jnp.float32) * MODEL_DIM ** -0.5).astype(jnp.bfloat16)
    w_o = (jax.random.normal(weight_keys[7], (LAYERS, q_width, MODEL_DIM), jnp.float32) * q_width ** -0.5).astype(jnp.bfloat16)
    w_gate = (jax.random.normal(weight_keys[8], (LAYERS, MODEL_DIM, FFN_DIM), jnp.float32) * MODEL_DIM ** -0.5).astype(jnp.bfloat16)
    w_up = (jax.random.normal(weight_keys[9], (LAYERS, MODEL_DIM, FFN_DIM), jnp.float32) * MODEL_DIM ** -0.5).astype(jnp.bfloat16)
    w_down = (jax.random.normal(weight_keys[10], (LAYERS, FFN_DIM, MODEL_DIM), jnp.float32) * FFN_DIM ** -0.5).astype(jnp.bfloat16)
    return {'hidden': hidden, 'positions': positions, 'k_cache': k_cache, 'v_cache': v_cache, 'g_attn': g_attn, 'g_mlp': g_mlp, 'q_gain': q_gain, 'k_gain': k_gain, 'w_q': w_q, 'w_k': w_k, 'w_v': w_v, 'w_o': w_o, 'w_gate': w_gate, 'w_up': w_up, 'w_down': w_down}


def reference(hidden, positions, k_cache, v_cache, g_attn, g_mlp, q_gain, k_gain, w_q, w_k, w_v, w_o, w_gate, w_up, w_down):
    def layer_step(carry_hidden, layer_params):
        new_hidden, k_new, v_new = decoder_layer(carry_hidden, positions, layer_params)
        return new_hidden, (k_new, v_new)
    out_hidden, cache_pair = lax.scan(layer_step, hidden, (k_cache, v_cache, g_attn, g_mlp, q_gain, k_gain, w_q, w_k, w_v, w_o, w_gate, w_up, w_down))
    return out_hidden, cache_pair[0], cache_pair[1]
```

```python
import functools

import jax
import jax.numpy as jnp
from jax import lax
from jax.experimental import pallas as pl
from jax.experimental.pallas import tpu as pltpu
from jax.sharding import PartitionSpec as P

HEAD_DIM = 128
NORM_EPS = 1e-6
ROPE_BASE = 1000000.0
MESH = pl.DeviceIdType.MESH
BF16 = jnp.bfloat16
F32 = jnp.float32

NM = 1
CW = 256
IW = 2 * CW
O2, O3, O4, O5 = 1, 3, 5, 6
SB = 8
MASK = (0, 2, 1, 3)
POS = (0, 2, 1, 3)


def dot(a, b):
    return jnp.dot(a, b, preferred_element_type=F32)


def chain_kernel(head, tail, layer, model_dim, *refs):
    it = iter(refs)
    hid_in = next(it)
    if head:
        attn_in, g_mlp = next(it), next(it)
        wo_in, wg_in, wu_in, wd_in = (next(it).at[layer] for _ in range(4))
    if tail:
        tail_layer = layer + 1 if head else layer
        g_attn = next(it)
        wq_in, wk_in, wv_in = (next(it).at[tail_layer] for _ in range(3))
    if head:
        hid_out = next(it)
    if tail:
        qkv_out = next(it)
    h_buf, n_buf, stat_buf, keep_buf, own_buf, dsend, drecv, xsend, xrecv = (next(it) for _ in range(9))
    h_sem, st_ss, st_rs, d_ss, d_rs, x_ss, x_rs = (next(it) for _ in range(7))
    if head:
        attn_all, wo_buf, wgu_buf, wd_buf, acc_buf, act_all, y_send, y_recv = (next(it) for _ in range(8))
        ag_ss, ag_rs, y_ss, y_rs, act_ss, act_rs, wo_sem, wgu_sem, wd_sem, o_sem = (next(it) for _ in range(10))
    if tail:
        wqkv_buf, wqkv_sem = (next(it) for _ in range(2))

    me = lax.axis_index('x')
    yy = lax.axis_index('y')
    chip, core = lax.div(me, 2), lax.rem(me, 2)
    d1 = chip * 2 + (1 - core)
    d2 = (1 - chip) * 2 + core
    d3 = (1 - chip) * 2 + (1 - core)
    quarter = (me, d2, d1, d3)
    R = h_buf.shape[1] // 4
    M = 4 * R
    n_ffn = act_all.shape[0] // NM if head else 0
    n_mlp = n_ffn * NM
    n_qkv = 6

    barrier = pltpu.get_barrier_semaphore()
    for peer in ({'x': d1}, {'x': d2}, {'x': d3}, {'y': 1 - yy}):
        pl.semaphore_signal(barrier, inc=1, device_id=peer, device_id_type=MESH)

    def remote(src, dst, ss, rs, peer):
        return pltpu.make_async_remote_copy(src_ref=src, dst_ref=dst, send_sem=ss, recv_sem=rs, device_id=peer, device_id_type=MESH)

    def hid_copy(m, k):
        row = pl.multiple_of(quarter[k] * (NM * R) + m * R, R)
        return pltpu.make_async_copy(hid_in.at[pl.ds(row, R)], h_buf.at[m, pl.ds(k * R, R)], h_sem.at[m, k])

    for m in range(NM):
        for k in range(4):
            hid_copy(m, k).start()

    def wgu_copy(j):
        off = pl.multiple_of(j * CW, CW)
        return (pltpu.make_async_copy(wg_in.at[:, pl.ds(off, CW)], wgu_buf.at[j, :, pl.ds(0, CW)], wgu_sem.at[0, j]),
                pltpu.make_async_copy(wu_in.at[:, pl.ds(off, CW)], wgu_buf.at[j, :, pl.ds(CW, CW)], wgu_sem.at[1, j]))

    if head:
        wo_copy = pltpu.make_async_copy(wo_in, wo_buf, wo_sem)
        wd_copy = pltpu.make_async_copy(wd_in, wd_buf, wd_sem)
    if tail:
        wqkv_copies = [pltpu.make_async_copy(wq_in.at[:, pl.ds(j * IW, IW)], wqkv_buf.at[j], wqkv_sem.at[j]) for j in range(4)]
        wqkv_copies += [pltpu.make_async_copy(w, wqkv_buf.at[j], wqkv_sem.at[j]) for j, w in ((4, wk_in), (5, wv_in))]
    if head:
        wo_copy.start()

        def start_wgu(j, c):
            for cp in wgu_copy(j):
                cp.start()
            return c
        lax.fori_loop(0, n_ffn, start_wgu, 0)
        wd_copy.start()
    if tail:
        for cp in wqkv_copies:
            cp.start()

    def diag():
        return lax.broadcasted_iota(jnp.int32, (R, 128), 0) == lax.broadcasted_iota(jnp.int32, (R, 128), 1)

    def stat_send(kind, m, a):
        peer = (None, d1, d2, d3)[a]
        return remote(stat_buf.at[kind, m, 0], stat_buf.at[kind, m, a], st_ss.at[kind, m, a - 1], st_rs.at[kind, m, a - 1], {'x': peer})

    def stats_start(kind, m):
        for k in range(4):
            hv = h_buf[m, pl.ds(k * R, R), :].astype(F32)
            row_sum = jnp.sum(hv * hv, axis=1, keepdims=True)
            stat_buf[kind, m, 0, pl.ds(k, 1), :] = jnp.sum(jnp.where(diag(), row_sum, 0.0), axis=0, keepdims=True)
        for a in (1, 2, 3):
            stat_send(kind, m, a).start()

    def norm(kind, m, gain):
        for a in (1, 2, 3):
            stat_send(kind, m, a).wait()
        gain_row = gain.astype(F32)
        for k in range(4):
            total = stat_buf[kind, m, 0, pl.ds(k, 1), :]
            for a in (1, 2, 3):
                total = total + stat_buf[kind, m, a, pl.ds(POS[MASK[k] ^ a], 1), :]
            col = jnp.sum(jnp.where(diag(), total, 0.0), axis=1, keepdims=True)
            hv = h_buf[m, pl.ds(k * R, R), :].astype(F32)
            n_buf[m, pl.ds(k * R, R), :] = (hv * lax.rsqrt(col / model_dim + NORM_EPS) * gain_row).astype(BF16)

    def d_copy(s):
        return remote(dsend.at[s], drecv.at[s], d_ss.at[s], d_rs.at[s], {'x': d1})

    def x_copy(s):
        return remote(xsend.at[s], xrecv.at[s], x_ss.at[s], x_rs.at[s], {'x': d2})

    def stage1(s, m, w):
        part = dot(n_buf[m], w)
        keep_buf[lax.rem(s, keep_buf.shape[0])] = part[:2 * R]
        dsend[s] = part[2 * R:].astype(BF16)
        d_copy(s).start()

    def stage2(s):
        d_copy(s).wait_recv()
        slot = lax.rem(s, keep_buf.shape[0])
        xsend[s] = (keep_buf[slot, pl.ds(R, R), :] + drecv[s, pl.ds(R, R), :].astype(F32)).astype(BF16)
        x_copy(s).start()
        own_buf[lax.rem(s, own_buf.shape[0])] = keep_buf[slot, pl.ds(0, R), :] + drecv[s, pl.ds(0, R), :].astype(F32)

    def stage3(s):
        x_copy(s).wait_recv()
        return (own_buf[lax.rem(s, own_buf.shape[0])] + xrecv[s].astype(F32)).astype(BF16)

    def gather_copies(buf, i, ss, rs):
        own, other = buf.at[i, pl.ds(0, R)], buf.at[i, pl.ds(R, R)]
        return (lambda: remote(own, buf.at[i, pl.ds(2 * R, R)], ss.at[0, i], rs.at[0, i], {'x': d1}),
                lambda: remote(own, buf.at[i, pl.ds(R, R)], ss.at[1, i], rs.at[1, i], {'x': d2}),
                lambda: remote(other, buf.at[i, pl.ds(3 * R, R)], ss.at[2, i], rs.at[2, i], {'x': d1}))

    def attn_copies(m):
        return gather_copies(attn_all, m, ag_ss, ag_rs)

    def y_copy(kind, m):
        return remote(y_send.at[kind, m], y_recv.at[kind, m], y_ss.at[kind, m], y_rs.at[kind, m], {'y': 1 - yy})

    def y_start(kind, m, value):
        y_send[kind, m] = value.astype(BF16)
        y_copy(kind, m).start()

    def y_finish(kind, m):
        y_copy(kind, m).wait()
        total = (y_send[kind, m].astype(F32) + y_recv[kind, m].astype(F32)).astype(BF16)
        h_buf[m] = (h_buf[m].astype(F32) + total.astype(F32)).astype(BF16)

    def act_copies(t):
        return gather_copies(act_all, t, act_ss, act_rs)

    def out_copy(m, k):
        row = pl.multiple_of(quarter[k] * (NM * R) + m * R, R)
        return pltpu.make_async_copy(h_buf.at[m, pl.ds(k * R, R)], hid_out.at[pl.ds(row, R)], o_sem.at[m, k])

    def mlp_iter(t):
        @pl.when((t >= O2) & (t < n_mlp + O2))
        def _():
            stage2(t - O2)

        @pl.when((t >= O3) & (t < n_mlp + O3))
        def _():
            s = t - O3
            full = stage3(s)
            gate, up = full[:, :CW].astype(F32), full[:, CW:].astype(F32)
            act_all[s, pl.ds(0, R), :] = (jax.nn.silu(gate) * up).astype(BF16)
            to_core, to_chip, _ = act_copies(s)
            to_chip().start()
            to_core().start()

        @pl.when((t >= O4) & (t < n_mlp + O4))
        def _():
            _, to_chip, relay = act_copies(t - O4)
            to_chip().wait_recv()
            relay().start()

        @pl.when(t < n_mlp)
        def _():
            m, j = (0, t) if NM == 1 else (lax.div(t, n_ffn), lax.rem(t, n_ffn))

            @pl.when(t < n_ffn)
            def _():
                for cp in wgu_copy(t):
                    cp.wait()
            stage1(t, m, wgu_buf[j])

        @pl.when((t >= O5) & (t < n_mlp + O5))
        def _():
            s = t - O5
            m, j = (0, s) if NM == 1 else (lax.div(s, n_ffn), lax.rem(s, n_ffn))
            to_core, _, relay = act_copies(s)
            to_core().wait_recv()
            relay().wait_recv()

            @pl.when(s == 0)
            def _():
                wd_copy.wait()
            acc_buf[m] += dot(act_all[s], wd_buf[pl.ds(pl.multiple_of(j * CW, CW), CW), :])

    pl.semaphore_wait(barrier, 4)

    if head:
        for m in range(NM):
            attn_all[m, pl.ds(0, R), :] = attn_in[pl.ds(m * R, R), :]
            to_core, to_chip, _ = attn_copies(m)
            to_chip().start()
            to_core().start()
            acc_buf[m] = jnp.zeros(acc_buf.shape[1:], F32)
        for m in range(NM):
            _, to_chip, relay = attn_copies(m)
            to_chip().wait_recv()
            relay().start()
        for m in range(NM):
            for k in range(4):
                hid_copy(m, k).wait()
        wo_copy.wait()
        for m in range(NM):
            to_core, _, relay = attn_copies(m)
            to_core().wait_recv()
            relay().wait_recv()
            y_start(0, m, dot(attn_all[m], wo_buf[...]))
        for m in range(NM):
            y_finish(0, m)
            stats_start(0, m)
        for m in range(NM):
            norm(0, m, g_mlp[pl.ds(layer, 1), :])

        def body(t, c):
            mlp_iter(t)
            return c
        lax.fori_loop(0, n_mlp + O5, body, 0)
        for m in range(NM):
            y_start(1, m, acc_buf[m])
        for m in range(NM):
            y_finish(1, m)
            if tail:
                stats_start(1, m)
            for k in range(4):
                out_copy(m, k).start()
    else:
        for m in range(NM):
            for k in range(4):
                hid_copy(m, k).wait()
            stats_start(1, m)

    if tail:
        for cp in wqkv_copies:
            cp.wait()
        for m in range(NM):
            norm(1, m, g_attn[pl.ds(tail_layer, 1), :])
        n_all = n_qkv * NM
        for t in range(n_all + 3):
            if 1 <= t < n_all + 1:
                stage2(n_mlp + t - 1)
            if t < n_all:
                stage1(n_mlp + t, t // n_qkv, wqkv_buf[t % n_qkv])
            if t >= 3:
                m, j = divmod(t - 3, n_qkv)
                qkv_out[j, pl.ds(m * R, R), :] = stage3(n_mlp + t - 3)

    def drain(s, c):
        d_copy(s).wait_send()
        x_copy(s).wait_send()
        return c
    lax.fori_loop(0, dsend.shape[0], drain, 0)
    if head:
        def drain_act(s, c):
            for cp in act_copies(s):
                cp().wait_send()
            return c
        lax.fori_loop(0, n_mlp, drain_act, 0)
        for m in range(NM):
            for cp in attn_copies(m):
                cp().wait_send()
            for k in range(4):
                out_copy(m, k).wait()


def chain_call(head, tail, layer, cid, model_dim, hidden, attn=None, g_mlp=None, wo=None, wg=None, wu=None, wd=None, g_attn=None, wq=None, wk=None, wv=None):
    batch, feat = hidden.shape
    M = batch // NM
    R = M // 4
    vmem = pl.BlockSpec(memory_space=pltpu.VMEM)
    hbm = pl.BlockSpec(memory_space=pl.ANY)
    args, in_specs = [hidden], [hbm]
    out_shape, out_specs = [], []
    n_items = 0
    if head:
        args += [attn, g_mlp, wo, wg, wu, wd]
        in_specs += [vmem, vmem, hbm, hbm, hbm, hbm]
        out_shape.append(jax.ShapeDtypeStruct(hidden.shape, hidden.dtype))
        out_specs.append(hbm)
        n_ffn = wg.shape[2] // CW
        n_items += n_ffn * NM
    if tail:
        args += [g_attn, wq, wk, wv]
        in_specs += [vmem, hbm, hbm, hbm]
        out_shape.append(jax.ShapeDtypeStruct((6, batch // 4, IW), BF16))
        out_specs.append(vmem)
        n_items += 6 * NM
    dma = pltpu.SemaphoreType.DMA
    scratch = [
        pltpu.VMEM((NM, M, feat), BF16), pltpu.VMEM((NM, M, feat), BF16), pltpu.VMEM((2, NM, 4, 8, 128), F32),
        pltpu.VMEM((4, 2 * R, IW), F32), pltpu.VMEM((4, R, IW), F32),
        pltpu.VMEM((n_items, 2 * R, IW), BF16), pltpu.VMEM((n_items, 2 * R, IW), BF16),
        pltpu.VMEM((n_items, R, IW), BF16), pltpu.VMEM((n_items, R, IW), BF16),
        dma((NM, 4)), dma((2, NM, 3)), dma((2, NM, 3)), dma((n_items,)), dma((n_items,)), dma((n_items,)), dma((n_items,))]
    if head:
        scratch += [
            pltpu.VMEM((NM, M, attn.shape[1]), BF16), pltpu.VMEM(wo.shape[1:], BF16), pltpu.VMEM((n_ffn, feat, IW), BF16),
            pltpu.VMEM(wd.shape[1:], BF16), pltpu.VMEM((NM, M, feat), F32), pltpu.VMEM((n_ffn * NM, M, CW), BF16),
            pltpu.VMEM((2, NM, M, feat), BF16), pltpu.VMEM((2, NM, M, feat), BF16),
            dma((3, NM)), dma((3, NM)), dma((2, NM)), dma((2, NM)), dma((3, n_ffn * NM)), dma((3, n_ffn * NM)),
            dma, dma((2, n_ffn)), dma, dma((NM, 4))]
    if tail:
        scratch += [pltpu.VMEM((6, feat, IW), BF16), dma((6,))]
    return pl.pallas_call(
        functools.partial(chain_kernel, head, tail, layer, model_dim),
        out_shape=out_shape, in_specs=in_specs, out_specs=out_specs, scratch_shapes=scratch,
        name=f'chain_{int(head)}{int(tail)}',
        compiler_params=pltpu.CompilerParams(collective_id=cid, has_side_effects=True, vmem_limit_bytes=60 * 1024 * 1024),
    )(*args)


def attn_kernel(layer, pos_ref, qkv_ref, cos_ref, sin_ref, qg_ref, kg_ref, k_ref, v_ref, *refs):
    k_out, v_out, o_ref, q_buf, kv_buf, o_buf = refs[-6:]
    step = pl.program_id(0)
    local = o_ref.shape[0]
    n_q = q_buf.shape[0] // local
    n_kv = kv_buf.shape[1] // local
    n_rows = k_ref.shape[2]
    group = n_q // n_kv
    per_chunk = qkv_ref.shape[2] // HEAD_DIM

    def head_of(idx):
        return qkv_ref[idx // per_chunk, :, pl.ds((idx % per_chunk) * HEAD_DIM, HEAD_DIM)].astype(F32)

    @pl.when(step == 0)
    def _():
        cos_tab, sin_tab = cos_ref[...], sin_ref[...]

        def norm_rope(vals, gain):
            normed = vals * lax.rsqrt(jnp.mean(vals * vals, axis=-1, keepdims=True) + NORM_EPS) * gain
            return (normed * cos_tab + pltpu.roll(normed, HEAD_DIM // 2, 1) * sin_tab).astype(BF16).astype(F32)
        for h in range(n_q):
            q_buf[pl.ds(h * local, local), :] = norm_rope(head_of(h), qg_ref[pl.ds(layer, 1), :].astype(F32))
        for h in range(n_kv):
            kv_buf[0, pl.ds(h * local, local), :] = norm_rope(head_of(n_q + h), kg_ref[pl.ds(layer, 1), :].astype(F32))
            kv_buf[1, pl.ds(h * local, local), :] = head_of(n_q + n_kv + h)

    row_ids = lax.broadcasted_iota(jnp.int32, (16, HEAD_DIM), 0)
    lane_ids = lax.broadcasted_iota(jnp.int32, (n_q, n_rows), 1)
    head_hit = lax.rem(lane_ids, n_kv) == lax.div(lax.broadcasted_iota(jnp.int32, (n_q, n_rows), 0), group)
    lane_of = jnp.where(head_hit, lane_ids, n_rows)
    for i in range(SB):
        b = step * SB + i
        pos = pos_ref[b]
        row = pos * n_kv
        base = pl.multiple_of(lax.div(row, 16) * 16, 16)
        hit = lax.div(row_ids, n_kv) == lax.div(row - base, n_kv)
        for src, dst, which in ((k_ref, k_out, 0), (v_ref, v_out, 1)):
            dst[0, i] = src[0, i]
            new = kv_buf[which, pl.ds(b, n_kv, stride=local), :]
            new = jnp.concatenate([new] * (16 // n_kv), axis=0)
            old = src[0, i, pl.ds(base, 16), :]
            dst[0, i, pl.ds(base, 16), :] = jnp.where(hit, new, old.astype(F32)).astype(BF16)
        q = q_buf[pl.ds(b, n_q, stride=local), :].astype(BF16)
        scores = lax.dot_general(q, k_out[0, i], (((1,), (1,)), ((), ())), preferred_element_type=F32) * (HEAD_DIM ** -0.5)
        scores = jnp.where(lane_of < row + n_kv, scores, -1e30)
        e = jnp.exp(scores - jnp.max(scores, axis=-1, keepdims=True))
        probs = (e / jnp.sum(e, axis=-1, keepdims=True)).astype(BF16)
        o_buf[pl.ds(b, n_q, stride=local), :] = dot(probs, v_out[0, i])

    @pl.when(step == pl.num_programs(0) - 1)
    def _():
        for h in range(n_q):
            o_ref[:, pl.ds(h * HEAD_DIM, HEAD_DIM)] = o_buf[pl.ds(h * local, local), :].astype(BF16)


def attn_call(layer, pos, qkv, cos_tab, sin_tab, q_gain, k_gain, k_cache, v_cache, prev):
    layers, local, n_rows, _ = k_cache.shape
    n_kv = 4
    n_q = 16
    smem = pl.BlockSpec(memory_space=pltpu.SMEM)
    vmem = pl.BlockSpec(memory_space=pltpu.VMEM)
    block = pl.BlockSpec((1, SB, n_rows, HEAD_DIM), lambda s: (layer, s, 0, 0))
    args = [pos, qkv, cos_tab, sin_tab, q_gain, k_gain, k_cache, v_cache]
    in_specs = [smem, vmem, vmem, vmem, vmem, vmem, block, block]
    aliases = {}
    if prev is not None:
        args += list(prev)
        in_specs += [pl.BlockSpec(memory_space=pl.ANY)] * 2
        aliases = {8: 0, 9: 1}
    return pl.pallas_call(
        functools.partial(attn_kernel, layer), grid=(local // SB,),
        out_shape=[jax.ShapeDtypeStruct(k_cache.shape, BF16)] * 2 + [jax.ShapeDtypeStruct((local, n_q * HEAD_DIM), BF16)],
        in_specs=in_specs,
        out_specs=[block, block, pl.BlockSpec((local, n_q * HEAD_DIM), lambda s: (0, 0))],
        scratch_shapes=[pltpu.VMEM((n_q * local, HEAD_DIM), F32), pltpu.VMEM((2, n_kv * local, HEAD_DIM), F32), pltpu.VMEM((n_q * local, HEAD_DIM), F32)],
        input_output_aliases=aliases, name=f'attn_{layer}',
        compiler_params=pltpu.CompilerParams(dimension_semantics=('arbitrary',), vmem_limit_bytes=48 * 1024 * 1024),
    )(*args)


def solution(mesh):
    group_size = mesh.shape['x']
    cache_spec = P(None, ('dp', 'x'), None, 'y', None)
    col_spec = P(None, 'x', 'y')
    row_spec = P(None, 'y', 'x')
    in_specs = (P('dp', 'x'), P('dp'), cache_spec, cache_spec, P(None, 'x'), P(None, 'x'), P(), P(), col_spec, col_spec, col_spec, row_spec, col_spec, col_spec, row_spec)
    out_specs = (P('dp', 'x'), cache_spec, cache_spec)

    def device_step(hidden, positions, k_cache, v_cache, g_attn, g_mlp, q_gain, k_gain, w_q, w_k, w_v, w_o, w_gate, w_up, w_down):
        model_dim = hidden.shape[1] * group_size
        layers, local, cache_len, n_kv, _ = k_cache.shape
        my_pos = lax.dynamic_slice_in_dim(positions, lax.axis_index('x') * local, local)
        half = HEAD_DIM // 2
        inv_freq = jnp.power(ROPE_BASE, -2.0 * jnp.arange(half, dtype=F32) / HEAD_DIM)
        angles = my_pos.astype(F32)[:, None] * inv_freq[None, :]
        cos_half, sin_half = jnp.cos(angles), jnp.sin(angles)
        cos_tab = jnp.concatenate([cos_half, cos_half], axis=1)
        sin_tab = jnp.concatenate([-sin_half, sin_half], axis=1)
        k_rows = k_cache.reshape(layers, local, cache_len * n_kv, HEAD_DIM)
        v_rows = v_cache.reshape(layers, local, cache_len * n_kv, HEAD_DIM)
        (qkv,) = chain_call(False, True, 0, 0, model_dim, hidden, g_attn=g_attn, wq=w_q, wk=w_k, wv=w_v)
        k_new, v_new, attn = attn_call(0, my_pos, qkv, cos_tab, sin_tab, q_gain, k_gain, k_rows, v_rows, None)
        hidden, qkv = chain_call(True, True, 0, 1, model_dim, hidden, attn, g_mlp, w_o, w_gate, w_up, w_down, g_attn, w_q, w_k, w_v)
        k_new, v_new, attn = attn_call(1, my_pos, qkv, cos_tab, sin_tab, q_gain, k_gain, k_rows, v_rows, (k_new, v_new))
        (hidden,) = chain_call(True, False, 1, 2, model_dim, hidden, attn, g_mlp, w_o, w_gate, w_up, w_down)
        return hidden, k_new.reshape(k_cache.shape), v_new.reshape(v_cache.shape)

    return jax.shard_map(device_step, mesh=mesh, in_specs=in_specs, out_specs=out_specs, check_vma=False)
```

```python
import functools

import jax
import jax.numpy as jnp
from jax import lax
from jax.experimental import pallas as pl
from jax.experimental.pallas import tpu as pltpu
from jax.sharding import PartitionSpec as P

HEAD_DIM = 128
NORM_EPS = 1e-6
ROPE_BASE = 1000000.0
MESH = pl.DeviceIdType.MESH
BF16 = jnp.bfloat16
F32 = jnp.float32

CW = 256
IW = 2 * CW
O2, O3, O4, O5 = 2, 5, 8, 10
E1, E2, E3, E4 = 2, 8, 6, 10
RING = 8
SB = 8
NBUF = 3
MASK = (0, 2, 1, 3)
POS = (0, 2, 1, 3)


def groups(head):
    return 2 if head else 1


def dot(a, b):
    return jnp.dot(a, b, preferred_element_type=F32)


def chain_kernel(head, tail, layer, n_pref, model_dim, *refs):
    NM = groups(head)
    it = iter(refs)
    hid_in = next(it)
    if head:
        attn_in, g_mlp = next(it), next(it)
        wo_in, wg_in, wu_in, wd_in = (next(it).at[layer] for _ in range(4))
    if tail:
        tail_layer = layer + 1 if head else layer
        g_attn = next(it)
        wq_in, wk_in, wv_in, k_in, v_in = (next(it).at[tail_layer] for _ in range(5))
    if head:
        hid_out = next(it)
    if tail:
        qkv_out, pref_out = next(it), next(it)
    h_buf, n_buf, stat_buf, keep_buf, own_buf, dsend, drecv, xsend, xrecv = (next(it) for _ in range(9))
    h_sem, st_ss, st_rs, d_ss, d_rs, x_ss, x_rs = (next(it) for _ in range(7))
    if head:
        attn_all, wo_buf, wgu_buf, wd_buf, acc_buf, act_all, y_send, y_recv = (next(it) for _ in range(8))
        ag_ss, ag_rs, y_ss, y_rs, act_ss, act_rs, wo_sem, wgu_sem, wd_sem, o_sem, a_sem = (next(it) for _ in range(11))
    if tail:
        wqkv_buf, wqkv_sem, pref_sem = (next(it) for _ in range(3))

    me = lax.axis_index('x')
    yy = lax.axis_index('y')
    chip, core = lax.div(me, 2), lax.rem(me, 2)
    d1 = chip * 2 + (1 - core)
    d2 = (1 - chip) * 2 + core
    d3 = (1 - chip) * 2 + (1 - core)
    quarter = (me, d2, d1, d3)
    R = h_buf.shape[1] // 4
    M = 4 * R
    n_ffn = act_all.shape[0] // NM if head else 0
    n_mlp = n_ffn * NM
    n_qkv = 6
    ring = dsend.shape[0]
    n_items = drecv.shape[0]

    def after_ring(s, action):
        if isinstance(s, int):
            if s >= ring:
                action()
        else:
            pl.when(s >= ring)(action)

    barrier = pltpu.get_barrier_semaphore()
    for peer in ({'x': d1}, {'x': d2}, {'x': d3}, {'y': 1 - yy}):
        pl.semaphore_signal(barrier, inc=1, device_id=peer, device_id_type=MESH)

    def remote(src, dst, ss, rs, peer):
        return pltpu.make_async_remote_copy(src_ref=src, dst_ref=dst, send_sem=ss, recv_sem=rs, device_id=peer, device_id_type=MESH)

    def attn_own(m):
        return pltpu.make_async_copy(attn_in.at[pl.ds(m * R, R)], attn_all.at[m, pl.ds(0, R)], a_sem.at[m])
    if head:
        for m in range(NM):
            attn_own(m).start()

    def hid_copy(m, k):
        row = pl.multiple_of(quarter[k] * (NM * R) + m * R, R)
        return pltpu.make_async_copy(hid_in.at[pl.ds(row, R)], h_buf.at[m, pl.ds(k * R, R)], h_sem.at[m, k])

    for m in range(NM):
        for k in range(4):
            hid_copy(m, k).start()

    def wgu_copy(j):
        off = pl.multiple_of(j * CW, CW)
        return (pltpu.make_async_copy(wg_in.at[:, pl.ds(off, CW)], wgu_buf.at[j, :, pl.ds(0, CW)], wgu_sem.at[0, j]),
                pltpu.make_async_copy(wu_in.at[:, pl.ds(off, CW)], wgu_buf.at[j, :, pl.ds(CW, CW)], wgu_sem.at[1, j]))

    if head:
        wo_copy = pltpu.make_async_copy(wo_in, wo_buf, wo_sem)
        wd_copy = pltpu.make_async_copy(wd_in, wd_buf, wd_sem)
    if tail:
        wqkv_copies = [pltpu.make_async_copy(wq_in.at[:, pl.ds(j * IW, IW)], wqkv_buf.at[j], wqkv_sem.at[j]) for j in range(4)]
        wqkv_copies += [pltpu.make_async_copy(w, wqkv_buf.at[j], wqkv_sem.at[j]) for j, w in ((4, wk_in), (5, wv_in))]
    if head:
        wo_copy.start()

        def start_wgu(j, c):
            for cp in wgu_copy(j):
                cp.start()
            return c
        lax.fori_loop(0, n_ffn, start_wgu, 0)
        wd_copy.start()
    if tail:
        for cp in wqkv_copies:
            cp.start()

    def pref_copy(blk, c):
        seqs = pl.ds(blk * SB, SB)
        return pltpu.make_async_copy((k_in, v_in)[c].at[seqs], pref_out.at[blk, c], pref_sem.at[blk, c])
    if tail:
        for blk in range(n_pref):
            for c in (0, 1):
                pref_copy(blk, c).start()

    def diag():
        return lax.broadcasted_iota(jnp.int32, (R, 128), 0) == lax.broadcasted_iota(jnp.int32, (R, 128), 1)

    def stat_send(kind, m, a):
        peer = (None, d1, d2, d3)[a]
        return remote(stat_buf.at[kind, m, 0], stat_buf.at[kind, m, a], st_ss.at[kind, m, a - 1], st_rs.at[kind, m, a - 1], {'x': peer})

    def stats_start(kind, m):
        for k in range(4):
            hv = h_buf[m, pl.ds(k * R, R), :].astype(F32)
            row_sum = jnp.sum(hv * hv, axis=1, keepdims=True)
            stat_buf[kind, m, 0, pl.ds(k, 1), :] = jnp.sum(jnp.where(diag(), row_sum, 0.0), axis=0, keepdims=True)
        for a in (1, 2, 3):
            stat_send(kind, m, a).start()

    def norm(kind, m, gain):
        for a in (1, 2, 3):
            stat_send(kind, m, a).wait()
        gain_row = gain.astype(F32)
        for k in range(4):
            total = stat_buf[kind, m, 0, pl.ds(k, 1), :]
            for a in (1, 2, 3):
                total = total + stat_buf[kind, m, a, pl.ds(POS[MASK[k] ^ a], 1), :]
            col = jnp.sum(jnp.where(diag(), total, 0.0), axis=1, keepdims=True)
            hv = h_buf[m, pl.ds(k * R, R), :].astype(F32)
            n_buf[m, pl.ds(k * R, R), :] = (hv * lax.rsqrt(col / model_dim + NORM_EPS) * gain_row).astype(BF16)

    def d_copy(s):
        return remote(dsend.at[lax.rem(s, ring)], drecv.at[s], d_ss.at[s], d_rs.at[s], {'x': d1})

    def x_copy(s):
        return remote(xsend.at[lax.rem(s, ring)], xrecv.at[s], x_ss.at[s], x_rs.at[s], {'x': d2})

    def stage1(s, m, w):
        part = dot(n_buf[m], w)
        keep_buf[lax.rem(s, keep_buf.shape[0])] = part[:2 * R]
        after_ring(s, lambda: d_copy(s - ring).wait_send())
        dsend[lax.rem(s, ring)] = part[2 * R:].astype(BF16)
        d_copy(s).start()

    def stage2(s):
        d_copy(s).wait_recv()
        slot = lax.rem(s, keep_buf.shape[0])
        after_ring(s, lambda: x_copy(s - ring).wait_send())
        xsend[lax.rem(s, ring)] = (keep_buf[slot, pl.ds(R, R), :] + drecv[s, pl.ds(R, R), :].astype(F32)).astype(BF16)
        x_copy(s).start()
        own_buf[lax.rem(s, own_buf.shape[0])] = keep_buf[slot, pl.ds(0, R), :] + drecv[s, pl.ds(0, R), :].astype(F32)

    def stage3(s):
        x_copy(s).wait_recv()
        return (own_buf[lax.rem(s, own_buf.shape[0])] + xrecv[s].astype(F32)).astype(BF16)

    def gather_copies(buf, i, ss, rs):
        own, other = buf.at[i, pl.ds(0, R)], buf.at[i, pl.ds(R, R)]
        return (lambda: remote(own, buf.at[i, pl.ds(2 * R, R)], ss.at[0, i], rs.at[0, i], {'x': d1}),
                lambda: remote(own, buf.at[i, pl.ds(R, R)], ss.at[1, i], rs.at[1, i], {'x': d2}),
                lambda: remote(other, buf.at[i, pl.ds(3 * R, R)], ss.at[2, i], rs.at[2, i], {'x': d1}))

    def attn_copies(m):
        return gather_copies(attn_all, m, ag_ss, ag_rs)

    def y_copy(kind, m):
        return remote(y_send.at[kind, m], y_recv.at[kind, m], y_ss.at[kind, m], y_rs.at[kind, m], {'y': 1 - yy})

    def y_start(kind, m, value):
        y_send[kind, m] = value.astype(BF16)
        y_copy(kind, m).start()

    def y_finish(kind, m):
        y_copy(kind, m).wait()
        total = (y_send[kind, m].astype(F32) + y_recv[kind, m].astype(F32)).astype(BF16)
        h_buf[m] = (h_buf[m].astype(F32) + total.astype(F32)).astype(BF16)

    def act_copies(t):
        return gather_copies(act_all, t, act_ss, act_rs)

    def out_copy(m, k):
        row = pl.multiple_of(quarter[k] * (NM * R) + m * R, R)
        return pltpu.make_async_copy(h_buf.at[m, pl.ds(k * R, R)], hid_out.at[pl.ds(row, R)], o_sem.at[m, k])

    def mid_ready(m):
        y_finish(0, m)
        stats_start(0, m)

    def layer_done(m):
        y_finish(1, m)
        if tail:
            stats_start(1, m)
        for k in range(4):
            out_copy(m, k).start()

    def mlp_iter(t):
        @pl.when((t >= O2) & (t < n_mlp + O2))
        def _():
            stage2(t - O2)

        @pl.when((t >= O3) & (t < n_mlp + O3))
        def _():
            s = t - O3
            full = stage3(s)
            gate, up = full[:, :CW].astype(F32), full[:, CW:].astype(F32)
            act_all[s, pl.ds(0, R), :] = (jax.nn.silu(gate) * up).astype(BF16)
            to_core, to_chip, _ = act_copies(s)
            to_chip().start()
            to_core().start()

        @pl.when((t >= O4) & (t < n_mlp + O4))
        def _():
            _, to_chip, relay = act_copies(t - O4)
            to_chip().wait_recv()
            relay().start()

        @pl.when(t < n_mlp)
        def _():
            m, j = (0, t) if NM == 1 else (lax.div(t, n_ffn), lax.rem(t, n_ffn))

            @pl.when(t < n_ffn)
            def _():
                for cp in wgu_copy(t):
                    cp.wait()
            stage1(t, m, wgu_buf[j])

        @pl.when((t >= O5) & (t < n_mlp + O5))
        def _():
            s = t - O5
            m, j = (0, s) if NM == 1 else (lax.div(s, n_ffn), lax.rem(s, n_ffn))
            to_core, _, relay = act_copies(s)
            to_core().wait_recv()
            relay().wait_recv()

            @pl.when(s == 0)
            def _():
                wd_copy.wait()
            acc_buf[m] += dot(act_all[s], wd_buf[pl.ds(pl.multiple_of(j * CW, CW), CW), :])

    pl.semaphore_wait(barrier, 4)

    if head:
        for m in range(NM):
            attn_own(m).wait()
            to_core, to_chip, _ = attn_copies(m)
            to_chip().start()
            to_core().start()
            acc_buf[m] = jnp.zeros(acc_buf.shape[1:], F32)
        for m in range(NM):
            _, to_chip, relay = attn_copies(m)
            to_chip().wait_recv()
            relay().start()
        for m in range(NM):
            for k in range(4):
                hid_copy(m, k).wait()
        wo_copy.wait()
        for m in range(NM):
            to_core, _, relay = attn_copies(m)
            to_core().wait_recv()
            relay().wait_recv()
            y_start(0, m, dot(attn_all[m], wo_buf[...]))
        y_finish(0, 0)
        stats_start(0, 0)
        norm(0, 0, g_mlp[pl.ds(layer, 1), :])
        events = {}
        if NM == 2:
            first_done = n_ffn - 1 + O5
            events = {E1: lambda: mid_ready(1), E2: lambda: norm(0, 1, g_mlp[pl.ds(layer, 1), :]),
                      first_done: lambda: y_start(1, 0, acc_buf[0]), first_done + E3: lambda: layer_done(0)}
            if tail:
                events[first_done + E4] = lambda: norm(1, 0, g_attn[pl.ds(tail_layer, 1), :])

        def body(t, c):
            mlp_iter(t)
            for at, event in events.items():
                pl.when(t == at)(event)
            return c
        lax.fori_loop(0, n_mlp + O5, body, 0)
        y_start(1, NM - 1, acc_buf[NM - 1])
        if not (tail and NM == 2):
            layer_done(NM - 1)
    else:
        for m in range(NM):
            for k in range(4):
                hid_copy(m, k).wait()
            stats_start(1, m)

    if tail:
        for cp in wqkv_copies:
            cp.wait()
        n_all = n_qkv * NM
        if not (head and NM == 2):
            for m in range(NM):
                norm(1, m, g_attn[pl.ds(tail_layer, 1), :])
        for t in range(n_all + 3):
            if 1 <= t < n_all + 1:
                stage2(n_mlp + t - 1)
            if head and NM == 2 and t == n_qkv:
                layer_done(1)
                norm(1, 1, g_attn[pl.ds(tail_layer, 1), :])
            if t < n_all:
                stage1(n_mlp + t, t // n_qkv, wqkv_buf[t % n_qkv])
            if t >= 3:
                m, j = divmod(t - 3, n_qkv)
                qkv_out[j, pl.ds(m * R, R), :] = stage3(n_mlp + t - 3)

    if tail:
        for blk in range(n_pref):
            for c in (0, 1):
                pref_copy(blk, c).wait()

    def drain(s, c):
        d_copy(s).wait_send()
        x_copy(s).wait_send()
        return c
    lax.fori_loop(max(n_items - ring, 0), n_items, drain, 0)
    if head:
        def drain_act(s, c):
            for cp in act_copies(s):
                cp().wait_send()
            return c
        lax.fori_loop(0, n_mlp, drain_act, 0)
        for m in range(NM):
            for cp in attn_copies(m):
                cp().wait_send()
            for k in range(4):
                out_copy(m, k).wait()


def chain_call(head, tail, layer, cid, n_pref, vmem_mib, model_dim, hidden, attn=None, g_mlp=None, wo=None, wg=None, wu=None, wd=None, g_attn=None, wq=None, wk=None, wv=None, k_rows=None, v_rows=None):
    batch, feat = hidden.shape
    NM = groups(head)
    M = batch // NM
    R = M // 4
    vmem = pl.BlockSpec(memory_space=pltpu.VMEM)
    hbm = pl.BlockSpec(memory_space=pltpu.HBM)
    args, in_specs = [hidden], [hbm]
    out_shape, out_specs = [], []
    n_items = 0
    if head:
        args += [attn, g_mlp, wo, wg, wu, wd]
        in_specs += [hbm, vmem, hbm, hbm, hbm, hbm]
        out_shape.append(jax.ShapeDtypeStruct(hidden.shape, hidden.dtype))
        out_specs.append(hbm)
        n_ffn = wg.shape[2] // CW
        n_items += n_ffn * NM
    if tail:
        args += [g_attn, wq, wk, wv, k_rows, v_rows]
        in_specs += [vmem] + [hbm] * 5
        out_shape.append(jax.ShapeDtypeStruct((6, batch // 4, IW), BF16))
        out_specs.append(vmem)
        out_shape.append(pltpu.VMEM((n_pref, 2, SB) + k_rows.shape[2:], BF16))
        out_specs.append(vmem)
        n_items += 6 * NM
    dma = pltpu.SemaphoreType.DMA
    scratch = [
        pltpu.VMEM((NM, M, feat), BF16), pltpu.VMEM((NM, M, feat), BF16), pltpu.VMEM((2, NM, 4, 8, 128), F32),
        pltpu.VMEM((O2 + 1, 2 * R, IW), F32), pltpu.VMEM((O3 - O2 + 1, R, IW), F32),
        pltpu.VMEM((RING, 2 * R, IW), BF16), pltpu.VMEM((n_items, 2 * R, IW), BF16),
        pltpu.VMEM((RING, R, IW), BF16), pltpu.VMEM((n_items, R, IW), BF16),
        dma((NM, 4)), dma((2, NM, 3)), dma((2, NM, 3)), dma((n_items,)), dma((n_items,)), dma((n_items,)), dma((n_items,))]
    if head:
        scratch += [
            pltpu.VMEM((NM, M, attn.shape[1]), BF16), pltpu.VMEM(wo.shape[1:], BF16), pltpu.VMEM((n_ffn, feat, IW), BF16),
            pltpu.VMEM(wd.shape[1:], BF16), pltpu.VMEM((NM, M, feat), F32), pltpu.VMEM((n_ffn * NM, M, CW), BF16),
            pltpu.VMEM((2, NM, M, feat), BF16), pltpu.VMEM((2, NM, M, feat), BF16),
            dma((3, NM)), dma((3, NM)), dma((2, NM)), dma((2, NM)), dma((3, n_ffn * NM)), dma((3, n_ffn * NM)),
            dma, dma((2, n_ffn)), dma, dma((NM, 4)), dma((NM,))]
    if tail:
        scratch += [pltpu.VMEM((6, feat, IW), BF16), dma((6,)), dma((n_pref, 2))]
    return pl.pallas_call(
        functools.partial(chain_kernel, head, tail, layer, n_pref, model_dim),
        out_shape=out_shape, in_specs=in_specs, out_specs=out_specs, scratch_shapes=scratch,
        name=f'chain_{int(head)}{int(tail)}',
        compiler_params=pltpu.CompilerParams(collective_id=cid, has_side_effects=True, vmem_limit_bytes=vmem_mib * 1024 * 1024),
    )(*args)


def attn_kernel(layer, n_pref, pos_ref, qkv_hbm, tabs_hbm, k_hbm, v_hbm, *refs):
    k_out, v_out, o_ref, pref, kv_slots, q_buf, kv_buf, o_buf, s_buf, p_buf, qkv_ref, tabs_ref, in_sem, out_sem, small_sem = refs[-15:]
    small = (pltpu.make_async_copy(qkv_hbm, qkv_ref, small_sem.at[0]), pltpu.make_async_copy(tabs_hbm, tabs_ref, small_sem.at[1]))
    for cp in small:
        cp.start()
    local = o_ref.shape[0]
    n_q = q_buf.shape[0] // local
    n_kv = kv_buf.shape[1] // local
    n_rows = k_hbm.shape[2]
    group = n_q // n_kv
    per_chunk = qkv_ref.shape[2] // HEAD_DIM
    n_blocks = local // SB

    def held(blk, early):
        return pref.at[blk] if early else kv_slots.at[lax.rem(blk - n_pref, NBUF)]

    def run(blk, early, out, wait):
        seqs = pl.ds(blk * SB, SB)
        for c in (0, 1):
            here = held(blk, early).at[c]
            if out:
                cp = pltpu.make_async_copy(here, (k_out, v_out)[c].at[layer, seqs], out_sem.at[blk, c])
            else:
                cp = pltpu.make_async_copy((k_hbm, v_hbm)[c].at[layer, seqs], here, in_sem.at[blk, c])
            cp.wait() if wait else cp.start()

    for blk in range(n_pref, min(n_pref + NBUF, n_blocks)):
        run(blk, False, False, False)

    def head_of(idx):
        return qkv_ref[idx // per_chunk, :, pl.ds((idx % per_chunk) * HEAD_DIM, HEAD_DIM)].astype(F32)

    for cp in small:
        cp.wait()
    cos_tab, sin_tab = tabs_ref[pl.ds(0, local), :], tabs_ref[pl.ds(local, local), :]
    gains = [tabs_ref[pl.ds(2 * local + 2 * layer + i, 1), :] for i in (0, 1)]

    def norm_rope(vals, gain):
        normed = vals * lax.rsqrt(jnp.mean(vals * vals, axis=-1, keepdims=True) + NORM_EPS) * gain
        return (normed * cos_tab + pltpu.roll(normed, HEAD_DIM // 2, 1) * sin_tab).astype(BF16).astype(F32)
    for h in range(n_q):
        q_buf[pl.ds(h * local, local), :] = norm_rope(head_of(h), gains[0])
    for h in range(n_kv):
        kv_buf[0, pl.ds(h * local, local), :] = norm_rope(head_of(n_q + h), gains[1])
        kv_buf[1, pl.ds(h * local, local), :] = head_of(n_q + n_kv + h)

    row_ids = lax.broadcasted_iota(jnp.int32, (16, HEAD_DIM), 0)
    lane_ids = lax.broadcasted_iota(jnp.int32, (n_q, n_rows), 1)
    head_hit = lax.rem(lane_ids, n_kv) == lax.div(lax.broadcasted_iota(jnp.int32, (n_q, n_rows), 0), group)
    lane_of = jnp.where(head_hit, lane_ids, n_rows)

    def block_step(blk, early):
        ref = held(blk, early)
        if not early:
            run(blk, False, False, True)
        for i in range(SB):
            b = blk * SB + i
            row = pos_ref[b] * n_kv
            base = pl.multiple_of(lax.div(row, 16) * 16, 16)
            hit = lax.div(row_ids, n_kv) == lax.div(row - base, n_kv)
            for c in (0, 1):
                new = kv_buf[c, pl.ds(b, n_kv, stride=local), :]
                new = jnp.concatenate([new] * (16 // n_kv), axis=0)
                old = ref[c, i, pl.ds(base, 16), :]
                ref[c, i, pl.ds(base, 16), :] = jnp.where(hit, new, old.astype(F32)).astype(BF16)
        for i in range(SB):
            q = q_buf[pl.ds(blk * SB + i, n_q, stride=local), :].astype(BF16)
            s_buf[i] = lax.dot_general(q, ref[0, i], (((1,), (1,)), ((), ())), preferred_element_type=F32)
        run(blk, early, True, False)
        for i in range(SB):
            row = pos_ref[blk * SB + i] * n_kv
            scores = jnp.where(lane_of < row + n_kv, s_buf[i] * (HEAD_DIM ** -0.5), -1e30)
            e = jnp.exp(scores - jnp.max(scores, axis=-1, keepdims=True))
            p_buf[i] = (e / jnp.sum(e, axis=-1, keepdims=True)).astype(BF16)
        for i in range(SB):
            o_buf[pl.ds(blk * SB + i, n_q, stride=local), :] = dot(p_buf[i], ref[1, i])

    def early_step(blk, carry):
        block_step(blk, True)
        return carry

    def late_step(blk, carry):
        block_step(blk, False)

        @pl.when((blk > n_pref) & (blk - 1 + NBUF < n_blocks))
        def _():
            run(blk - 1, False, True, True)
            run(blk - 1 + NBUF, False, False, False)
        return carry
    lax.fori_loop(0, n_pref, early_step, 0)
    if n_pref < n_blocks:
        lax.fori_loop(n_pref, n_blocks, late_step, 0)

    for h in range(n_q):
        o_ref[:, pl.ds(h * HEAD_DIM, HEAD_DIM)] = o_buf[pl.ds(h * local, local), :].astype(BF16)
    for blk in range(n_pref):
        run(blk, True, True, True)
    for blk in range(max(n_blocks - NBUF, n_pref), n_blocks):
        run(blk, False, True, True)


def attn_call(layer, pos, qkv, tabs, k_cache, v_cache, pref, prev):
    layers, local, n_rows, _ = k_cache.shape
    n_kv = 4
    n_q = 16
    smem = pl.BlockSpec(memory_space=pltpu.SMEM)
    vmem = pl.BlockSpec(memory_space=pltpu.VMEM)
    hbm = pl.BlockSpec(memory_space=pltpu.HBM)
    args = [pos, qkv, tabs, k_cache, v_cache, pref]
    in_specs = [smem, hbm, hbm, hbm, hbm, vmem]
    aliases = {5: 3}
    n_pref, n_blocks = pref.shape[0], local // SB
    if prev is not None:
        args += list(prev)
        in_specs += [hbm] * 2
        aliases.update({6: 0, 7: 1})
    return pl.pallas_call(
        functools.partial(attn_kernel, layer, n_pref),
        out_shape=[jax.ShapeDtypeStruct(k_cache.shape, BF16)] * 2 + [jax.ShapeDtypeStruct((local, n_q * HEAD_DIM), BF16), jax.ShapeDtypeStruct(pref.shape, BF16)],
        in_specs=in_specs,
        out_specs=[hbm, hbm, vmem, vmem],
        scratch_shapes=[pltpu.VMEM((min(NBUF, max(n_blocks - n_pref, 1)) if n_pref < n_blocks else 1, 2, SB if n_pref < n_blocks else 1, n_rows, HEAD_DIM), BF16),
                        pltpu.VMEM((n_q * local, HEAD_DIM), F32), pltpu.VMEM((2, n_kv * local, HEAD_DIM), F32), pltpu.VMEM((n_q * local, HEAD_DIM), F32),
                        pltpu.VMEM((SB, n_q, n_rows), F32), pltpu.VMEM((SB, n_q, n_rows), BF16),
                        pltpu.VMEM(qkv.shape, BF16), pltpu.VMEM(tabs.shape, F32),
                        pltpu.SemaphoreType.DMA((n_blocks, 2)), pltpu.SemaphoreType.DMA((n_blocks, 2)), pltpu.SemaphoreType.DMA((2,))],
        input_output_aliases=aliases, name=f'attn_{layer}',
        compiler_params=pltpu.CompilerParams(vmem_limit_bytes=(20 if n_pref == n_blocks else 22) * 1024 * 1024),
    )(*args)


def solution(mesh):
    group_size = mesh.shape['x']
    cache_spec = P(None, ('dp', 'x'), None, 'y', None)
    col_spec = P(None, 'x', 'y')
    row_spec = P(None, 'y', 'x')
    in_specs = (P('dp', 'x'), P('dp'), cache_spec, cache_spec, P(None, 'x'), P(None, 'x'), P(), P(), col_spec, col_spec, col_spec, row_spec, col_spec, col_spec, row_spec)
    out_specs = (P('dp', 'x'), cache_spec, cache_spec)

    def device_step(hidden, positions, k_cache, v_cache, g_attn, g_mlp, q_gain, k_gain, w_q, w_k, w_v, w_o, w_gate, w_up, w_down):
        model_dim = hidden.shape[1] * group_size
        layers, local, cache_len, n_kv, _ = k_cache.shape
        my_pos = lax.dynamic_slice_in_dim(positions, lax.axis_index('x') * local, local)
        half = HEAD_DIM // 2
        inv_freq = jnp.power(ROPE_BASE, -2.0 * jnp.arange(half, dtype=F32) / HEAD_DIM)
        angles = my_pos.astype(F32)[:, None] * inv_freq[None, :]
        cos_half, sin_half = jnp.cos(angles), jnp.sin(angles)
        gains = jnp.stack([q_gain[0], k_gain[0], q_gain[1], k_gain[1]]).astype(F32)
        tabs = jnp.concatenate([jnp.concatenate([cos_half, cos_half], axis=1), jnp.concatenate([-sin_half, sin_half], axis=1), gains, jnp.zeros((4, HEAD_DIM), F32)])
        tabs, my_pos, hidden = lax.optimization_barrier((tabs, my_pos, hidden))
        k_rows = k_cache.reshape(layers, local, cache_len * n_kv, HEAD_DIM)
        v_rows = v_cache.reshape(layers, local, cache_len * n_kv, HEAD_DIM)
        attn_tabs = (tabs, k_rows, v_rows)
        caches = {'k_rows': k_rows, 'v_rows': v_rows}
        qkv, pref = chain_call(False, True, 0, 0, 8, 16, model_dim, hidden, g_attn=g_attn, wq=w_q, wk=w_k, wv=w_v, **caches)
        k_new, v_new, attn, _ = attn_call(0, my_pos, qkv, *attn_tabs, pref, None)
        hidden, qkv, pref = chain_call(True, True, 0, 1, 5, 40, model_dim, hidden, attn, g_mlp, w_o, w_gate, w_up, w_down, g_attn, w_q, w_k, w_v, **caches)
        k_new, v_new, attn, _ = attn_call(1, my_pos, qkv, *attn_tabs, pref, (k_new, v_new))
        (hidden,) = chain_call(True, False, 1, 2, 0, 60, model_dim, hidden, attn, g_mlp, w_o, w_gate, w_up, w_down)
        return hidden, k_new.reshape(k_cache.shape), v_new.reshape(v_cache.shape)

    return jax.shard_map(device_step, mesh=mesh, in_specs=in_specs, out_specs=out_specs, check_vma=False)
```

```python
import functools

import jax
import jax.numpy as jnp
from jax import lax
from jax.experimental import pallas as pl
from jax.experimental.pallas import tpu as pltpu
from jax.sharding import PartitionSpec as P

HEAD_DIM = 128
NORM_EPS = 1e-6
ROPE_BASE = 1000000.0
MESH = pl.DeviceIdType.MESH
BF16 = jnp.bfloat16
F32 = jnp.float32

CW = 256
IW = 2 * CW
O2, O3, O4, O5 = 3, 8, 13, 16
E1, E2, E3, E4 = 2, 8, 6, 10
RING = 8
SB = 8
NBUF = 3
MASK = (0, 2, 1, 3)
POS = (0, 2, 1, 3)
HALVES = ((0, 2), (1, 3))


def groups(head):
    return 2 if head else 1


def dot(a, b):
    return jnp.dot(a, b, preferred_element_type=F32)


def chain_kernel(head, tail, layer, n_pref, model_dim, *refs):
    NM = groups(head)
    it = iter(refs)
    hid_in = next(it)
    if head:
        attn_in, g_mlp = next(it), next(it)
        wo_in, wg_in, wu_in, wd_in = (next(it).at[layer] for _ in range(4))
    if tail:
        tail_layer = layer + 1 if head else layer
        g_attn = next(it)
        wq_in, wk_in, wv_in, k_in, v_in = (next(it).at[tail_layer] for _ in range(5))
    if head:
        hid_out = next(it)
    if tail:
        qkv_out, pref_out = next(it), next(it)
    h_buf, n_buf, stat_buf, keep_buf, own_buf, dsend, drecv, xsend, xrecv = (next(it) for _ in range(9))
    h_sem, st_ss, st_rs, d_ss, d_rs, x_ss, x_rs = (next(it) for _ in range(7))
    if head:
        attn_all, wo_buf, wgu_buf, wd_buf, acc_buf, act_all, y_send, y_recv = (next(it) for _ in range(8))
        ag_ss, ag_rs, y_ss, y_rs, act_ss, act_rs, wo_sem, wgu_sem, wd_sem, o_sem, a_sem = (next(it) for _ in range(11))
    if tail:
        wqkv_buf, wqkv_sem, pref_sem = (next(it) for _ in range(3))

    me = lax.axis_index('x')
    yy = lax.axis_index('y')
    chip, core = lax.div(me, 2), lax.rem(me, 2)
    d1 = chip * 2 + (1 - core)
    d2 = (1 - chip) * 2 + core
    d3 = (1 - chip) * 2 + (1 - core)
    quarter = (me, d2, d1, d3)
    R = h_buf.shape[1] // 4
    M = 4 * R
    n_ffn = act_all.shape[0] // NM if head else 0
    n_mlp = n_ffn * NM
    n_qkv = 6
    ring = dsend.shape[0]
    n_items = drecv.shape[0]

    def after_ring(s, action):
        if isinstance(s, int):
            if s >= ring:
                action()
        else:
            pl.when(s >= ring)(action)

    barrier = pltpu.get_barrier_semaphore()
    for peer in ({'x': d1}, {'x': d2}, {'x': d3}, {'y': 1 - yy}):
        pl.semaphore_signal(barrier, inc=1, device_id=peer, device_id_type=MESH)

    def remote(src, dst, ss, rs, peer):
        return pltpu.make_async_remote_copy(src_ref=src, dst_ref=dst, send_sem=ss, recv_sem=rs, device_id=peer, device_id_type=MESH)

    def attn_own(m):
        return pltpu.make_async_copy(attn_in.at[pl.ds(m * R, R)], attn_all.at[m, pl.ds(0, R)], a_sem.at[m])
    if head:
        for m in range(NM):
            attn_own(m).start()

    def hid_copy(m, k):
        row = pl.multiple_of(quarter[k] * (NM * R) + m * R, R)
        return pltpu.make_async_copy(hid_in.at[pl.ds(row, R)], h_buf.at[m, pl.ds(k * R, R)], h_sem.at[m, k])

    for m in range(NM):
        for k in range(4):
            hid_copy(m, k).start()

    def wgu_copy(j):
        off = pl.multiple_of(j * CW, CW)
        return (pltpu.make_async_copy(wg_in.at[:, pl.ds(off, CW)], wgu_buf.at[j, :, pl.ds(0, CW)], wgu_sem.at[0, j]),
                pltpu.make_async_copy(wu_in.at[:, pl.ds(off, CW)], wgu_buf.at[j, :, pl.ds(CW, CW)], wgu_sem.at[1, j]))

    if head:
        wo_copy = pltpu.make_async_copy(wo_in, wo_buf, wo_sem)
        wd_copy = pltpu.make_async_copy(wd_in, wd_buf, wd_sem)
    if tail:
        wqkv_copies = [pltpu.make_async_copy(wq_in.at[:, pl.ds(j * IW, IW)], wqkv_buf.at[j], wqkv_sem.at[j]) for j in range(4)]
        wqkv_copies += [pltpu.make_async_copy(w, wqkv_buf.at[j], wqkv_sem.at[j]) for j, w in ((4, wk_in), (5, wv_in))]
    if head:
        wo_copy.start()

        def start_wgu(j, c):
            for cp in wgu_copy(j):
                cp.start()
            return c
        lax.fori_loop(0, n_ffn, start_wgu, 0)
        wd_copy.start()
    if tail:
        for cp in wqkv_copies:
            cp.start()

    def pref_copy(blk, c):
        seqs = pl.ds(blk * SB, SB)
        return pltpu.make_async_copy((k_in, v_in)[c].at[seqs], pref_out.at[blk, c], pref_sem.at[blk, c])
    if tail:
        for blk in range(n_pref):
            for c in (0, 1):
                pref_copy(blk, c).start()

    def diag():
        return lax.broadcasted_iota(jnp.int32, (R, 128), 0) == lax.broadcasted_iota(jnp.int32, (R, 128), 1)

    def stat_send(kind, m, a):
        peer = (None, d1, d2, d3)[a]
        return remote(stat_buf.at[kind, m, 0], stat_buf.at[kind, m, a], st_ss.at[kind, m, a - 1], st_rs.at[kind, m, a - 1], {'x': peer})

    def stats_start(kind, m):
        for k in range(4):
            hv = h_buf[m, pl.ds(k * R, R), :].astype(F32)
            row_sum = jnp.sum(hv * hv, axis=1, keepdims=True)
            stat_buf[kind, m, 0, pl.ds(k, 1), :] = jnp.sum(jnp.where(diag(), row_sum, 0.0), axis=0, keepdims=True)
        for a in (1, 2, 3):
            stat_send(kind, m, a).start()

    def norm(kind, m, gain):
        for a in (1, 2, 3):
            stat_send(kind, m, a).wait()
        gain_row = gain.astype(F32)
        for k in range(4):
            total = stat_buf[kind, m, 0, pl.ds(k, 1), :]
            for a in (1, 2, 3):
                total = total + stat_buf[kind, m, a, pl.ds(POS[MASK[k] ^ a], 1), :]
            col = jnp.sum(jnp.where(diag(), total, 0.0), axis=1, keepdims=True)
            hv = h_buf[m, pl.ds(k * R, R), :].astype(F32)
            n_buf[m, pl.ds(k * R, R), :] = (hv * lax.rsqrt(col / model_dim + NORM_EPS) * gain_row).astype(BF16)

    def d_copy(s):
        return remote(dsend.at[lax.rem(s, ring)], drecv.at[s], d_ss.at[s], d_rs.at[s], {'x': d1})

    def x_copy(s):
        return remote(xsend.at[lax.rem(s, ring)], xrecv.at[s], x_ss.at[s], x_rs.at[s], {'x': d2})

    def stage1_math(s, m, w):
        part = dot(n_buf[m], w)
        keep_buf[lax.rem(s, keep_buf.shape[0])] = part[:2 * R]
        dsend[lax.rem(s, ring)] = part[2 * R:].astype(BF16)

    def stage1(s, m, w):
        after_ring(s, lambda: d_copy(s - ring).wait_send())
        stage1_math(s, m, w)
        d_copy(s).start()

    def stage2_wait(s):
        d_copy(s).wait_recv()
        after_ring(s, lambda: x_copy(s - ring).wait_send())

    def stage2_math(s):
        slot = lax.rem(s, keep_buf.shape[0])
        xsend[lax.rem(s, ring)] = (keep_buf[slot, pl.ds(R, R), :] + drecv[s, pl.ds(R, R), :].astype(F32)).astype(BF16)
        own_buf[lax.rem(s, own_buf.shape[0])] = keep_buf[slot, pl.ds(0, R), :] + drecv[s, pl.ds(0, R), :].astype(F32)

    def stage2(s):
        stage2_wait(s)
        stage2_math(s)
        x_copy(s).start()

    def stage3_sum(s):
        return (own_buf[lax.rem(s, own_buf.shape[0])] + xrecv[s].astype(F32)).astype(BF16)

    def stage3(s):
        x_copy(s).wait_recv()
        return stage3_sum(s)

    def gather_copies(buf, i, ss, rs):
        own, other = buf.at[i, pl.ds(0, R)], buf.at[i, pl.ds(R, R)]
        return (lambda: remote(own, buf.at[i, pl.ds(2 * R, R)], ss.at[0, i], rs.at[0, i], {'x': d1}),
                lambda: remote(own, buf.at[i, pl.ds(R, R)], ss.at[1, i], rs.at[1, i], {'x': d2}),
                lambda: remote(other, buf.at[i, pl.ds(3 * R, R)], ss.at[2, i], rs.at[2, i], {'x': d1}))

    def attn_copies(m):
        return gather_copies(attn_all, m, ag_ss, ag_rs)

    def y_copy(kind, m, half):
        rows = pl.ds(half * 2 * R, 2 * R)
        return remote(y_send.at[kind, m, rows], y_recv.at[kind, m, rows], y_ss.at[kind, m, half], y_rs.at[kind, m, half], {'y': 1 - yy})

    def attn_half(m, half):
        rows = jnp.concatenate([attn_all[m, pl.ds(k * R, R), :] for k in HALVES[half]], axis=0)
        y_send[0, m, pl.ds(half * 2 * R, 2 * R), :] = dot(rows, wo_buf[...]).astype(BF16)
        y_copy(0, m, half).start()

    def attn_finish(m):
        for half in (0, 1):
            y_copy(0, m, half).wait()
            for i, k in enumerate(HALVES[half]):
                here, there = pl.ds(k * R, R), pl.ds((half * 2 + i) * R, R)
                total = (y_send[0, m, there, :].astype(F32) + y_recv[0, m, there, :].astype(F32)).astype(BF16)
                h_buf[m, here, :] = (h_buf[m, here, :].astype(F32) + total.astype(F32)).astype(BF16)

    def mlp_start(m):
        y_send[1, m] = acc_buf[m].astype(BF16)
        for half in (0, 1):
            y_copy(1, m, half).start()

    def mlp_finish(m):
        for half in (0, 1):
            y_copy(1, m, half).wait()
            rows = pl.ds(half * 2 * R, 2 * R)
            total = (y_send[1, m, rows, :].astype(F32) + y_recv[1, m, rows, :].astype(F32)).astype(BF16)
            h_buf[m, rows, :] = (h_buf[m, rows, :].astype(F32) + total.astype(F32)).astype(BF16)

    def act_copies(t):
        return gather_copies(act_all, t, act_ss, act_rs)

    def out_copy(m, k):
        row = pl.multiple_of(quarter[k] * (NM * R) + m * R, R)
        return pltpu.make_async_copy(h_buf.at[m, pl.ds(k * R, R)], hid_out.at[pl.ds(row, R)], o_sem.at[m, k])

    def mid_ready(m):
        attn_finish(m)
        stats_start(0, m)

    def layer_done(m):
        mlp_finish(m)
        if tail:
            stats_start(1, m)
        for k in range(4):
            out_copy(m, k).start()

    def split(t):
        return (0, t) if NM == 1 else (lax.div(t, n_ffn), lax.rem(t, n_ffn))

    def mlp_iter(t, steady):
        def stage(first, action):
            if steady:
                action()
            else:
                pl.when((t >= first) & (t < n_mlp + first))(action)

        def relay_on():
            _, to_chip, relay = act_copies(t - O4)
            to_chip().wait_recv()
            relay().start()

        def act_ready():
            to_core, _, relay = act_copies(t - O5)
            to_core().wait_recv()
            relay().wait_recv()

        @pl.when(t < n_ffn)
        def _():
            for cp in wgu_copy(t):
                cp.wait()
        stage(O4, relay_on)
        stage(O2, lambda: stage2_wait(t - O2))
        stage(O3, lambda: x_copy(t - O3).wait_recv())
        stage(O5, act_ready)
        stage(0, lambda: after_ring(t, lambda: d_copy(t - ring).wait_send()))

        def activate():
            s = t - O3
            full = stage3_sum(s)
            gate, up = full[:, :CW].astype(F32), full[:, CW:].astype(F32)
            act_all[s, pl.ds(0, R), :] = (jax.nn.silu(gate) * up).astype(BF16)

        def product():
            m, j = split(t)
            stage1_math(t, m, wgu_buf[j])

        def down():
            s = t - O5
            m, j = split(s)
            acc_buf[m] += dot(act_all[s], wd_buf[pl.ds(pl.multiple_of(j * CW, CW), CW), :])

        def send_act():
            to_core, to_chip, _ = act_copies(t - O3)
            to_chip().start()
            to_core().start()

        stage(O2, lambda: stage2_math(t - O2))
        stage(O3, activate)
        stage(0, product)
        stage(O5, down)
        stage(O2, lambda: x_copy(t - O2).start())
        stage(O3, send_act)
        stage(0, lambda: d_copy(t).start())

    pl.semaphore_wait(barrier, 4)

    if head:
        for m in range(NM):
            attn_own(m).wait()
            to_core, to_chip, _ = attn_copies(m)
            to_chip().start()
            to_core().start()
            acc_buf[m] = jnp.zeros(acc_buf.shape[1:], F32)
        for m in range(NM):
            for k in range(4):
                hid_copy(m, k).wait()
        wo_copy.wait()
        for m in range(NM):
            attn_copies(m)[0]().wait_recv()
            attn_half(m, 0)
        for m in range(NM):
            _, to_chip, relay = attn_copies(m)
            to_chip().wait_recv()
            relay().start()
            relay().wait_recv()
            attn_half(m, 1)
        mid_ready(0)
        norm(0, 0, g_mlp[pl.ds(layer, 1), :])
        events = {}
        if NM == 2:
            first_done = n_ffn - 1 + O5
            events = {E1: lambda: mid_ready(1), E2: lambda: norm(0, 1, g_mlp[pl.ds(layer, 1), :]),
                      first_done: lambda: mlp_start(0), first_done + E3: lambda: layer_done(0)}
            if tail:
                events[first_done + E4] = lambda: norm(1, 0, g_attn[pl.ds(tail_layer, 1), :])

        def body(steady, t, c):
            mlp_iter(t, steady)
            for at, event in events.items():
                pl.when(t == at)(event)
            return c
        lax.fori_loop(0, O5, functools.partial(body, False), 0)
        wd_copy.wait()
        lax.fori_loop(O5, n_mlp, functools.partial(body, True), 0)
        lax.fori_loop(n_mlp, n_mlp + O5, functools.partial(body, False), 0)
        mlp_start(NM - 1)
        if not (tail and NM == 2):
            layer_done(NM - 1)
    else:
        for m in range(NM):
            for k in range(4):
                hid_copy(m, k).wait()
            stats_start(1, m)

    if tail:
        for cp in wqkv_copies:
            cp.wait()
        n_all = n_qkv * NM
        if not (head and NM == 2):
            for m in range(NM):
                norm(1, m, g_attn[pl.ds(tail_layer, 1), :])
        for t in range(n_all + 3):
            if 1 <= t < n_all + 1:
                stage2(n_mlp + t - 1)
            if head and NM == 2 and t == n_qkv:
                layer_done(1)
                norm(1, 1, g_attn[pl.ds(tail_layer, 1), :])
            if t < n_all:
                stage1(n_mlp + t, t // n_qkv, wqkv_buf[t % n_qkv])
            if t >= 3:
                m, j = divmod(t - 3, n_qkv)
                qkv_out[j, pl.ds(m * R, R), :] = stage3(n_mlp + t - 3)

    if tail:
        for blk in range(n_pref):
            for c in (0, 1):
                pref_copy(blk, c).wait()

    def drain(s, c):
        d_copy(s).wait_send()
        x_copy(s).wait_send()
        return c
    lax.fori_loop(max(n_items - ring, 0), n_items, drain, 0)
    if head:
        def drain_act(s, c):
            for cp in act_copies(s):
                cp().wait_send()
            return c
        lax.fori_loop(0, n_mlp, drain_act, 0)
        for m in range(NM):
            for cp in attn_copies(m):
                cp().wait_send()
            for k in range(4):
                out_copy(m, k).wait()


def chain_call(head, tail, layer, cid, n_pref, vmem_mib, model_dim, hidden, attn=None, g_mlp=None, wo=None, wg=None, wu=None, wd=None, g_attn=None, wq=None, wk=None, wv=None, k_rows=None, v_rows=None):
    batch, feat = hidden.shape
    NM = groups(head)
    M = batch // NM
    R = M // 4
    vmem = pl.BlockSpec(memory_space=pltpu.VMEM)
    hbm = pl.BlockSpec(memory_space=pltpu.HBM)
    args, in_specs = [hidden], [hbm]
    out_shape, out_specs = [], []
    n_items = 0
    if head:
        args += [attn, g_mlp, wo, wg, wu, wd]
        in_specs += [hbm, vmem, hbm, hbm, hbm, hbm]
        out_shape.append(jax.ShapeDtypeStruct(hidden.shape, hidden.dtype))
        out_specs.append(hbm)
        n_ffn = wg.shape[2] // CW
        n_items += n_ffn * NM
    if tail:
        args += [g_attn, wq, wk, wv, k_rows, v_rows]
        in_specs += [vmem] + [hbm] * 5
        out_shape.append(jax.ShapeDtypeStruct((6, batch // 4, IW), BF16))
        out_specs.append(vmem)
        out_shape.append(pltpu.VMEM((n_pref, 2, SB) + k_rows.shape[2:], BF16))
        out_specs.append(vmem)
        n_items += 6 * NM
    dma = pltpu.SemaphoreType.DMA
    scratch = [
        pltpu.VMEM((NM, M, feat), BF16), pltpu.VMEM((NM, M, feat), BF16), pltpu.VMEM((2, NM, 4, 8, 128), F32),
        pltpu.VMEM((O2 + 1, 2 * R, IW), F32), pltpu.VMEM((O3 - O2 + 1, R, IW), F32),
        pltpu.VMEM((RING, 2 * R, IW), BF16), pltpu.VMEM((n_items, 2 * R, IW), BF16),
        pltpu.VMEM((RING, R, IW), BF16), pltpu.VMEM((n_items, R, IW), BF16),
        dma((NM, 4)), dma((2, NM, 3)), dma((2, NM, 3)), dma((n_items,)), dma((n_items,)), dma((n_items,)), dma((n_items,))]
    if head:
        scratch += [
            pltpu.VMEM((NM, M, attn.shape[1]), BF16), pltpu.VMEM(wo.shape[1:], BF16), pltpu.VMEM((n_ffn, feat, IW), BF16),
            pltpu.VMEM(wd.shape[1:], BF16), pltpu.VMEM((NM, M, feat), F32), pltpu.VMEM((n_ffn * NM, M, CW), BF16),
            pltpu.VMEM((2, NM, M, feat), BF16), pltpu.VMEM((2, NM, M, feat), BF16),
            dma((3, NM)), dma((3, NM)), dma((2, NM, 2)), dma((2, NM, 2)), dma((3, n_ffn * NM)), dma((3, n_ffn * NM)),
            dma, dma((2, n_ffn)), dma, dma((NM, 4)), dma((NM,))]
    if tail:
        scratch += [pltpu.VMEM((6, feat, IW), BF16), dma((6,)), dma((n_pref, 2))]
    return pl.pallas_call(
        functools.partial(chain_kernel, head, tail, layer, n_pref, model_dim),
        out_shape=out_shape, in_specs=in_specs, out_specs=out_specs, scratch_shapes=scratch,
        name=f'chain_{int(head)}{int(tail)}',
        compiler_params=pltpu.CompilerParams(collective_id=cid, has_side_effects=True, vmem_limit_bytes=vmem_mib * 1024 * 1024),
    )(*args)


def attn_kernel(layer, n_pref, pos_ref, qkv_hbm, tabs_hbm, k_hbm, v_hbm, *refs):
    k_out, v_out, o_ref, pref, kv_slots, q_buf, kv_buf, o_buf, s_buf, p_buf, qkv_ref, tabs_ref, in_sem, out_sem, small_sem = refs[-15:]
    small = (pltpu.make_async_copy(qkv_hbm, qkv_ref, small_sem.at[0]), pltpu.make_async_copy(tabs_hbm, tabs_ref, small_sem.at[1]))
    for cp in small:
        cp.start()
    local = o_ref.shape[0]
    n_q = q_buf.shape[0] // local
    n_kv = kv_buf.shape[1] // local
    n_rows = k_hbm.shape[2]
    group = n_q // n_kv
    per_chunk = qkv_ref.shape[2] // HEAD_DIM
    n_blocks = local // SB

    def held(blk, early):
        return pref.at[blk] if early else kv_slots.at[lax.rem(blk - n_pref, NBUF)]

    def run(blk, early, out, wait):
        seqs = pl.ds(blk * SB, SB)
        for c in (0, 1):
            here = held(blk, early).at[c]
            if out:
                cp = pltpu.make_async_copy(here, (k_out, v_out)[c].at[layer, seqs], out_sem.at[blk, c])
            else:
                cp = pltpu.make_async_copy((k_hbm, v_hbm)[c].at[layer, seqs], here, in_sem.at[blk, c])
            cp.wait() if wait else cp.start()

    for blk in range(n_pref, min(n_pref + NBUF, n_blocks)):
        run(blk, False, False, False)

    def head_of(idx):
        return qkv_ref[idx // per_chunk, :, pl.ds((idx % per_chunk) * HEAD_DIM, HEAD_DIM)].astype(F32)

    for cp in small:
        cp.wait()
    cos_tab, sin_tab = tabs_ref[pl.ds(0, local), :], tabs_ref[pl.ds(local, local), :]
    gains = [tabs_ref[pl.ds(2 * local + 2 * layer + i, 1), :] for i in (0, 1)]

    def norm_rope(vals, gain):
        normed = vals * lax.rsqrt(jnp.mean(vals * vals, axis=-1, keepdims=True) + NORM_EPS) * gain
        return (normed * cos_tab + pltpu.roll(normed, HEAD_DIM // 2, 1) * sin_tab).astype(BF16).astype(F32)
    for h in range(n_q):
        q_buf[pl.ds(h * local, local), :] = norm_rope(head_of(h), gains[0])
    for h in range(n_kv):
        kv_buf[0, pl.ds(h * local, local), :] = norm_rope(head_of(n_q + h), gains[1])
        kv_buf[1, pl.ds(h * local, local), :] = head_of(n_q + n_kv + h)

    row_ids = lax.broadcasted_iota(jnp.int32, (16, HEAD_DIM), 0)
    lane_ids = lax.broadcasted_iota(jnp.int32, (n_q, n_rows), 1)
    head_hit = lax.rem(lane_ids, n_kv) == lax.div(lax.broadcasted_iota(jnp.int32, (n_q, n_rows), 0), group)
    lane_of = jnp.where(head_hit, lane_ids, n_rows)

    def block_step(blk, early):
        ref = held(blk, early)
        if not early:
            run(blk, False, False, True)
        for i in range(SB):
            b = blk * SB + i
            row = pos_ref[b] * n_kv
            base = pl.multiple_of(lax.div(row, 16) * 16, 16)
            hit = lax.div(row_ids, n_kv) == lax.div(row - base, n_kv)
            for c in (0, 1):
                new = kv_buf[c, pl.ds(b, n_kv, stride=local), :]
                new = jnp.concatenate([new] * (16 // n_kv), axis=0)
                old = ref[c, i, pl.ds(base, 16), :]
                ref[c, i, pl.ds(base, 16), :] = jnp.where(hit, new, old.astype(F32)).astype(BF16)
        for i in range(SB):
            q = q_buf[pl.ds(blk * SB + i, n_q, stride=local), :].astype(BF16)
            s_buf[i] = lax.dot_general(q, ref[0, i], (((1,), (1,)), ((), ())), preferred_element_type=F32)
        run(blk, early, True, False)
        for i in range(SB):
            row = pos_ref[blk * SB + i] * n_kv
            scores = jnp.where(lane_of < row + n_kv, s_buf[i] * (HEAD_DIM ** -0.5), -1e30)
            e = jnp.exp(scores - jnp.max(scores, axis=-1, keepdims=True))
            p_buf[i] = (e / jnp.sum(e, axis=-1, keepdims=True)).astype(BF16)
        for i in range(SB):
            o_buf[pl.ds(blk * SB + i, n_q, stride=local), :] = dot(p_buf[i], ref[1, i])

    def early_step(blk, carry):
        block_step(blk, True)
        return carry

    def late_step(blk, carry):
        block_step(blk, False)

        @pl.when((blk > n_pref) & (blk - 1 + NBUF < n_blocks))
        def _():
            run(blk - 1, False, True, True)
            run(blk - 1 + NBUF, False, False, False)
        return carry
    lax.fori_loop(0, n_pref, early_step, 0)
    if n_pref < n_blocks:
        lax.fori_loop(n_pref, n_blocks, late_step, 0)

    for h in range(n_q):
        o_ref[:, pl.ds(h * HEAD_DIM, HEAD_DIM)] = o_buf[pl.ds(h * local, local), :].astype(BF16)
    for blk in range(n_pref):
        run(blk, True, True, True)
    for blk in range(max(n_blocks - NBUF, n_pref), n_blocks):
        run(blk, False, True, True)


def attn_call(layer, pos, qkv, tabs, k_cache, v_cache, pref, prev):
    layers, local, n_rows, _ = k_cache.shape
    n_kv = 4
    n_q = 16
    smem = pl.BlockSpec(memory_space=pltpu.SMEM)
    vmem = pl.BlockSpec(memory_space=pltpu.VMEM)
    hbm = pl.BlockSpec(memory_space=pltpu.HBM)
    args = [pos, qkv, tabs, k_cache, v_cache, pref]
    in_specs = [smem, hbm, hbm, hbm, hbm, vmem]
    aliases = {5: 3}
    n_pref, n_blocks = pref.shape[0], local // SB
    if prev is not None:
        args += list(prev)
        in_specs += [hbm] * 2
        aliases.update({6: 0, 7: 1})
    return pl.pallas_call(
        functools.partial(attn_kernel, layer, n_pref),
        out_shape=[jax.ShapeDtypeStruct(k_cache.shape, BF16)] * 2 + [jax.ShapeDtypeStruct((local, n_q * HEAD_DIM), BF16), jax.ShapeDtypeStruct(pref.shape, BF16)],
        in_specs=in_specs,
        out_specs=[hbm, hbm, vmem, vmem],
        scratch_shapes=[pltpu.VMEM((min(NBUF, max(n_blocks - n_pref, 1)) if n_pref < n_blocks else 1, 2, SB if n_pref < n_blocks else 1, n_rows, HEAD_DIM), BF16),
                        pltpu.VMEM((n_q * local, HEAD_DIM), F32), pltpu.VMEM((2, n_kv * local, HEAD_DIM), F32), pltpu.VMEM((n_q * local, HEAD_DIM), F32),
                        pltpu.VMEM((SB, n_q, n_rows), F32), pltpu.VMEM((SB, n_q, n_rows), BF16),
                        pltpu.VMEM(qkv.shape, BF16), pltpu.VMEM(tabs.shape, F32),
                        pltpu.SemaphoreType.DMA((n_blocks, 2)), pltpu.SemaphoreType.DMA((n_blocks, 2)), pltpu.SemaphoreType.DMA((2,))],
        input_output_aliases=aliases, name=f'attn_{layer}',
        compiler_params=pltpu.CompilerParams(vmem_limit_bytes=(20 if n_pref == n_blocks else 22) * 1024 * 1024),
    )(*args)


def solution(mesh):
    group_size = mesh.shape['x']
    cache_spec = P(None, ('dp', 'x'), None, 'y', None)
    col_spec = P(None, 'x', 'y')
    row_spec = P(None, 'y', 'x')
    in_specs = (P('dp', 'x'), P('dp'), cache_spec, cache_spec, P(None, 'x'), P(None, 'x'), P(), P(), col_spec, col_spec, col_spec, row_spec, col_spec, col_spec, row_spec)
    out_specs = (P('dp', 'x'), cache_spec, cache_spec)

    def device_step(hidden, positions, k_cache, v_cache, g_attn, g_mlp, q_gain, k_gain, w_q, w_k, w_v, w_o, w_gate, w_up, w_down):
        model_dim = hidden.shape[1] * group_size
        layers, local, cache_len, n_kv, _ = k_cache.shape
        my_pos = lax.dynamic_slice_in_dim(positions, lax.axis_index('x') * local, local)
        half = HEAD_DIM // 2
        inv_freq = jnp.power(ROPE_BASE, -2.0 * jnp.arange(half, dtype=F32) / HEAD_DIM)
        angles = my_pos.astype(F32)[:, None] * inv_freq[None, :]
        cos_half, sin_half = jnp.cos(angles), jnp.sin(angles)
        gains = jnp.stack([q_gain[0], k_gain[0], q_gain[1], k_gain[1]]).astype(F32)
        tabs = jnp.concatenate([jnp.concatenate([cos_half, cos_half], axis=1), jnp.concatenate([-sin_half, sin_half], axis=1), gains, jnp.zeros((4, HEAD_DIM), F32)])
        tabs, my_pos, hidden = lax.optimization_barrier((tabs, my_pos, hidden))
        k_rows = k_cache.reshape(layers, local, cache_len * n_kv, HEAD_DIM)
        v_rows = v_cache.reshape(layers, local, cache_len * n_kv, HEAD_DIM)
        attn_tabs = (tabs, k_rows, v_rows)
        caches = {'k_rows': k_rows, 'v_rows': v_rows}
        qkv, pref = chain_call(False, True, 0, 0, 8, 16, model_dim, hidden, g_attn=g_attn, wq=w_q, wk=w_k, wv=w_v, **caches)
        k_new, v_new, attn, _ = attn_call(0, my_pos, qkv, *attn_tabs, pref, None)
        hidden, qkv, pref = chain_call(True, True, 0, 1, 5, 40, model_dim, hidden, attn, g_mlp, w_o, w_gate, w_up, w_down, g_attn, w_q, w_k, w_v, **caches)
        k_new, v_new, attn, _ = attn_call(1, my_pos, qkv, *attn_tabs, pref, (k_new, v_new))
        (hidden,) = chain_call(True, False, 1, 2, 0, 60, model_dim, hidden, attn, g_mlp, w_o, w_gate, w_up, w_down)
        return hidden, k_new.reshape(k_cache.shape), v_new.reshape(v_cache.shape)

    return jax.shard_map(device_step, mesh=mesh, in_specs=in_specs, out_specs=out_specs, check_vma=False)
```

```python
import functools

import jax
import jax.numpy as jnp
from jax import lax
from jax.experimental import pallas as pl
from jax.experimental.pallas import tpu as pltpu
from jax.sharding import PartitionSpec as P

HEAD_DIM = 128
NORM_EPS = 1e-6
ROPE_BASE = 1000000.0
MESH = pl.DeviceIdType.MESH
BF16 = jnp.bfloat16
F32 = jnp.float32

CW = 256
IW = 2 * CW
O2, O3, O4, O5 = 3, 8, 13, 16
E1, E2, E3, E4 = 2, 8, 6, 10
HEAD_GROUPS = 2
RING = 8
SB = 8
AHEAD = 2
NBUF = 3
MASK = (0, 2, 1, 3)
POS = (0, 2, 1, 3)
HALVES = ((0, 2), (1, 3))


def in_hbm(x):
    return pltpu.with_memory_space_constraint(x, pltpu.HBM)


def groups(head):
    return HEAD_GROUPS if head else 1


def dot(a, b):
    return jnp.dot(a, b, preferred_element_type=F32)


def chain_kernel(head, tail, layer, n_pref, model_dim, *refs):
    NM = groups(head)
    it = iter(refs)
    hid_in = next(it)
    if head:
        attn_in, g_mlp_in = next(it), next(it)
        wo_in, wg_in, wu_in, wd_in = (next(it).at[layer] for _ in range(4))
    if tail:
        tail_layer = layer + 1 if head else layer
        g_attn_in = next(it)
        wq_in, wk_in, wv_in, k_in, v_in = (next(it).at[tail_layer] for _ in range(5))
    if head:
        hid_out = next(it)
    if tail:
        qkv_out, pref_out = next(it), next(it)
    h_buf, n_buf, stat_buf, keep_buf, own_buf, dsend, drecv, xsend, xrecv = (next(it) for _ in range(9))
    gain_buf, gain_sem = next(it), next(it)
    h_sem, st_ss, st_rs, d_ss, d_rs, x_ss, x_rs = (next(it) for _ in range(7))
    if head:
        attn_all, wo_buf, wgu_buf, wd_buf, acc_buf, act_all, y_send, y_recv = (next(it) for _ in range(8))
        ag_ss, ag_rs, y_ss, y_rs, act_ss, act_rs, wo_sem, wgu_sem, wd_sem, o_sem, a_sem = (next(it) for _ in range(11))
    if tail:
        wqkv_buf, wqkv_sem, pref_sem = (next(it) for _ in range(3))

    me = lax.axis_index('x')
    yy = lax.axis_index('y')
    chip, core = lax.div(me, 2), lax.rem(me, 2)
    d1 = chip * 2 + (1 - core)
    d2 = (1 - chip) * 2 + core
    d3 = (1 - chip) * 2 + (1 - core)
    quarter = (me, d2, d1, d3)
    R = h_buf.shape[1] // 4
    M = 4 * R
    n_ffn = act_all.shape[0] // NM if head else 0
    n_mlp = n_ffn * NM
    n_qkv = 6
    ring = dsend.shape[0]
    n_items = drecv.shape[0]

    def after_ring(s, action):
        if isinstance(s, int):
            if s >= ring:
                action()
        else:
            pl.when(s >= ring)(action)

    barrier = pltpu.get_barrier_semaphore()
    for peer in ({'x': d1}, {'x': d2}, {'x': d3}, {'y': 1 - yy}):
        pl.semaphore_signal(barrier, inc=1, device_id=peer, device_id_type=MESH)

    def remote(src, dst, ss, rs, peer):
        return pltpu.make_async_remote_copy(src_ref=src, dst_ref=dst, send_sem=ss, recv_sem=rs, device_id=peer, device_id_type=MESH)

    def attn_own(m):
        return pltpu.make_async_copy(attn_in.at[pl.ds(m * R, R)], attn_all.at[m, pl.ds(0, R)], a_sem.at[m])
    if head:
        for m in range(NM):
            attn_own(m).start()

    def hid_copy(m, k):
        row = pl.multiple_of(quarter[k] * (NM * R) + m * R, R)
        return pltpu.make_async_copy(hid_in.at[pl.ds(row, R)], h_buf.at[m, pl.ds(k * R, R)], h_sem.at[m, k])

    for m in range(NM):
        for k in range(4):
            hid_copy(m, k).start()
    gain_copies = []
    if head:
        gain_copies.append(pltpu.make_async_copy(g_mlp_in, gain_buf.at[0], gain_sem.at[0]))
    if tail:
        gain_copies.append(pltpu.make_async_copy(g_attn_in, gain_buf.at[1], gain_sem.at[1]))
    for cp in gain_copies:
        cp.start()

    def wgu_copy(j):
        off = pl.multiple_of(j * CW, CW)
        return (pltpu.make_async_copy(wg_in.at[:, pl.ds(off, CW)], wgu_buf.at[j, :, pl.ds(0, CW)], wgu_sem.at[0, j]),
                pltpu.make_async_copy(wu_in.at[:, pl.ds(off, CW)], wgu_buf.at[j, :, pl.ds(CW, CW)], wgu_sem.at[1, j]))

    if head:
        wo_copy = pltpu.make_async_copy(wo_in, wo_buf, wo_sem)
        wd_copy = pltpu.make_async_copy(wd_in, wd_buf, wd_sem)
    if tail:
        wqkv_copies = [pltpu.make_async_copy(wq_in.at[:, pl.ds(j * IW, IW)], wqkv_buf.at[j], wqkv_sem.at[j]) for j in range(4)]
        wqkv_copies += [pltpu.make_async_copy(w, wqkv_buf.at[j], wqkv_sem.at[j]) for j, w in ((4, wk_in), (5, wv_in))]
    def start_wgu(j, c):
        for cp in wgu_copy(j):
            cp.start()
        return c
    if head:
        wo_copy.start()
    else:
        for cp in wqkv_copies:
            cp.start()

    def pref_copy(blk, c):
        seqs = pl.ds(blk * SB, SB)
        return pltpu.make_async_copy((k_in, v_in)[c].at[seqs], pref_out.at[blk, c], pref_sem.at[blk, c])
    def pref_start():
        for blk in range(n_pref):
            for c in (0, 1):
                pref_copy(blk, c).start()

    def diag():
        return lax.broadcasted_iota(jnp.int32, (R, 128), 0) == lax.broadcasted_iota(jnp.int32, (R, 128), 1)

    def stat_send(kind, m, a):
        peer = (None, d1, d2, d3)[a]
        return remote(stat_buf.at[kind, m, 0], stat_buf.at[kind, m, a], st_ss.at[kind, m, a - 1], st_rs.at[kind, m, a - 1], {'x': peer})

    def stats_start(kind, m):
        for k in range(4):
            hv = h_buf[m, pl.ds(k * R, R), :].astype(F32)
            row_sum = jnp.sum(hv * hv, axis=1, keepdims=True)
            stat_buf[kind, m, 0, pl.ds(k, 1), :] = jnp.sum(jnp.where(diag(), row_sum, 0.0), axis=0, keepdims=True)
        for a in (1, 2, 3):
            stat_send(kind, m, a).start()

    def norm(kind, m, gain):
        for a in (1, 2, 3):
            stat_send(kind, m, a).wait()
        gain_row = gain.astype(F32)
        for k in range(4):
            total = stat_buf[kind, m, 0, pl.ds(k, 1), :]
            for a in (1, 2, 3):
                total = total + stat_buf[kind, m, a, pl.ds(POS[MASK[k] ^ a], 1), :]
            col = jnp.sum(jnp.where(diag(), total, 0.0), axis=1, keepdims=True)
            hv = h_buf[m, pl.ds(k * R, R), :].astype(F32)
            n_buf[m, pl.ds(k * R, R), :] = (hv * lax.rsqrt(col / model_dim + NORM_EPS) * gain_row).astype(BF16)

    def d_copy(s):
        return remote(dsend.at[lax.rem(s, ring)], drecv.at[s], d_ss.at[s], d_rs.at[s], {'x': d1})

    def x_copy(s):
        return remote(xsend.at[lax.rem(s, ring)], xrecv.at[s], x_ss.at[s], x_rs.at[s], {'x': d2})

    def stage1_math(s, m, w):
        part = dot(n_buf[m], w)
        keep_buf[lax.rem(s, keep_buf.shape[0])] = part[:2 * R]
        dsend[lax.rem(s, ring)] = part[2 * R:].astype(BF16)

    def stage1(s, m, w):
        after_ring(s, lambda: d_copy(s - ring).wait_send())
        stage1_math(s, m, w)
        d_copy(s).start()

    def stage2_wait(s):
        d_copy(s).wait_recv()
        after_ring(s, lambda: x_copy(s - ring).wait_send())

    def stage2_math(s):
        slot = lax.rem(s, keep_buf.shape[0])
        xsend[lax.rem(s, ring)] = (keep_buf[slot, pl.ds(R, R), :] + drecv[s, pl.ds(R, R), :].astype(F32)).astype(BF16)
        own_buf[lax.rem(s, own_buf.shape[0])] = keep_buf[slot, pl.ds(0, R), :] + drecv[s, pl.ds(0, R), :].astype(F32)

    def stage2(s):
        stage2_wait(s)
        stage2_math(s)
        x_copy(s).start()

    def stage3_sum(s):
        return (own_buf[lax.rem(s, own_buf.shape[0])] + xrecv[s].astype(F32)).astype(BF16)

    def stage3(s):
        x_copy(s).wait_recv()
        return stage3_sum(s)

    def gather_copies(buf, i, ss, rs):
        own, other = buf.at[i, pl.ds(0, R)], buf.at[i, pl.ds(R, R)]
        return (lambda: remote(own, buf.at[i, pl.ds(2 * R, R)], ss.at[0, i], rs.at[0, i], {'x': d1}),
                lambda: remote(own, buf.at[i, pl.ds(R, R)], ss.at[1, i], rs.at[1, i], {'x': d2}),
                lambda: remote(other, buf.at[i, pl.ds(3 * R, R)], ss.at[2, i], rs.at[2, i], {'x': d1}))

    def attn_copies(m):
        return gather_copies(attn_all, m, ag_ss, ag_rs)

    def y_copy(kind, m, half):
        rows = pl.ds(half * 2 * R, 2 * R)
        return remote(y_send.at[kind, m, rows], y_recv.at[kind, m, rows], y_ss.at[kind, m, half], y_rs.at[kind, m, half], {'y': 1 - yy})

    def attn_half(m, half):
        rows = jnp.concatenate([attn_all[m, pl.ds(k * R, R), :] for k in HALVES[half]], axis=0)
        y_send[0, m, pl.ds(half * 2 * R, 2 * R), :] = dot(rows, wo_buf[...]).astype(BF16)
        y_copy(0, m, half).start()

    def attn_finish(m):
        for half in (0, 1):
            y_copy(0, m, half).wait()
            for i, k in enumerate(HALVES[half]):
                here, there = pl.ds(k * R, R), pl.ds((half * 2 + i) * R, R)
                total = (y_send[0, m, there, :].astype(F32) + y_recv[0, m, there, :].astype(F32)).astype(BF16)
                h_buf[m, here, :] = (h_buf[m, here, :].astype(F32) + total.astype(F32)).astype(BF16)

    def mlp_start(m):
        y_send[1, m] = acc_buf[m].astype(BF16)
        for half in (0, 1):
            y_copy(1, m, half).start()

    def mlp_finish(m):
        for half in (0, 1):
            y_copy(1, m, half).wait()
            rows = pl.ds(half * 2 * R, 2 * R)
            total = (y_send[1, m, rows, :].astype(F32) + y_recv[1, m, rows, :].astype(F32)).astype(BF16)
            h_buf[m, rows, :] = (h_buf[m, rows, :].astype(F32) + total.astype(F32)).astype(BF16)

    def act_copies(t):
        return gather_copies(act_all, t, act_ss, act_rs)

    def out_copy(m, k):
        row = pl.multiple_of(quarter[k] * (NM * R) + m * R, R)
        return pltpu.make_async_copy(h_buf.at[m, pl.ds(k * R, R)], hid_out.at[pl.ds(row, R)], o_sem.at[m, k])

    def mid_ready(m):
        attn_finish(m)
        stats_start(0, m)

    def layer_done(m):
        mlp_finish(m)
        if tail:
            stats_start(1, m)
        for k in range(4):
            out_copy(m, k).start()

    def split(t):
        return (0, t) if NM == 1 else (lax.div(t, n_ffn), lax.rem(t, n_ffn))

    def mlp_iter(t, steady):
        def stage(first, action):
            if steady:
                action()
            else:
                pl.when((t >= first) & (t < n_mlp + first))(action)

        def relay_on():
            _, to_chip, relay = act_copies(t - O4)
            to_chip().wait_recv()
            relay().start()

        def act_ready():
            to_core, _, relay = act_copies(t - O5)
            to_core().wait_recv()
            relay().wait_recv()

        @pl.when(t < n_ffn)
        def _():
            for cp in wgu_copy(t):
                cp.wait()
        stage(O4, relay_on)
        stage(O2, lambda: stage2_wait(t - O2))
        stage(O3, lambda: x_copy(t - O3).wait_recv())
        stage(O5, act_ready)
        stage(0, lambda: after_ring(t, lambda: d_copy(t - ring).wait_send()))

        def activate():
            s = t - O3
            full = stage3_sum(s)
            gate, up = full[:, :CW].astype(F32), full[:, CW:].astype(F32)
            act_all[s, pl.ds(0, R), :] = (jax.nn.silu(gate) * up).astype(BF16)

        def product():
            m, j = split(t)
            stage1_math(t, m, wgu_buf[j])

        def down():
            s = t - O5
            m, j = split(s)
            acc_buf[m] += dot(act_all[s], wd_buf[pl.ds(pl.multiple_of(j * CW, CW), CW), :])

        def send_act():
            to_core, to_chip, _ = act_copies(t - O3)
            to_chip().start()
            to_core().start()

        stage(O2, lambda: stage2_math(t - O2))
        stage(O3, activate)
        stage(0, product)
        stage(O5, down)
        stage(O2, lambda: x_copy(t - O2).start())
        stage(O3, send_act)
        stage(0, lambda: d_copy(t).start())

    pl.semaphore_wait(barrier, 4)
    for cp in gain_copies:
        cp.wait()

    if head:
        for m in range(NM):
            attn_own(m).wait()
            to_core, to_chip, _ = attn_copies(m)
            to_chip().start()
            to_core().start()
            acc_buf[m] = jnp.zeros(acc_buf.shape[1:], F32)
        for m in range(NM):
            for k in range(4):
                hid_copy(m, k).wait()
        wo_copy.wait()
        lax.fori_loop(0, n_ffn, start_wgu, 0)
        wd_copy.start()
        if tail:
            for cp in wqkv_copies:
                cp.start()
        for m in range(NM):
            attn_copies(m)[0]().wait_recv()
            attn_half(m, 0)
        for m in range(NM):
            _, to_chip, relay = attn_copies(m)
            to_chip().wait_recv()
            relay().start()
            relay().wait_recv()
            attn_half(m, 1)
        mid_ready(0)
        norm(0, 0, gain_buf[0, pl.ds(layer, 1), :])
        if tail:
            pref_start()
        events = {}

        def at(t, action, *operands):
            events.setdefault(t, []).append(functools.partial(action, *operands))
        for m in range(1, NM):
            at((m - 1) * n_ffn + E1, mid_ready, m)
            at((m - 1) * n_ffn + E2, lambda m: norm(0, m, gain_buf[0, pl.ds(layer, 1), :]), m)
        for m in range(NM - 1):
            done = (m + 1) * n_ffn - 1 + O5
            at(done, mlp_start, m)
            at(min(done + E3, n_mlp + O5 - 2), layer_done, m)
            if tail:
                at(min(done + E4, n_mlp + O5 - 1), lambda m: norm(1, m, gain_buf[1, pl.ds(tail_layer, 1), :]), m)

        def body(steady, t, c):
            mlp_iter(t, steady)
            for when, actions in events.items():
                @pl.when(t == when)
                def _(actions=actions):
                    for action in actions:
                        action()
            return c
        lax.fori_loop(0, O5, functools.partial(body, False), 0)
        wd_copy.wait()
        lax.fori_loop(O5, n_mlp, functools.partial(body, True), 0)
        lax.fori_loop(n_mlp, n_mlp + O5, functools.partial(body, False), 0)
        mlp_start(NM - 1)
        if not tail:
            layer_done(NM - 1)
    else:
        for m in range(NM):
            for k in range(4):
                hid_copy(m, k).wait()
            stats_start(1, m)

    if tail:
        for cp in wqkv_copies:
            cp.wait()
        if not head:
            pref_start()
        n_all = n_qkv * NM
        if not head:
            for m in range(NM):
                norm(1, m, gain_buf[1, pl.ds(tail_layer, 1), :])
        for t in range(n_all + 3):
            if 1 <= t < n_all + 1:
                stage2(n_mlp + t - 1)
            if head and t == n_qkv * (NM - 1):
                layer_done(NM - 1)
                norm(1, NM - 1, gain_buf[1, pl.ds(tail_layer, 1), :])
            if t < n_all:
                stage1(n_mlp + t, t // n_qkv, wqkv_buf[t % n_qkv])
            if t >= 3:
                m, j = divmod(t - 3, n_qkv)
                qkv_out[j, pl.ds(m * R, R), :] = stage3(n_mlp + t - 3)

    if tail:
        for blk in range(n_pref):
            for c in (0, 1):
                pref_copy(blk, c).wait()

    def drain(s, c):
        d_copy(s).wait_send()
        x_copy(s).wait_send()
        return c
    lax.fori_loop(max(n_items - ring, 0), n_items, drain, 0)
    if head:
        def drain_act(s, c):
            for cp in act_copies(s):
                cp().wait_send()
            return c
        lax.fori_loop(0, n_mlp, drain_act, 0)
        for m in range(NM):
            for cp in attn_copies(m):
                cp().wait_send()
            for k in range(4):
                out_copy(m, k).wait()


def chain_call(head, tail, layer, cid, n_pref, vmem_mib, model_dim, hidden, attn=None, g_mlp=None, wo=None, wg=None, wu=None, wd=None, g_attn=None, wq=None, wk=None, wv=None, k_rows=None, v_rows=None):
    batch, feat = hidden.shape
    NM = groups(head)
    M = batch // NM
    R = M // 4
    vmem = pl.BlockSpec(memory_space=pltpu.VMEM)
    hbm = pl.BlockSpec(memory_space=pltpu.HBM)
    args, in_specs = [in_hbm(hidden)], [hbm]
    out_shape, out_specs = [], []
    n_items = 0
    if head:
        args += [attn, in_hbm(g_mlp), in_hbm(wo), in_hbm(wg), in_hbm(wu), in_hbm(wd)]
        in_specs += [hbm] * 6
        out_shape.append(jax.ShapeDtypeStruct(hidden.shape, hidden.dtype))
        out_specs.append(hbm)
        n_ffn = wg.shape[2] // CW
        n_items += n_ffn * NM
    if tail:
        args += [in_hbm(g_attn), in_hbm(wq), in_hbm(wk), in_hbm(wv), in_hbm(k_rows), in_hbm(v_rows)]
        in_specs += [hbm] * 6
        out_shape.append(jax.ShapeDtypeStruct((6, batch // 4, IW), BF16))
        out_specs.append(vmem)
        out_shape.append(pltpu.VMEM((n_pref, 2, SB) + k_rows.shape[2:], BF16))
        out_specs.append(vmem)
        n_items += 6 * NM
    dma = pltpu.SemaphoreType.DMA
    scratch = [
        pltpu.VMEM((NM, M, feat), BF16), pltpu.VMEM((NM, M, feat), BF16), pltpu.VMEM((2, NM, 4, 8, 128), F32),
        pltpu.VMEM((O2 + 1, 2 * R, IW), F32), pltpu.VMEM((O3 - O2 + 1, R, IW), F32),
        pltpu.VMEM((RING, 2 * R, IW), BF16), pltpu.VMEM((n_items, 2 * R, IW), BF16),
        pltpu.VMEM((RING, R, IW), BF16), pltpu.VMEM((n_items, R, IW), BF16),
        pltpu.VMEM((2,) + (g_mlp if head else g_attn).shape, BF16), dma((2,)),
        dma((NM, 4)), dma((2, NM, 3)), dma((2, NM, 3)), dma((n_items,)), dma((n_items,)), dma((n_items,)), dma((n_items,))]
    if head:
        scratch += [
            pltpu.VMEM((NM, M, attn.shape[1]), BF16), pltpu.VMEM(wo.shape[1:], BF16), pltpu.VMEM((n_ffn, feat, IW), BF16),
            pltpu.VMEM(wd.shape[1:], BF16), pltpu.VMEM((NM, M, feat), F32), pltpu.VMEM((n_ffn * NM, M, CW), BF16),
            pltpu.VMEM((2, NM, M, feat), BF16), pltpu.VMEM((2, NM, M, feat), BF16),
            dma((3, NM)), dma((3, NM)), dma((2, NM, 2)), dma((2, NM, 2)), dma((3, n_ffn * NM)), dma((3, n_ffn * NM)),
            dma, dma((2, n_ffn)), dma, dma((NM, 4)), dma((NM,))]
    if tail:
        scratch += [pltpu.VMEM((6, feat, IW), BF16), dma((6,)), dma((n_pref, 2))]
    return pl.pallas_call(
        functools.partial(chain_kernel, head, tail, layer, n_pref, model_dim),
        out_shape=out_shape, in_specs=in_specs, out_specs=out_specs, scratch_shapes=scratch,
        name=f'chain_{int(head)}{int(tail)}',
        compiler_params=pltpu.CompilerParams(collective_id=cid, has_side_effects=True, vmem_limit_bytes=vmem_mib * 1024 * 1024),
    )(*args)


def attn_kernel(layer, n_pref, pos_hbm, qkv_hbm, tabs_hbm, k_hbm, v_hbm, *refs):
    k_out, v_out, o_ref, pref, kv_slots, q_buf, kv_buf, o_buf, s_buf, p_buf, qkv_ref, tabs_ref, pos_ref, in_sem, out_sem, small_sem = refs[-16:]
    small = (pltpu.make_async_copy(qkv_hbm, qkv_ref, small_sem.at[0]), pltpu.make_async_copy(tabs_hbm, tabs_ref, small_sem.at[1]),
             pltpu.make_async_copy(pos_hbm, pos_ref, small_sem.at[2]))
    for cp in small:
        cp.start()
    local = o_ref.shape[0]
    n_q = q_buf.shape[0] // local
    n_kv = kv_buf.shape[1] // local
    n_rows = k_hbm.shape[2]
    group = n_q // n_kv
    per_chunk = qkv_ref.shape[2] // HEAD_DIM
    n_blocks = local // SB

    def held(blk, early):
        return pref.at[blk] if early else kv_slots.at[lax.rem(blk - n_pref, NBUF)]

    def run(blk, early, out, wait):
        seqs = pl.ds(blk * SB, SB)
        for c in (0, 1):
            here = held(blk, early).at[c]
            if out:
                cp = pltpu.make_async_copy(here, (k_out, v_out)[c].at[layer, seqs], out_sem.at[blk, c])
            else:
                cp = pltpu.make_async_copy((k_hbm, v_hbm)[c].at[layer, seqs], here, in_sem.at[blk, c])
            cp.wait() if wait else cp.start()

    for blk in range(n_pref, min(n_pref + NBUF, n_blocks)):
        run(blk, False, False, False)

    def head_of(idx):
        return qkv_ref[idx // per_chunk, :, pl.ds((idx % per_chunk) * HEAD_DIM, HEAD_DIM)].astype(F32)

    for cp in small:
        cp.wait()
    cos_tab, sin_tab = tabs_ref[pl.ds(0, local), :], tabs_ref[pl.ds(local, local), :]
    gains = [tabs_ref[pl.ds(2 * local + 2 * layer + i, 1), :] for i in (0, 1)]

    def norm_rope(vals, gain):
        normed = vals * lax.rsqrt(jnp.mean(vals * vals, axis=-1, keepdims=True) + NORM_EPS) * gain
        return (normed * cos_tab + pltpu.roll(normed, HEAD_DIM // 2, 1) * sin_tab).astype(BF16).astype(F32)
    for h in range(n_kv):
        kv_buf[0, pl.ds(h * local, local), :] = norm_rope(head_of(n_q + h), gains[1])
        kv_buf[1, pl.ds(h * local, local), :] = head_of(n_q + n_kv + h)

    row_ids = lax.broadcasted_iota(jnp.int32, (16, HEAD_DIM), 0)
    lane_ids = lax.broadcasted_iota(jnp.int32, (n_q, n_rows), 1)
    head_hit = lax.rem(lane_ids, n_kv) == lax.div(lax.broadcasted_iota(jnp.int32, (n_q, n_rows), 0), group)
    lane_of = jnp.where(head_hit, lane_ids, n_rows)

    def patch(blk, early):
        ref = held(blk, early)
        for i in range(SB):
            b = blk * SB + i
            row = pos_ref[b] * n_kv
            base = pl.multiple_of(lax.div(row, 16) * 16, 16)
            hit = lax.div(row_ids, n_kv) == lax.div(row - base, n_kv)
            for c in (0, 1):
                new = kv_buf[c, pl.ds(b, n_kv, stride=local), :]
                new = jnp.concatenate([new] * (16 // n_kv), axis=0)
                old = ref[c, i, pl.ds(base, 16), :]
                ref[c, i, pl.ds(base, 16), :] = jnp.where(hit, new, old.astype(F32)).astype(BF16)

    for blk in range(min(AHEAD, n_pref)):
        patch(blk, True)
    for h in range(n_q):
        q_buf[pl.ds(h * local, local), :] = norm_rope(head_of(h), gains[0])
    for blk in range(min(AHEAD, n_pref)):
        run(blk, True, True, False)

    def block_step(blk, early):
        ref = held(blk, early)
        if early:
            @pl.when(blk + AHEAD < n_pref)
            def _():
                patch(blk + AHEAD, True)
        else:
            run(blk, False, False, True)
            patch(blk, False)
        for i in range(SB):
            q = q_buf[pl.ds(blk * SB + i, n_q, stride=local), :].astype(BF16)
            s_buf[i] = lax.dot_general(q, ref[0, i], (((1,), (1,)), ((), ())), preferred_element_type=F32)
        if early:
            @pl.when(blk + AHEAD < n_pref)
            def _():
                run(blk + AHEAD, True, True, False)
        else:
            run(blk, False, True, False)
        for i in range(SB):
            row = pos_ref[blk * SB + i] * n_kv
            scores = jnp.where(lane_of < row + n_kv, s_buf[i] * (HEAD_DIM ** -0.5), -1e30)
            e = jnp.exp(scores - jnp.max(scores, axis=-1, keepdims=True))
            p_buf[i] = (e / jnp.sum(e, axis=-1, keepdims=True)).astype(BF16)
        for i in range(SB):
            o_buf[pl.ds(blk * SB + i, n_q, stride=local), :] = dot(p_buf[i], ref[1, i])

    def early_step(blk, carry):
        block_step(blk, True)
        return carry

    def late_step(blk, carry):
        block_step(blk, False)

        @pl.when((blk > n_pref) & (blk - 1 + NBUF < n_blocks))
        def _():
            run(blk - 1, False, True, True)
            run(blk - 1 + NBUF, False, False, False)
        return carry
    lax.fori_loop(0, n_pref, early_step, 0)
    if n_pref < n_blocks:
        lax.fori_loop(n_pref, n_blocks, late_step, 0)

    for h in range(n_q):
        o_ref[:, pl.ds(h * HEAD_DIM, HEAD_DIM)] = o_buf[pl.ds(h * local, local), :].astype(BF16)
    for blk in range(n_pref):
        run(blk, True, True, True)
    for blk in range(max(n_blocks - NBUF, n_pref), n_blocks):
        run(blk, False, True, True)


def attn_call(layer, pos, qkv, tabs, k_cache, v_cache, pref, prev):
    layers, local, n_rows, _ = k_cache.shape
    n_kv = 4
    n_q = 16
    vmem = pl.BlockSpec(memory_space=pltpu.VMEM)
    hbm = pl.BlockSpec(memory_space=pltpu.HBM)
    args = [in_hbm(pos), qkv if layer == 0 else in_hbm(qkv), in_hbm(tabs), in_hbm(k_cache), in_hbm(v_cache), pltpu.with_memory_space_constraint(pref, pltpu.VMEM)]
    in_specs = [hbm, hbm, hbm, hbm, hbm, vmem]
    aliases = {5: 3}
    n_pref, n_blocks = pref.shape[0], local // SB
    if prev is not None:
        args += list(prev)
        in_specs += [hbm] * 2
        aliases.update({6: 0, 7: 1})
    return pl.pallas_call(
        functools.partial(attn_kernel, layer, n_pref),
        out_shape=[jax.ShapeDtypeStruct(k_cache.shape, BF16)] * 2 + [jax.ShapeDtypeStruct((local, n_q * HEAD_DIM), BF16), jax.ShapeDtypeStruct(pref.shape, BF16)],
        in_specs=in_specs,
        out_specs=[hbm, hbm, vmem, vmem],
        scratch_shapes=[pltpu.VMEM((min(NBUF, max(n_blocks - n_pref, 1)) if n_pref < n_blocks else 1, 2, SB if n_pref < n_blocks else 1, n_rows, HEAD_DIM), BF16),
                        pltpu.VMEM((n_q * local, HEAD_DIM), F32), pltpu.VMEM((2, n_kv * local, HEAD_DIM), F32), pltpu.VMEM((n_q * local, HEAD_DIM), F32),
                        pltpu.VMEM((SB, n_q, n_rows), F32), pltpu.VMEM((SB, n_q, n_rows), BF16),
                        pltpu.VMEM(qkv.shape, BF16), pltpu.VMEM(tabs.shape, F32), pltpu.SMEM(pos.shape, jnp.int32),
                        pltpu.SemaphoreType.DMA((n_blocks, 2)), pltpu.SemaphoreType.DMA((n_blocks, 2)), pltpu.SemaphoreType.DMA((3,))],
        input_output_aliases=aliases, name=f'attn_{layer}',
        compiler_params=pltpu.CompilerParams(vmem_limit_bytes=(20 if layer == 0 else 22) * 1024 * 1024),
    )(*args)


def solution(mesh):
    group_size = mesh.shape['x']
    cache_spec = P(None, ('dp', 'x'), None, 'y', None)
    col_spec = P(None, 'x', 'y')
    row_spec = P(None, 'y', 'x')
    in_specs = (P('dp', 'x'), P('dp'), cache_spec, cache_spec, P(None, 'x'), P(None, 'x'), P(), P(), col_spec, col_spec, col_spec, row_spec, col_spec, col_spec, row_spec)
    out_specs = (P('dp', 'x'), cache_spec, cache_spec)

    def device_step(hidden, positions, k_cache, v_cache, g_attn, g_mlp, q_gain, k_gain, w_q, w_k, w_v, w_o, w_gate, w_up, w_down):
        model_dim = hidden.shape[1] * group_size
        layers, local, cache_len, n_kv, _ = k_cache.shape
        my_pos = lax.dynamic_slice_in_dim(positions, lax.axis_index('x') * local, local)
        half = HEAD_DIM // 2
        inv_freq = jnp.power(ROPE_BASE, -2.0 * jnp.arange(half, dtype=F32) / HEAD_DIM)
        angles = my_pos.astype(F32)[:, None] * inv_freq[None, :]
        cos_half, sin_half = jnp.cos(angles), jnp.sin(angles)
        gains = jnp.stack([q_gain[0], k_gain[0], q_gain[1], k_gain[1]]).astype(F32)
        tabs = jnp.concatenate([jnp.concatenate([cos_half, cos_half], axis=1), jnp.concatenate([-sin_half, sin_half], axis=1), gains, jnp.zeros((4, HEAD_DIM), F32)])
        tabs, my_pos, hidden = lax.optimization_barrier((tabs, my_pos, hidden))
        k_rows = k_cache.reshape(layers, local, cache_len * n_kv, HEAD_DIM)
        v_rows = v_cache.reshape(layers, local, cache_len * n_kv, HEAD_DIM)
        attn_tabs = (tabs, k_rows, v_rows)
        caches = {'k_rows': k_rows, 'v_rows': v_rows}
        qkv, pref = chain_call(False, True, 0, 0, 8, 16, model_dim, hidden, g_attn=g_attn, wq=w_q, wk=w_k, wv=w_v, **caches)
        k_new, v_new, attn, _ = attn_call(0, my_pos, qkv, *attn_tabs, pref, None)
        hidden, qkv, pref = chain_call(True, True, 0, 1, 5, 40, model_dim, hidden, attn, g_mlp, w_o, w_gate, w_up, w_down, g_attn, w_q, w_k, w_v, **caches)
        k_new, v_new, attn, _ = attn_call(1, my_pos, qkv, *attn_tabs, pref, (k_new, v_new))
        (hidden,) = chain_call(True, False, 1, 2, 0, 46, model_dim, hidden, attn, g_mlp, w_o, w_gate, w_up, w_down)
        return hidden, k_new.reshape(k_cache.shape), v_new.reshape(v_cache.shape)

    return jax.shard_map(device_step, mesh=mesh, in_specs=in_specs, out_specs=out_specs, check_vma=False)
```

```python
import functools

import jax
import jax.numpy as jnp
from jax import lax
from jax.experimental import pallas as pl
from jax.experimental.pallas import tpu as pltpu
from jax.sharding import PartitionSpec as P

HEAD_DIM = 128
NORM_EPS = 1e-6
ROPE_BASE = 1000000.0
MESH = pl.DeviceIdType.MESH
BF16 = jnp.bfloat16
F32 = jnp.float32

CW = 256
IW = 2 * CW
O2, O3, O4, O5 = 3, 8, 13, 16
E1, E2, E3, E4 = 2, 8, 6, 10
QKV_LAG = 2
HEAD_GROUPS = 2
RING = 8
SB = 8
AHEAD = 2
NBUF = 3
MASK = (0, 2, 1, 3)
POS = (0, 2, 1, 3)
HALVES = ((0, 2), (1, 3))


def in_hbm(x):
    return pltpu.with_memory_space_constraint(x, pltpu.HBM)


def groups(head):
    return HEAD_GROUPS if head else 1


def dot(a, b):
    return jnp.dot(a, b, preferred_element_type=F32)


def chain_kernel(head, tail, layer, n_pref, model_dim, *refs):
    NM = groups(head)
    it = iter(refs)
    hid_in = next(it)
    if head:
        attn_in, g_mlp_in = next(it), next(it)
        wo_in, wg_in, wu_in, wd_in = (next(it).at[layer] for _ in range(4))
    if tail:
        tail_layer = layer + 1 if head else layer
        g_attn_in = next(it)
        wq_in, wk_in, wv_in, k_in, v_in = (next(it).at[tail_layer] for _ in range(5))
    if head:
        hid_out = next(it)
    if tail:
        qkv_out, pref_out = next(it), next(it)
    h_buf, n_buf, stat_buf, keep_buf, own_buf, dsend, drecv, xsend, xrecv = (next(it) for _ in range(9))
    gain_buf, gain_sem = next(it), next(it)
    h_sem, st_ss, st_rs, d_ss, d_rs, x_ss, x_rs = (next(it) for _ in range(7))
    if head:
        attn_all, wo_buf, wgu_buf, wd_buf, acc_buf, act_all, y_send, y_recv = (next(it) for _ in range(8))
        ag_ss, ag_rs, y_ss, y_rs, act_ss, act_rs, wo_sem, wgu_sem, wd_sem, o_sem, a_sem = (next(it) for _ in range(11))
    if tail:
        wqkv_buf, wqkv_sem, pref_sem = (next(it) for _ in range(3))

    me = lax.axis_index('x')
    yy = lax.axis_index('y')
    chip, core = lax.div(me, 2), lax.rem(me, 2)
    d1 = chip * 2 + (1 - core)
    d2 = (1 - chip) * 2 + core
    d3 = (1 - chip) * 2 + (1 - core)
    quarter = (me, d2, d1, d3)
    R = h_buf.shape[1] // 4
    M = 4 * R
    n_ffn = act_all.shape[0] // NM if head else 0
    n_mlp = n_ffn * NM
    n_qkv = 6
    ring = dsend.shape[0]
    n_items = drecv.shape[0]

    def after_ring(s, action):
        if isinstance(s, int):
            if s >= ring:
                action()
        else:
            pl.when(s >= ring)(action)

    barrier = pltpu.get_barrier_semaphore()
    for peer in ({'x': d1}, {'x': d2}, {'x': d3}, {'y': 1 - yy}):
        pl.semaphore_signal(barrier, inc=1, device_id=peer, device_id_type=MESH)

    def remote(src, dst, ss, rs, peer):
        return pltpu.make_async_remote_copy(src_ref=src, dst_ref=dst, send_sem=ss, recv_sem=rs, device_id=peer, device_id_type=MESH)

    def attn_own(m):
        return pltpu.make_async_copy(attn_in.at[pl.ds(m * R, R)], attn_all.at[m, pl.ds(0, R)], a_sem.at[m])
    if head:
        for m in range(NM):
            attn_own(m).start()

    def hid_copy(m, k):
        row = pl.multiple_of(quarter[k] * (NM * R) + m * R, R)
        return pltpu.make_async_copy(hid_in.at[pl.ds(row, R)], h_buf.at[m, pl.ds(k * R, R)], h_sem.at[m, k])

    for m in range(NM):
        for k in range(4):
            hid_copy(m, k).start()
    gain_copies = []
    if head:
        gain_copies.append(pltpu.make_async_copy(g_mlp_in, gain_buf.at[0], gain_sem.at[0]))
    if tail:
        gain_copies.append(pltpu.make_async_copy(g_attn_in, gain_buf.at[1], gain_sem.at[1]))
    for cp in gain_copies:
        cp.start()

    def wgu_copy(j):
        off = pl.multiple_of(j * CW, CW)
        return (pltpu.make_async_copy(wg_in.at[:, pl.ds(off, CW)], wgu_buf.at[j, :, pl.ds(0, CW)], wgu_sem.at[0, j]),
                pltpu.make_async_copy(wu_in.at[:, pl.ds(off, CW)], wgu_buf.at[j, :, pl.ds(CW, CW)], wgu_sem.at[1, j]))

    if head:
        wo_copy = pltpu.make_async_copy(wo_in, wo_buf, wo_sem)
        wd_copy = pltpu.make_async_copy(wd_in, wd_buf, wd_sem)
    if tail:
        wqkv_copies = [pltpu.make_async_copy(wq_in.at[:, pl.ds(j * IW, IW)], wqkv_buf.at[j], wqkv_sem.at[j]) for j in range(4)]
        wqkv_copies += [pltpu.make_async_copy(w, wqkv_buf.at[j], wqkv_sem.at[j]) for j, w in ((4, wk_in), (5, wv_in))]
    def start_wgu(j, c):
        for cp in wgu_copy(j):
            cp.start()
        return c
    if head:
        wo_copy.start()
    else:
        for cp in wqkv_copies:
            cp.start()

    def pref_copy(blk, c):
        seqs = pl.ds(blk * SB, SB)
        return pltpu.make_async_copy((k_in, v_in)[c].at[seqs], pref_out.at[blk, c], pref_sem.at[blk, c])
    def pref_start():
        for blk in range(n_pref):
            for c in (0, 1):
                pref_copy(blk, c).start()

    def diag():
        return lax.broadcasted_iota(jnp.int32, (R, 128), 0) == lax.broadcasted_iota(jnp.int32, (R, 128), 1)

    def stat_send(kind, m, a):
        peer = (None, d1, d2, d3)[a]
        return remote(stat_buf.at[kind, m, 0], stat_buf.at[kind, m, a], st_ss.at[kind, m, a - 1], st_rs.at[kind, m, a - 1], {'x': peer})

    def stats_start(kind, m):
        for k in range(4):
            hv = h_buf[m, pl.ds(k * R, R), :].astype(F32)
            row_sum = jnp.sum(hv * hv, axis=1, keepdims=True)
            stat_buf[kind, m, 0, pl.ds(k, 1), :] = jnp.sum(jnp.where(diag(), row_sum, 0.0), axis=0, keepdims=True)
        for a in (1, 2, 3):
            stat_send(kind, m, a).start()

    def norm(kind, m, gain):
        for a in (1, 2, 3):
            stat_send(kind, m, a).wait()
        gain_row = gain.astype(F32)
        for k in range(4):
            total = stat_buf[kind, m, 0, pl.ds(k, 1), :]
            for a in (1, 2, 3):
                total = total + stat_buf[kind, m, a, pl.ds(POS[MASK[k] ^ a], 1), :]
            col = jnp.sum(jnp.where(diag(), total, 0.0), axis=1, keepdims=True)
            hv = h_buf[m, pl.ds(k * R, R), :].astype(F32)
            n_buf[m, pl.ds(k * R, R), :] = (hv * lax.rsqrt(col / model_dim + NORM_EPS) * gain_row).astype(BF16)

    def d_copy(s):
        return remote(dsend.at[lax.rem(s, ring)], drecv.at[s], d_ss.at[s], d_rs.at[s], {'x': d1})

    def x_copy(s):
        return remote(xsend.at[lax.rem(s, ring)], xrecv.at[s], x_ss.at[s], x_rs.at[s], {'x': d2})

    def stage1_math(s, m, w):
        part = dot(n_buf[m], w)
        keep_buf[lax.rem(s, keep_buf.shape[0])] = part[:2 * R]
        dsend[lax.rem(s, ring)] = part[2 * R:].astype(BF16)

    def stage1(s, m, w):
        after_ring(s, lambda: d_copy(s - ring).wait_send())
        stage1_math(s, m, w)
        d_copy(s).start()

    def stage2_wait(s):
        d_copy(s).wait_recv()
        after_ring(s, lambda: x_copy(s - ring).wait_send())

    def stage2_math(s):
        slot = lax.rem(s, keep_buf.shape[0])
        xsend[lax.rem(s, ring)] = (keep_buf[slot, pl.ds(R, R), :] + drecv[s, pl.ds(R, R), :].astype(F32)).astype(BF16)
        own_buf[lax.rem(s, own_buf.shape[0])] = keep_buf[slot, pl.ds(0, R), :] + drecv[s, pl.ds(0, R), :].astype(F32)

    def stage2(s):
        stage2_wait(s)
        stage2_math(s)
        x_copy(s).start()

    def stage3_sum(s):
        return (own_buf[lax.rem(s, own_buf.shape[0])] + xrecv[s].astype(F32)).astype(BF16)

    def stage3(s):
        x_copy(s).wait_recv()
        return stage3_sum(s)

    def gather_copies(buf, i, ss, rs):
        own, other = buf.at[i, pl.ds(0, R)], buf.at[i, pl.ds(R, R)]
        return (lambda: remote(own, buf.at[i, pl.ds(2 * R, R)], ss.at[0, i], rs.at[0, i], {'x': d1}),
                lambda: remote(own, buf.at[i, pl.ds(R, R)], ss.at[1, i], rs.at[1, i], {'x': d2}),
                lambda: remote(other, buf.at[i, pl.ds(3 * R, R)], ss.at[2, i], rs.at[2, i], {'x': d1}))

    def attn_copies(m):
        return gather_copies(attn_all, m, ag_ss, ag_rs)

    def y_copy(kind, m, half):
        rows = pl.ds(half * 2 * R, 2 * R)
        return remote(y_send.at[kind, m, rows], y_recv.at[kind, m, rows], y_ss.at[kind, m, half], y_rs.at[kind, m, half], {'y': 1 - yy})

    def attn_half(m, half):
        rows = jnp.concatenate([attn_all[m, pl.ds(k * R, R), :] for k in HALVES[half]], axis=0)
        y_send[0, m, pl.ds(half * 2 * R, 2 * R), :] = dot(rows, wo_buf[...]).astype(BF16)
        y_copy(0, m, half).start()

    def attn_finish(m):
        for half in (0, 1):
            y_copy(0, m, half).wait()
            for i, k in enumerate(HALVES[half]):
                here, there = pl.ds(k * R, R), pl.ds((half * 2 + i) * R, R)
                total = (y_send[0, m, there, :].astype(F32) + y_recv[0, m, there, :].astype(F32)).astype(BF16)
                h_buf[m, here, :] = (h_buf[m, here, :].astype(F32) + total.astype(F32)).astype(BF16)

    def mlp_start(m):
        y_send[1, m] = acc_buf[m].astype(BF16)
        for half in (0, 1):
            y_copy(1, m, half).start()

    def mlp_finish(m):
        for half in (0, 1):
            y_copy(1, m, half).wait()
            rows = pl.ds(half * 2 * R, 2 * R)
            total = (y_send[1, m, rows, :].astype(F32) + y_recv[1, m, rows, :].astype(F32)).astype(BF16)
            h_buf[m, rows, :] = (h_buf[m, rows, :].astype(F32) + total.astype(F32)).astype(BF16)

    def act_copies(t):
        return gather_copies(act_all, t, act_ss, act_rs)

    def out_copy(m, k):
        row = pl.multiple_of(quarter[k] * (NM * R) + m * R, R)
        return pltpu.make_async_copy(h_buf.at[m, pl.ds(k * R, R)], hid_out.at[pl.ds(row, R)], o_sem.at[m, k])

    def mid_ready(m):
        attn_finish(m)
        stats_start(0, m)

    def layer_done(m):
        mlp_finish(m)
        if tail:
            stats_start(1, m)
        for k in range(4):
            out_copy(m, k).start()

    def split(t):
        return (0, t) if NM == 1 else (lax.div(t, n_ffn), lax.rem(t, n_ffn))

    def mlp_iter(t, steady):
        def stage(first, action):
            if steady:
                action()
            else:
                pl.when((t >= first) & (t < n_mlp + first))(action)

        def relay_on():
            _, to_chip, relay = act_copies(t - O4)
            to_chip().wait_recv()
            relay().start()

        def act_ready():
            to_core, _, relay = act_copies(t - O5)
            to_core().wait_recv()
            relay().wait_recv()

        @pl.when(t < n_ffn)
        def _():
            for cp in wgu_copy(t):
                cp.wait()
        stage(O4, relay_on)
        stage(O2, lambda: stage2_wait(t - O2))
        stage(O3, lambda: x_copy(t - O3).wait_recv())
        stage(O5, act_ready)
        stage(0, lambda: after_ring(t, lambda: d_copy(t - ring).wait_send()))

        def activate():
            s = t - O3
            full = stage3_sum(s)
            gate, up = full[:, :CW].astype(F32), full[:, CW:].astype(F32)
            act_all[s, pl.ds(0, R), :] = (jax.nn.silu(gate) * up).astype(BF16)

        def product():
            m, j = split(t)
            stage1_math(t, m, wgu_buf[j])

        def down():
            s = t - O5
            m, j = split(s)
            acc_buf[m] += dot(act_all[s], wd_buf[pl.ds(pl.multiple_of(j * CW, CW), CW), :])

        def send_act():
            to_core, to_chip, _ = act_copies(t - O3)
            to_chip().start()
            to_core().start()

        stage(O2, lambda: stage2_math(t - O2))
        stage(O3, activate)
        stage(0, product)
        stage(O5, down)
        stage(O2, lambda: x_copy(t - O2).start())
        stage(O3, send_act)
        stage(0, lambda: d_copy(t).start())

    pl.semaphore_wait(barrier, 4)
    for cp in gain_copies:
        cp.wait()

    if head:
        for m in range(NM):
            attn_own(m).wait()
            to_core, to_chip, _ = attn_copies(m)
            to_chip().start()
            to_core().start()
            acc_buf[m] = jnp.zeros(acc_buf.shape[1:], F32)
        for m in range(NM):
            for k in range(4):
                hid_copy(m, k).wait()
        wo_copy.wait()
        lax.fori_loop(0, n_ffn, start_wgu, 0)
        wd_copy.start()
        if tail:
            for cp in wqkv_copies:
                cp.start()
        for m in range(NM):
            attn_copies(m)[0]().wait_recv()
            attn_half(m, 0)
        for m in range(NM):
            _, to_chip, relay = attn_copies(m)
            to_chip().wait_recv()
            relay().start()
            relay().wait_recv()
            attn_half(m, 1)
        mid_ready(0)
        norm(0, 0, gain_buf[0, pl.ds(layer, 1), :])
        if tail:
            pref_start()
        events = {}

        def at(t, action, *operands):
            events.setdefault(t, []).append(functools.partial(action, *operands))
        for m in range(1, NM):
            at((m - 1) * n_ffn + E1, mid_ready, m)
            at((m - 1) * n_ffn + E2, lambda m: norm(0, m, gain_buf[0, pl.ds(layer, 1), :]), m)
        for m in range(NM - 1):
            done = (m + 1) * n_ffn - 1 + O5
            at(done, mlp_start, m)
            at(min(done + E3, n_mlp + O5 - 2), layer_done, m)
            if tail:
                at(min(done + E4, n_mlp + O5 - 1), lambda m: norm(1, m, gain_buf[1, pl.ds(tail_layer, 1), :]), m)

        def body(steady, t, c):
            mlp_iter(t, steady)
            for when, actions in events.items():
                @pl.when(t == when)
                def _(actions=actions):
                    for action in actions:
                        action()
            return c
        lax.fori_loop(0, O5, functools.partial(body, False), 0)
        wd_copy.wait()
        lax.fori_loop(O5, n_mlp, functools.partial(body, True), 0)
        lax.fori_loop(n_mlp, n_mlp + O5, functools.partial(body, False), 0)
        mlp_start(NM - 1)
        if not tail:
            layer_done(NM - 1)
    else:
        for m in range(NM):
            for k in range(4):
                hid_copy(m, k).wait()
            stats_start(1, m)

    if tail:
        for cp in wqkv_copies:
            cp.wait()
        if not head:
            pref_start()

        def qkv_send(m):
            first = n_mlp + m * n_qkv
            for t in range(n_qkv + QKV_LAG):
                if t < n_qkv:
                    stage1(first + t, m, wqkv_buf[t])
                if t >= QKV_LAG:
                    stage2(first + t - QKV_LAG)

        def qkv_take(m):
            for j in range(n_qkv):
                qkv_out[j, pl.ds(m * R, R), :] = stage3(n_mlp + m * n_qkv + j)

        last = NM - 1
        for m in range(last):
            qkv_send(m)
        if head:
            layer_done(last)
        for m in range(last):
            qkv_take(m)
        norm(1, last, gain_buf[1, pl.ds(tail_layer, 1), :])
        qkv_send(last)
        qkv_take(last)

    if tail:
        for blk in range(n_pref):
            for c in (0, 1):
                pref_copy(blk, c).wait()

    def drain(s, c):
        d_copy(s).wait_send()
        x_copy(s).wait_send()
        return c
    lax.fori_loop(max(n_items - ring, 0), n_items, drain, 0)
    if head:
        def drain_act(s, c):
            for cp in act_copies(s):
                cp().wait_send()
            return c
        lax.fori_loop(0, n_mlp, drain_act, 0)
        for m in range(NM):
            for cp in attn_copies(m):
                cp().wait_send()
            for k in range(4):
                out_copy(m, k).wait()


def chain_call(head, tail, layer, cid, n_pref, vmem_mib, model_dim, hidden, attn=None, g_mlp=None, wo=None, wg=None, wu=None, wd=None, g_attn=None, wq=None, wk=None, wv=None, k_rows=None, v_rows=None):
    batch, feat = hidden.shape
    NM = groups(head)
    M = batch // NM
    R = M // 4
    vmem = pl.BlockSpec(memory_space=pltpu.VMEM)
    hbm = pl.BlockSpec(memory_space=pltpu.HBM)
    args, in_specs = [in_hbm(hidden)], [hbm]
    out_shape, out_specs = [], []
    n_items = 0
    if head:
        args += [attn, in_hbm(g_mlp), in_hbm(wo), in_hbm(wg), in_hbm(wu), in_hbm(wd)]
        in_specs += [hbm] * 6
        out_shape.append(jax.ShapeDtypeStruct(hidden.shape, hidden.dtype))
        out_specs.append(hbm)
        n_ffn = wg.shape[2] // CW
        n_items += n_ffn * NM
    if tail:
        args += [in_hbm(g_attn), in_hbm(wq), in_hbm(wk), in_hbm(wv), in_hbm(k_rows), in_hbm(v_rows)]
        in_specs += [hbm] * 6
        out_shape.append(jax.ShapeDtypeStruct((6, batch // 4, IW), BF16))
        out_specs.append(vmem)
        out_shape.append(pltpu.VMEM((n_pref, 2, SB) + k_rows.shape[2:], BF16))
        out_specs.append(vmem)
        n_items += 6 * NM
    dma = pltpu.SemaphoreType.DMA
    scratch = [
        pltpu.VMEM((NM, M, feat), BF16), pltpu.VMEM((NM, M, feat), BF16), pltpu.VMEM((2, NM, 4, 8, 128), F32),
        pltpu.VMEM((max(O2, QKV_LAG) + 1, 2 * R, IW), F32), pltpu.VMEM((max(O3 - O2 + 1, 6), R, IW), F32),
        pltpu.VMEM((RING, 2 * R, IW), BF16), pltpu.VMEM((n_items, 2 * R, IW), BF16),
        pltpu.VMEM((RING, R, IW), BF16), pltpu.VMEM((n_items, R, IW), BF16),
        pltpu.VMEM((2,) + (g_mlp if head else g_attn).shape, BF16), dma((2,)),
        dma((NM, 4)), dma((2, NM, 3)), dma((2, NM, 3)), dma((n_items,)), dma((n_items,)), dma((n_items,)), dma((n_items,))]
    if head:
        scratch += [
            pltpu.VMEM((NM, M, attn.shape[1]), BF16), pltpu.VMEM(wo.shape[1:], BF16), pltpu.VMEM((n_ffn, feat, IW), BF16),
            pltpu.VMEM(wd.shape[1:], BF16), pltpu.VMEM((NM, M, feat), F32), pltpu.VMEM((n_ffn * NM, M, CW), BF16),
            pltpu.VMEM((2, NM, M, feat), BF16), pltpu.VMEM((2, NM, M, feat), BF16),
            dma((3, NM)), dma((3, NM)), dma((2, NM, 2)), dma((2, NM, 2)), dma((3, n_ffn * NM)), dma((3, n_ffn * NM)),
            dma, dma((2, n_ffn)), dma, dma((NM, 4)), dma((NM,))]
    if tail:
        scratch += [pltpu.VMEM((6, feat, IW), BF16), dma((6,)), dma((n_pref, 2))]
    return pl.pallas_call(
        functools.partial(chain_kernel, head, tail, layer, n_pref, model_dim),
        out_shape=out_shape, in_specs=in_specs, out_specs=out_specs, scratch_shapes=scratch,
        name=f'chain_{int(head)}{int(tail)}',
        compiler_params=pltpu.CompilerParams(collective_id=cid, has_side_effects=True, vmem_limit_bytes=vmem_mib * 1024 * 1024),
    )(*args)


def attn_kernel(layer, n_pref, pos_hbm, qkv_hbm, tabs_hbm, k_hbm, v_hbm, *refs):
    k_out, v_out, o_ref, pref, kv_slots, q_buf, kv_buf, o_buf, s_buf, p_buf, qkv_ref, tabs_ref, pos_ref, in_sem, out_sem, small_sem = refs[-16:]
    small = (pltpu.make_async_copy(qkv_hbm, qkv_ref, small_sem.at[0]), pltpu.make_async_copy(tabs_hbm, tabs_ref, small_sem.at[1]),
             pltpu.make_async_copy(pos_hbm, pos_ref, small_sem.at[2]))
    for cp in small:
        cp.start()
    local = o_ref.shape[0]
    n_q = q_buf.shape[0] // local
    n_kv = kv_buf.shape[1] // local
    n_rows = k_hbm.shape[2]
    group = n_q // n_kv
    per_chunk = qkv_ref.shape[2] // HEAD_DIM
    n_blocks = local // SB

    def held(blk, early):
        return pref.at[blk] if early else kv_slots.at[lax.rem(blk - n_pref, NBUF)]

    def run(blk, early, out, wait):
        seqs = pl.ds(blk * SB, SB)
        for c in (0, 1):
            here = held(blk, early).at[c]
            if out:
                cp = pltpu.make_async_copy(here, (k_out, v_out)[c].at[layer, seqs], out_sem.at[blk, c])
            else:
                cp = pltpu.make_async_copy((k_hbm, v_hbm)[c].at[layer, seqs], here, in_sem.at[blk, c])
            cp.wait() if wait else cp.start()

    for blk in range(n_pref, min(n_pref + NBUF, n_blocks)):
        run(blk, False, False, False)

    def head_of(idx):
        return qkv_ref[idx // per_chunk, :, pl.ds((idx % per_chunk) * HEAD_DIM, HEAD_DIM)].astype(F32)

    for cp in small:
        cp.wait()
    cos_tab, sin_tab = tabs_ref[pl.ds(0, local), :], tabs_ref[pl.ds(local, local), :]
    gains = [tabs_ref[pl.ds(2 * local + 2 * layer + i, 1), :] for i in (0, 1)]

    def norm_rope(vals, gain):
        normed = vals * lax.rsqrt(jnp.mean(vals * vals, axis=-1, keepdims=True) + NORM_EPS) * gain
        return (normed * cos_tab + pltpu.roll(normed, HEAD_DIM // 2, 1) * sin_tab).astype(BF16).astype(F32)
    for h in range(n_kv):
        kv_buf[0, pl.ds(h * local, local), :] = norm_rope(head_of(n_q + h), gains[1])
        kv_buf[1, pl.ds(h * local, local), :] = head_of(n_q + n_kv + h)

    row_ids = lax.broadcasted_iota(jnp.int32, (16, HEAD_DIM), 0)
    lane_ids = lax.broadcasted_iota(jnp.int32, (n_q, n_rows), 1)
    head_hit = lax.rem(lane_ids, n_kv) == lax.div(lax.broadcasted_iota(jnp.int32, (n_q, n_rows), 0), group)
    lane_of = jnp.where(head_hit, lane_ids, n_rows)

    def patch(blk, early):
        ref = held(blk, early)
        for i in range(SB):
            b = blk * SB + i
            row = pos_ref[b] * n_kv
            base = pl.multiple_of(lax.div(row, 16) * 16, 16)
            hit = lax.div(row_ids, n_kv) == lax.div(row - base, n_kv)
            for c in (0, 1):
                new = kv_buf[c, pl.ds(b, n_kv, stride=local), :]
                new = jnp.concatenate([new] * (16 // n_kv), axis=0)
                old = ref[c, i, pl.ds(base, 16), :]
                ref[c, i, pl.ds(base, 16), :] = jnp.where(hit, new, old.astype(F32)).astype(BF16)

    for blk in range(min(AHEAD, n_pref)):
        patch(blk, True)
    for h in range(n_q):
        q_buf[pl.ds(h * local, local), :] = norm_rope(head_of(h), gains[0])
    for blk in range(min(AHEAD, n_pref)):
        run(blk, True, True, False)

    def block_step(blk, early, nxt, nxt_early):
        ref = held(blk, early)
        if nxt is not None:
            if not nxt_early:
                run(nxt, False, False, True)
            patch(nxt, nxt_early)
        for i in range(SB):
            q = q_buf[pl.ds(blk * SB + i, n_q, stride=local), :].astype(BF16)
            s_buf[i] = lax.dot_general(q, ref[0, i], (((1,), (1,)), ((), ())), preferred_element_type=F32)
        if nxt is not None:
            run(nxt, nxt_early, True, False)
        for i in range(SB):
            row = pos_ref[blk * SB + i] * n_kv
            scores = jnp.where(lane_of < row + n_kv, s_buf[i] * (HEAD_DIM ** -0.5), -1e30)
            e = jnp.exp(scores - jnp.max(scores, axis=-1, keepdims=True))
            p_buf[i] = (e / jnp.sum(e, axis=-1, keepdims=True)).astype(BF16)
        for i in range(SB):
            o_buf[pl.ds(blk * SB + i, n_q, stride=local), :] = dot(p_buf[i], ref[1, i])

    def early_step(blk, carry):
        block_step(blk, True, blk + AHEAD, True)
        return carry
    lax.fori_loop(0, n_pref - AHEAD, early_step, 0)
    for blk in range(n_pref - AHEAD, n_blocks):
        nxt = blk + AHEAD if blk + AHEAD < n_blocks else None
        block_step(blk, blk < n_pref, nxt, False)

    for h in range(n_q):
        o_ref[:, pl.ds(h * HEAD_DIM, HEAD_DIM)] = o_buf[pl.ds(h * local, local), :].astype(BF16)
    for blk in range(n_pref):
        run(blk, True, True, True)
    for blk in range(max(n_blocks - NBUF, n_pref), n_blocks):
        run(blk, False, True, True)


def attn_call(layer, pos, qkv, tabs, k_cache, v_cache, pref, prev):
    layers, local, n_rows, _ = k_cache.shape
    n_kv = 4
    n_q = 16
    vmem = pl.BlockSpec(memory_space=pltpu.VMEM)
    hbm = pl.BlockSpec(memory_space=pltpu.HBM)
    args = [in_hbm(pos), qkv if layer == 0 else in_hbm(qkv), in_hbm(tabs), in_hbm(k_cache), in_hbm(v_cache), pltpu.with_memory_space_constraint(pref, pltpu.VMEM)]
    in_specs = [hbm, hbm, hbm, hbm, hbm, vmem]
    aliases = {5: 3}
    n_pref, n_blocks = pref.shape[0], local // SB
    if prev is not None:
        args += list(prev)
        in_specs += [hbm] * 2
        aliases.update({6: 0, 7: 1})
    return pl.pallas_call(
        functools.partial(attn_kernel, layer, n_pref),
        out_shape=[jax.ShapeDtypeStruct(k_cache.shape, BF16)] * 2 + [jax.ShapeDtypeStruct((local, n_q * HEAD_DIM), BF16), jax.ShapeDtypeStruct(pref.shape, BF16)],
        in_specs=in_specs,
        out_specs=[hbm, hbm, vmem, vmem],
        scratch_shapes=[pltpu.VMEM((min(NBUF, max(n_blocks - n_pref, 1)) if n_pref < n_blocks else 1, 2, SB if n_pref < n_blocks else 1, n_rows, HEAD_DIM), BF16),
                        pltpu.VMEM((n_q * local, HEAD_DIM), F32), pltpu.VMEM((2, n_kv * local, HEAD_DIM), F32), pltpu.VMEM((n_q * local, HEAD_DIM), F32),
                        pltpu.VMEM((SB, n_q, n_rows), F32), pltpu.VMEM((SB, n_q, n_rows), BF16),
                        pltpu.VMEM(qkv.shape, BF16), pltpu.VMEM(tabs.shape, F32), pltpu.SMEM(pos.shape, jnp.int32),
                        pltpu.SemaphoreType.DMA((n_blocks, 2)), pltpu.SemaphoreType.DMA((n_blocks, 2)), pltpu.SemaphoreType.DMA((3,))],
        input_output_aliases=aliases, name=f'attn_{layer}',
        compiler_params=pltpu.CompilerParams(vmem_limit_bytes=(20 if layer == 0 else 22) * 1024 * 1024),
    )(*args)


def solution(mesh):
    group_size = mesh.shape['x']
    cache_spec = P(None, ('dp', 'x'), None, 'y', None)
    col_spec = P(None, 'x', 'y')
    row_spec = P(None, 'y', 'x')
    in_specs = (P('dp', 'x'), P('dp'), cache_spec, cache_spec, P(None, 'x'), P(None, 'x'), P(), P(), col_spec, col_spec, col_spec, row_spec, col_spec, col_spec, row_spec)
    out_specs = (P('dp', 'x'), cache_spec, cache_spec)

    def device_step(hidden, positions, k_cache, v_cache, g_attn, g_mlp, q_gain, k_gain, w_q, w_k, w_v, w_o, w_gate, w_up, w_down):
        model_dim = hidden.shape[1] * group_size
        layers, local, cache_len, n_kv, _ = k_cache.shape
        my_pos = lax.dynamic_slice_in_dim(positions, lax.axis_index('x') * local, local)
        half = HEAD_DIM // 2
        inv_freq = jnp.power(ROPE_BASE, -2.0 * jnp.arange(half, dtype=F32) / HEAD_DIM)
        angles = my_pos.astype(F32)[:, None] * inv_freq[None, :]
        cos_half, sin_half = jnp.cos(angles), jnp.sin(angles)
        gains = jnp.stack([q_gain[0], k_gain[0], q_gain[1], k_gain[1]]).astype(F32)
        tabs = jnp.concatenate([jnp.concatenate([cos_half, cos_half], axis=1), jnp.concatenate([-sin_half, sin_half], axis=1), gains, jnp.zeros((4, HEAD_DIM), F32)])
        tabs, my_pos, hidden = lax.optimization_barrier((tabs, my_pos, hidden))
        k_rows = k_cache.reshape(layers, local, cache_len * n_kv, HEAD_DIM)
        v_rows = v_cache.reshape(layers, local, cache_len * n_kv, HEAD_DIM)
        attn_tabs = (tabs, k_rows, v_rows)
        caches = {'k_rows': k_rows, 'v_rows': v_rows}
        qkv, pref = chain_call(False, True, 0, 0, 8, 16, model_dim, hidden, g_attn=g_attn, wq=w_q, wk=w_k, wv=w_v, **caches)
        k_new, v_new, attn, _ = attn_call(0, my_pos, qkv, *attn_tabs, pref, None)
        hidden, qkv, pref = chain_call(True, True, 0, 1, 5, 40, model_dim, hidden, attn, g_mlp, w_o, w_gate, w_up, w_down, g_attn, w_q, w_k, w_v, **caches)
        k_new, v_new, attn, _ = attn_call(1, my_pos, qkv, *attn_tabs, pref, (k_new, v_new))
        (hidden,) = chain_call(True, False, 1, 2, 0, 46, model_dim, hidden, attn, g_mlp, w_o, w_gate, w_up, w_down)
        return hidden, k_new.reshape(k_cache.shape), v_new.reshape(v_cache.shape)

    return jax.shard_map(device_step, mesh=mesh, in_specs=in_specs, out_specs=out_specs, check_vma=False)
```

```python
import functools

import jax
import jax.numpy as jnp
import numpy as np
from jax import lax
from jax.experimental import pallas as pl
from jax.experimental.pallas import tpu as pltpu
from jax.sharding import PartitionSpec as P

HEAD_DIM = 128
NORM_EPS = 1e-6
ROPE_BASE = 1000000.0
MESH = pl.DeviceIdType.MESH
BF16 = jnp.bfloat16
F32 = jnp.float32

CW = 256
IW = 2 * CW
O2, O3, O4, O5 = 2, 8, 14, 16
E1, E2, E3, E4 = 6, 12, 8, 14
QKV_LAG = 2
HEAD_GROUPS = 2
RING = 8
SB = 8
AHEAD = 2
NBUF = 3
MASK = (0, 2, 1, 3)
POS = (0, 2, 1, 3)
HALVES = ((0, 2), (1, 3))


def in_hbm(x):
    return pltpu.with_memory_space_constraint(x, pltpu.HBM)


def groups(head):
    return HEAD_GROUPS if head else 1


def dot(a, b):
    return jnp.dot(a, b, preferred_element_type=F32)


def chain_kernel(head, tail, layer, n_pref, model_dim, *refs):
    NM = groups(head)
    it = iter(refs)
    hid_in = next(it)
    if head:
        attn_in, g_mlp_in = next(it), next(it)
        wo_in, wg_in, wu_in, wd_in = (next(it).at[layer] for _ in range(4))
    if tail:
        tail_layer = layer + 1 if head else layer
        g_attn_in = next(it)
        wq_in, wk_in, wv_in, k_in, v_in = (next(it).at[tail_layer] for _ in range(5))
    if head:
        hid_out = next(it)
    if tail:
        qkv_out, pref_out = next(it), next(it)
    h_buf, n_buf, stat_buf, keep_buf, own_buf, dsend, drecv, xsend, xrecv = (next(it) for _ in range(9))
    gain_buf, gain_sem = next(it), next(it)
    h_sem, st_ss, st_rs, d_ss, d_rs, x_ss, x_rs = (next(it) for _ in range(7))
    if head:
        attn_all, wo_buf, wgu_buf, wd_buf, acc_buf, act_all, y_send, y_recv = (next(it) for _ in range(8))
        ag_ss, ag_rs, y_ss, y_rs, act_ss, act_rs, wo_sem, wgu_sem, wd_sem, o_sem, a_sem = (next(it) for _ in range(11))
    if tail:
        wqkv_buf, wqkv_sem, pref_sem = (next(it) for _ in range(3))

    me = lax.axis_index('x')
    yy = lax.axis_index('y')
    chip, core = lax.div(me, 2), lax.rem(me, 2)
    d1 = chip * 2 + (1 - core)
    d2 = (1 - chip) * 2 + core
    d3 = (1 - chip) * 2 + (1 - core)
    quarter = (me, d2, d1, d3)
    R = h_buf.shape[1] // 4
    M = 4 * R
    n_ffn = act_all.shape[0] // NM if head else 0
    n_mlp = n_ffn * NM
    n_qkv = 6
    ring = dsend.shape[0]
    n_items = drecv.shape[0]

    def after_ring(s, action):
        if isinstance(s, int):
            if s >= ring:
                action()
        else:
            pl.when(s >= ring)(action)

    barrier = pltpu.get_barrier_semaphore()
    for peer in ({'x': d1}, {'x': d2}, {'x': d3}, {'y': 1 - yy}):
        pl.semaphore_signal(barrier, inc=1, device_id=peer, device_id_type=MESH)

    def remote(src, dst, ss, rs, peer):
        return pltpu.make_async_remote_copy(src_ref=src, dst_ref=dst, send_sem=ss, recv_sem=rs, device_id=peer, device_id_type=MESH)

    def attn_own(m):
        return pltpu.make_async_copy(attn_in.at[pl.ds(m * R, R)], attn_all.at[m, pl.ds(0, R)], a_sem.at[m])
    if head:
        for m in range(NM):
            attn_own(m).start()

    def hid_copy(m, k):
        row = pl.multiple_of(quarter[k] * (NM * R) + m * R, R)
        return pltpu.make_async_copy(hid_in.at[pl.ds(row, R)], h_buf.at[m, pl.ds(k * R, R)], h_sem.at[m, k])

    for m in range(NM):
        for k in range(4):
            hid_copy(m, k).start()
    gain_copies = []
    if head:
        gain_copies.append(pltpu.make_async_copy(g_mlp_in, gain_buf.at[0], gain_sem.at[0]))
    if tail:
        gain_copies.append(pltpu.make_async_copy(g_attn_in, gain_buf.at[1], gain_sem.at[1]))
    for cp in gain_copies:
        cp.start()

    def wgu_copy(j):
        off = pl.multiple_of(j * CW, CW)
        return (pltpu.make_async_copy(wg_in.at[:, pl.ds(off, CW)], wgu_buf.at[j, :, pl.ds(0, CW)], wgu_sem.at[0, j]),
                pltpu.make_async_copy(wu_in.at[:, pl.ds(off, CW)], wgu_buf.at[j, :, pl.ds(CW, CW)], wgu_sem.at[1, j]))

    if head:
        wo_copy = pltpu.make_async_copy(wo_in, wo_buf, wo_sem)
        wd_copy = pltpu.make_async_copy(wd_in, wd_buf, wd_sem)
    if tail:
        wqkv_copies = [pltpu.make_async_copy(wq_in.at[:, pl.ds(j * IW, IW)], wqkv_buf.at[j], wqkv_sem.at[j]) for j in range(4)]
        wqkv_copies += [pltpu.make_async_copy(w, wqkv_buf.at[j], wqkv_sem.at[j]) for j, w in ((4, wk_in), (5, wv_in))]
    def start_wgu(j, c):
        for cp in wgu_copy(j):
            cp.start()
        return c
    if head:
        wo_copy.start()
    else:
        for cp in wqkv_copies:
            cp.start()

    def pref_copy(blk, c):
        seqs = pl.ds(blk * SB, SB)
        return pltpu.make_async_copy((k_in, v_in)[c].at[seqs], pref_out.at[blk, c], pref_sem.at[blk, c])
    def pref_start():
        for blk in range(n_pref):
            for c in (0, 1):
                pref_copy(blk, c).start()

    def diag():
        return lax.broadcasted_iota(jnp.int32, (R, 128), 0) == lax.broadcasted_iota(jnp.int32, (R, 128), 1)

    def stat_send(kind, m, a):
        peer = (None, d1, d2, d3)[a]
        return remote(stat_buf.at[kind, m, 0], stat_buf.at[kind, m, a], st_ss.at[kind, m, a - 1], st_rs.at[kind, m, a - 1], {'x': peer})

    def stats_start(kind, m):
        for k in range(4):
            hv = h_buf[m, pl.ds(k * R, R), :].astype(F32)
            row_sum = jnp.sum(hv * hv, axis=1, keepdims=True)
            stat_buf[kind, m, 0, pl.ds(k, 1), :] = jnp.sum(jnp.where(diag(), row_sum, 0.0), axis=0, keepdims=True)
        for a in (1, 2, 3):
            stat_send(kind, m, a).start()

    def norm(kind, m, gain):
        for a in (1, 2, 3):
            stat_send(kind, m, a).wait()
        gain_row = gain.astype(F32)
        for k in range(4):
            total = stat_buf[kind, m, 0, pl.ds(k, 1), :]
            for a in (1, 2, 3):
                total = total + stat_buf[kind, m, a, pl.ds(POS[MASK[k] ^ a], 1), :]
            col = jnp.sum(jnp.where(diag(), total, 0.0), axis=1, keepdims=True)
            hv = h_buf[m, pl.ds(k * R, R), :].astype(F32)
            n_buf[m, pl.ds(k * R, R), :] = (hv * lax.rsqrt(col / model_dim + NORM_EPS) * gain_row).astype(BF16)

    def d_copy(s):
        return remote(dsend.at[lax.rem(s, ring)], drecv.at[s], d_ss.at[s], d_rs.at[s], {'x': d1})

    def x_copy(s):
        return remote(xsend.at[lax.rem(s, ring)], xrecv.at[s], x_ss.at[s], x_rs.at[s], {'x': d2})

    def stage1_math(s, m, w):
        part = dot(n_buf[m], w)
        keep_buf[lax.rem(s, keep_buf.shape[0])] = part[:2 * R]
        dsend[lax.rem(s, ring)] = part[2 * R:].astype(BF16)

    def stage1(s, m, w):
        after_ring(s, lambda: d_copy(s - ring).wait_send())
        stage1_math(s, m, w)
        d_copy(s).start()

    def stage2_wait(s):
        d_copy(s).wait_recv()
        after_ring(s, lambda: x_copy(s - ring).wait_send())

    def stage2_math(s):
        slot = lax.rem(s, keep_buf.shape[0])
        xsend[lax.rem(s, ring)] = (keep_buf[slot, pl.ds(R, R), :] + drecv[s, pl.ds(R, R), :].astype(F32)).astype(BF16)
        own_buf[lax.rem(s, own_buf.shape[0])] = keep_buf[slot, pl.ds(0, R), :] + drecv[s, pl.ds(0, R), :].astype(F32)

    def stage2(s):
        stage2_wait(s)
        stage2_math(s)
        x_copy(s).start()

    def stage3_sum(s):
        return (own_buf[lax.rem(s, own_buf.shape[0])] + xrecv[s].astype(F32)).astype(BF16)

    def stage3(s):
        x_copy(s).wait_recv()
        return stage3_sum(s)

    def gather_copies(buf, i, ss, rs):
        own, other = buf.at[i, pl.ds(0, R)], buf.at[i, pl.ds(R, R)]
        return (lambda: remote(own, buf.at[i, pl.ds(2 * R, R)], ss.at[0, i], rs.at[0, i], {'x': d1}),
                lambda: remote(own, buf.at[i, pl.ds(R, R)], ss.at[1, i], rs.at[1, i], {'x': d2}),
                lambda: remote(other, buf.at[i, pl.ds(3 * R, R)], ss.at[2, i], rs.at[2, i], {'x': d1}))

    def attn_copies(m):
        return gather_copies(attn_all, m, ag_ss, ag_rs)

    def y_copy(kind, m, half):
        rows = pl.ds(half * 2 * R, 2 * R)
        return remote(y_send.at[kind, m, rows], y_recv.at[kind, m, rows], y_ss.at[kind, m, half], y_rs.at[kind, m, half], {'y': 1 - yy})

    def attn_half(m, half):
        rows = jnp.concatenate([attn_all[m, pl.ds(k * R, R), :] for k in HALVES[half]], axis=0)
        y_send[0, m, pl.ds(half * 2 * R, 2 * R), :] = dot(rows, wo_buf[...]).astype(BF16)
        y_copy(0, m, half).start()

    def attn_finish(m):
        for half in (0, 1):
            y_copy(0, m, half).wait()
            for i, k in enumerate(HALVES[half]):
                here, there = pl.ds(k * R, R), pl.ds((half * 2 + i) * R, R)
                total = (y_send[0, m, there, :].astype(F32) + y_recv[0, m, there, :].astype(F32)).astype(BF16)
                h_buf[m, here, :] = (h_buf[m, here, :].astype(F32) + total.astype(F32)).astype(BF16)

    def mlp_start(m):
        y_send[1, m] = acc_buf[m].astype(BF16)
        for half in (0, 1):
            y_copy(1, m, half).start()

    def mlp_finish(m):
        for half in (0, 1):
            y_copy(1, m, half).wait()
            rows = pl.ds(half * 2 * R, 2 * R)
            total = (y_send[1, m, rows, :].astype(F32) + y_recv[1, m, rows, :].astype(F32)).astype(BF16)
            h_buf[m, rows, :] = (h_buf[m, rows, :].astype(F32) + total.astype(F32)).astype(BF16)

    def act_copies(t):
        return gather_copies(act_all, t, act_ss, act_rs)

    def out_copy(m, k):
        row = pl.multiple_of(quarter[k] * (NM * R) + m * R, R)
        return pltpu.make_async_copy(h_buf.at[m, pl.ds(k * R, R)], hid_out.at[pl.ds(row, R)], o_sem.at[m, k])

    def mid_ready(m):
        attn_finish(m)
        stats_start(0, m)

    def layer_done(m):
        mlp_finish(m)
        if tail:
            stats_start(1, m)
        for k in range(4):
            out_copy(m, k).start()

    def split(t):
        return (0, t) if NM == 1 else (lax.div(t, n_ffn), lax.rem(t, n_ffn))

    def mlp_iter(t, steady):
        def stage(first, action):
            if steady:
                action()
            else:
                pl.when((t >= first) & (t < n_mlp + first))(action)

        def relay_on():
            _, to_chip, relay = act_copies(t - O4)
            to_chip().wait_recv()
            relay().start()

        def act_ready():
            to_core, _, relay = act_copies(t - O5)
            to_core().wait_recv()
            relay().wait_recv()

        @pl.when(t < n_ffn)
        def _():
            for cp in wgu_copy(t):
                cp.wait()
        stage(O4, relay_on)
        stage(O2, lambda: stage2_wait(t - O2))
        stage(O3, lambda: x_copy(t - O3).wait_recv())
        stage(O5, act_ready)
        stage(0, lambda: after_ring(t, lambda: d_copy(t - ring).wait_send()))

        def activate():
            s = t - O3
            full = stage3_sum(s)
            gate, up = full[:, :CW].astype(F32), full[:, CW:].astype(F32)
            act_all[s, pl.ds(0, R), :] = (jax.nn.silu(gate) * up).astype(BF16)

        def product():
            m, j = split(t)
            stage1_math(t, m, wgu_buf[j])

        def down():
            s = t - O5
            m, j = split(s)
            acc_buf[m] += dot(act_all[s], wd_buf[pl.ds(pl.multiple_of(j * CW, CW), CW), :])

        def send_act():
            to_core, to_chip, _ = act_copies(t - O3)
            to_chip().start()
            to_core().start()

        stage(O2, lambda: stage2_math(t - O2))
        stage(O3, activate)
        stage(0, product)
        stage(O5, down)
        stage(O2, lambda: x_copy(t - O2).start())
        stage(O3, send_act)
        stage(0, lambda: d_copy(t).start())

    pl.semaphore_wait(barrier, 4)
    for cp in gain_copies:
        cp.wait()

    if head:
        for m in range(NM):
            attn_own(m).wait()
            to_core, to_chip, _ = attn_copies(m)
            to_chip().start()
            to_core().start()
            acc_buf[m] = jnp.zeros(acc_buf.shape[1:], F32)
        for m in range(NM):
            for k in range(4):
                hid_copy(m, k).wait()
        wo_copy.wait()
        lax.fori_loop(0, n_ffn, start_wgu, 0)
        wd_copy.start()
        if tail:
            for cp in wqkv_copies:
                cp.start()
        for m in range(NM):
            attn_copies(m)[0]().wait_recv()
            attn_half(m, 0)
        for m in range(NM):
            _, to_chip, relay = attn_copies(m)
            to_chip().wait_recv()
            relay().start()
            relay().wait_recv()
            attn_half(m, 1)
        mid_ready(0)
        norm(0, 0, gain_buf[0, pl.ds(layer, 1), :])
        if tail:
            pref_start()
        events = {}

        def at(t, action, *operands):
            events.setdefault(t, []).append(functools.partial(action, *operands))
        for m in range(1, NM):
            at((m - 1) * n_ffn + E1, mid_ready, m)
            at((m - 1) * n_ffn + E2, lambda m: norm(0, m, gain_buf[0, pl.ds(layer, 1), :]), m)
        for m in range(NM - 1):
            done = (m + 1) * n_ffn - 1 + O5
            at(done, mlp_start, m)
            at(min(done + E3, n_mlp + O5 - 2), layer_done, m)
            if tail:
                at(min(done + E4, n_mlp + O5 - 1), lambda m: norm(1, m, gain_buf[1, pl.ds(tail_layer, 1), :]), m)

        def body(steady, t, c):
            mlp_iter(t, steady)
            for when, actions in events.items():
                @pl.when(t == when)
                def _(actions=actions):
                    for action in actions:
                        action()
            return c
        lax.fori_loop(0, O5, functools.partial(body, False), 0)
        wd_copy.wait()
        lax.fori_loop(O5, n_mlp, functools.partial(body, True), 0)
        lax.fori_loop(n_mlp, n_mlp + O5, functools.partial(body, False), 0)
        mlp_start(NM - 1)
        if not tail:
            layer_done(NM - 1)
    else:
        for m in range(NM):
            for k in range(4):
                hid_copy(m, k).wait()
            stats_start(1, m)

    if tail:
        for cp in wqkv_copies:
            cp.wait()
        if not head:
            pref_start()

        def qkv_send(m):
            first = n_mlp + m * n_qkv
            for t in range(n_qkv + QKV_LAG):
                if t < n_qkv:
                    stage1(first + t, m, wqkv_buf[t])
                if t >= QKV_LAG:
                    stage2(first + t - QKV_LAG)

        def qkv_take(m):
            for j in range(n_qkv):
                qkv_out[j, pl.ds(m * R, R), :] = stage3(n_mlp + m * n_qkv + j)

        last = NM - 1
        for m in range(last):
            qkv_send(m)
        if head:
            layer_done(last)
        for m in range(last):
            qkv_take(m)
        norm(1, last, gain_buf[1, pl.ds(tail_layer, 1), :])
        qkv_send(last)
        qkv_take(last)

    if tail:
        for blk in range(n_pref):
            for c in (0, 1):
                pref_copy(blk, c).wait()

    def drain(s, c):
        d_copy(s).wait_send()
        x_copy(s).wait_send()
        return c
    lax.fori_loop(max(n_items - ring, 0), n_items, drain, 0)
    if head:
        def drain_act(s, c):
            for cp in act_copies(s):
                cp().wait_send()
            return c
        lax.fori_loop(0, n_mlp, drain_act, 0)
        for m in range(NM):
            for cp in attn_copies(m):
                cp().wait_send()
            for k in range(4):
                out_copy(m, k).wait()


def chain_call(head, tail, layer, cid, n_pref, vmem_mib, model_dim, hidden, attn=None, g_mlp=None, wo=None, wg=None, wu=None, wd=None, g_attn=None, wq=None, wk=None, wv=None, k_rows=None, v_rows=None):
    batch, feat = hidden.shape
    NM = groups(head)
    M = batch // NM
    R = M // 4
    vmem = pl.BlockSpec(memory_space=pltpu.VMEM)
    hbm = pl.BlockSpec(memory_space=pltpu.HBM)
    args, in_specs = [in_hbm(hidden)], [hbm]
    out_shape, out_specs = [], []
    n_items = 0
    if head:
        args += [attn, in_hbm(g_mlp), in_hbm(wo), in_hbm(wg), in_hbm(wu), in_hbm(wd)]
        in_specs += [hbm] * 6
        out_shape.append(jax.ShapeDtypeStruct(hidden.shape, hidden.dtype))
        out_specs.append(hbm)
        n_ffn = wg.shape[2] // CW
        n_items += n_ffn * NM
    if tail:
        args += [in_hbm(g_attn), in_hbm(wq), in_hbm(wk), in_hbm(wv), in_hbm(k_rows), in_hbm(v_rows)]
        in_specs += [hbm] * 6
        out_shape.append(jax.ShapeDtypeStruct((6, batch // 4, IW), BF16))
        out_specs.append(vmem)
        out_shape.append(pltpu.VMEM((n_pref, 2, SB) + k_rows.shape[2:], BF16))
        out_specs.append(vmem)
        n_items += 6 * NM
    dma = pltpu.SemaphoreType.DMA
    scratch = [
        pltpu.VMEM((NM, M, feat), BF16), pltpu.VMEM((NM, M, feat), BF16), pltpu.VMEM((2, NM, 4, 8, 128), F32),
        pltpu.VMEM((max(O2, QKV_LAG) + 1, 2 * R, IW), F32), pltpu.VMEM((max(O3 - O2 + 1, 6), R, IW), F32),
        pltpu.VMEM((RING, 2 * R, IW), BF16), pltpu.VMEM((n_items, 2 * R, IW), BF16),
        pltpu.VMEM((RING, R, IW), BF16), pltpu.VMEM((n_items, R, IW), BF16),
        pltpu.VMEM((2,) + (g_mlp if head else g_attn).shape, BF16), dma((2,)),
        dma((NM, 4)), dma((2, NM, 3)), dma((2, NM, 3)), dma((n_items,)), dma((n_items,)), dma((n_items,)), dma((n_items,))]
    if head:
        scratch += [
            pltpu.VMEM((NM, M, attn.shape[1]), BF16), pltpu.VMEM(wo.shape[1:], BF16), pltpu.VMEM((n_ffn, feat, IW), BF16),
            pltpu.VMEM(wd.shape[1:], BF16), pltpu.VMEM((NM, M, feat), F32), pltpu.VMEM((n_ffn * NM, M, CW), BF16),
            pltpu.VMEM((2, NM, M, feat), BF16), pltpu.VMEM((2, NM, M, feat), BF16),
            dma((3, NM)), dma((3, NM)), dma((2, NM, 2)), dma((2, NM, 2)), dma((3, n_ffn * NM)), dma((3, n_ffn * NM)),
            dma, dma((2, n_ffn)), dma, dma((NM, 4)), dma((NM,))]
    if tail:
        scratch += [pltpu.VMEM((6, feat, IW), BF16), dma((6,)), dma((n_pref, 2))]
    return pl.pallas_call(
        functools.partial(chain_kernel, head, tail, layer, n_pref, model_dim),
        out_shape=out_shape, in_specs=in_specs, out_specs=out_specs, scratch_shapes=scratch,
        name=f'chain_{int(head)}{int(tail)}',
        compiler_params=pltpu.CompilerParams(collective_id=cid, has_side_effects=True, vmem_limit_bytes=vmem_mib * 1024 * 1024),
    )(*args)


def attn_kernel(layer, n_pref, pos_hbm, qkv_hbm, cos_hbm, sin_hbm, qg_hbm, kg_hbm, k_hbm, v_hbm, *refs):
    k_out, v_out, o_ref, pref, kv_slots, q_buf, kv_buf, o_buf, s_buf, p_buf, qkv_ref, tabs_ref, pos_ref, gain_ref, in_sem, out_sem, small_sem = refs[-17:]
    small = (pltpu.make_async_copy(qkv_hbm, qkv_ref, small_sem.at[0]), pltpu.make_async_copy(cos_hbm, tabs_ref.at[0], small_sem.at[1]), pltpu.make_async_copy(sin_hbm, tabs_ref.at[1], small_sem.at[5]),
             pltpu.make_async_copy(pos_hbm, pos_ref, small_sem.at[2]),
             pltpu.make_async_copy(qg_hbm, gain_ref.at[0], small_sem.at[3]), pltpu.make_async_copy(kg_hbm, gain_ref.at[1], small_sem.at[4]))
    for cp in small:
        cp.start()
    local = o_ref.shape[0]
    n_q = q_buf.shape[0] // local
    n_kv = kv_buf.shape[1] // local
    n_rows = k_hbm.shape[2]
    group = n_q // n_kv
    per_chunk = qkv_ref.shape[2] // HEAD_DIM
    n_blocks = local // SB

    def held(blk, early):
        return pref.at[blk] if early else kv_slots.at[lax.rem(blk - n_pref, NBUF)]

    def run(blk, early, out, wait):
        seqs = pl.ds(blk * SB, SB)
        for c in (0, 1):
            here = held(blk, early).at[c]
            if out:
                cp = pltpu.make_async_copy(here, (k_out, v_out)[c].at[layer, seqs], out_sem.at[blk, c])
            else:
                cp = pltpu.make_async_copy((k_hbm, v_hbm)[c].at[layer, seqs], here, in_sem.at[blk, c])
            cp.wait() if wait else cp.start()

    for blk in range(n_pref, min(n_pref + NBUF, n_blocks)):
        run(blk, False, False, False)

    def head_of(idx):
        return qkv_ref[idx // per_chunk, :, pl.ds((idx % per_chunk) * HEAD_DIM, HEAD_DIM)].astype(F32)

    for cp in small:
        cp.wait()
    cos_tab, sin_tab = tabs_ref[0], tabs_ref[1]
    gains = [gain_ref[i, pl.ds(layer, 1), :].astype(F32) for i in (0, 1)]

    def norm_rope(vals, gain):
        normed = vals * lax.rsqrt(jnp.mean(vals * vals, axis=-1, keepdims=True) + NORM_EPS) * gain
        return (normed * cos_tab + pltpu.roll(normed, HEAD_DIM // 2, 1) * sin_tab).astype(BF16).astype(F32)
    for h in range(n_kv):
        kv_buf[0, pl.ds(h * local, local), :] = norm_rope(head_of(n_q + h), gains[1])
        kv_buf[1, pl.ds(h * local, local), :] = head_of(n_q + n_kv + h)

    row_ids = lax.broadcasted_iota(jnp.int32, (16, HEAD_DIM), 0)
    lane_ids = lax.broadcasted_iota(jnp.int32, (n_q, n_rows), 1)
    head_hit = lax.rem(lane_ids, n_kv) == lax.div(lax.broadcasted_iota(jnp.int32, (n_q, n_rows), 0), group)
    lane_of = jnp.where(head_hit, lane_ids, n_rows)

    def patch(blk, early):
        ref = held(blk, early)
        for i in range(SB):
            b = blk * SB + i
            row = pos_ref[b] * n_kv
            base = pl.multiple_of(lax.div(row, 16) * 16, 16)
            hit = lax.div(row_ids, n_kv) == lax.div(row - base, n_kv)
            for c in (0, 1):
                new = kv_buf[c, pl.ds(b, n_kv, stride=local), :]
                new = jnp.concatenate([new] * (16 // n_kv), axis=0)
                old = ref[c, i, pl.ds(base, 16), :]
                ref[c, i, pl.ds(base, 16), :] = jnp.where(hit, new, old.astype(F32)).astype(BF16)

    for blk in range(min(AHEAD, n_pref)):
        patch(blk, True)
    for h in range(n_q):
        q_buf[pl.ds(h * local, local), :] = norm_rope(head_of(h), gains[0])
    for blk in range(min(AHEAD, n_pref)):
        run(blk, True, True, False)

    def block_step(blk, early, nxt, nxt_early):
        ref = held(blk, early)
        if nxt is not None:
            if not nxt_early:
                run(nxt, False, False, True)
            patch(nxt, nxt_early)
        for i in range(SB):
            q = q_buf[pl.ds(blk * SB + i, n_q, stride=local), :].astype(BF16)
            s_buf[i] = lax.dot_general(q, ref[0, i], (((1,), (1,)), ((), ())), preferred_element_type=F32)
        if nxt is not None:
            run(nxt, nxt_early, True, False)
        for i in range(SB):
            row = pos_ref[blk * SB + i] * n_kv
            scores = jnp.where(lane_of < row + n_kv, s_buf[i] * (HEAD_DIM ** -0.5), -1e30)
            e = jnp.exp(scores - jnp.max(scores, axis=-1, keepdims=True))
            p_buf[i] = (e / jnp.sum(e, axis=-1, keepdims=True)).astype(BF16)
        for i in range(SB):
            o_buf[pl.ds(blk * SB + i, n_q, stride=local), :] = dot(p_buf[i], ref[1, i])

    def early_step(blk, carry):
        block_step(blk, True, blk + AHEAD, True)
        return carry
    lax.fori_loop(0, n_pref - AHEAD, early_step, 0)
    for blk in range(n_pref - AHEAD, n_blocks):
        nxt = blk + AHEAD if blk + AHEAD < n_blocks else None
        block_step(blk, blk < n_pref, nxt, False)

    for h in range(n_q):
        o_ref[:, pl.ds(h * HEAD_DIM, HEAD_DIM)] = o_buf[pl.ds(h * local, local), :].astype(BF16)
    for blk in range(n_pref):
        run(blk, True, True, True)
    for blk in range(max(n_blocks - NBUF, n_pref), n_blocks):
        run(blk, False, True, True)


def attn_call(layer, pos, qkv, cos_tab, sin_tab, q_gain, k_gain, k_cache, v_cache, pref, prev):
    layers, local, n_rows, _ = k_cache.shape
    n_kv = 4
    n_q = 16
    vmem = pl.BlockSpec(memory_space=pltpu.VMEM)
    hbm = pl.BlockSpec(memory_space=pltpu.HBM)
    args = [in_hbm(pos), qkv if layer == 0 else in_hbm(qkv), in_hbm(cos_tab), in_hbm(sin_tab), in_hbm(q_gain), in_hbm(k_gain), in_hbm(k_cache), in_hbm(v_cache), pltpu.with_memory_space_constraint(pref, pltpu.VMEM)]
    in_specs = [hbm] * 8 + [vmem]
    aliases = {8: 3}
    n_pref, n_blocks = pref.shape[0], local // SB
    if prev is not None:
        args += list(prev)
        in_specs += [hbm] * 2
        aliases.update({9: 0, 10: 1})
    return pl.pallas_call(
        functools.partial(attn_kernel, layer, n_pref),
        out_shape=[jax.ShapeDtypeStruct(k_cache.shape, BF16)] * 2 + [jax.ShapeDtypeStruct((local, n_q * HEAD_DIM), BF16), jax.ShapeDtypeStruct(pref.shape, BF16)],
        in_specs=in_specs,
        out_specs=[hbm, hbm, vmem, vmem],
        scratch_shapes=[pltpu.VMEM((min(NBUF, max(n_blocks - n_pref, 1)) if n_pref < n_blocks else 1, 2, SB if n_pref < n_blocks else 1, n_rows, HEAD_DIM), BF16),
                        pltpu.VMEM((n_q * local, HEAD_DIM), F32), pltpu.VMEM((2, n_kv * local, HEAD_DIM), F32), pltpu.VMEM((n_q * local, HEAD_DIM), F32),
                        pltpu.VMEM((SB, n_q, n_rows), F32), pltpu.VMEM((SB, n_q, n_rows), BF16),
                        pltpu.VMEM(qkv.shape, BF16), pltpu.VMEM((2,) + cos_tab.shape, F32), pltpu.SMEM(pos.shape, jnp.int32), pltpu.VMEM((2,) + q_gain.shape, BF16),
                        pltpu.SemaphoreType.DMA((n_blocks, 2)), pltpu.SemaphoreType.DMA((n_blocks, 2)), pltpu.SemaphoreType.DMA((6,))],
        input_output_aliases=aliases, name=f'attn_{layer}',
        compiler_params=pltpu.CompilerParams(vmem_limit_bytes=(20 if layer == 0 else 22) * 1024 * 1024),
    )(*args)


def solution(mesh):
    group_size = mesh.shape['x']
    cache_spec = P(None, ('dp', 'x'), None, 'y', None)
    col_spec = P(None, 'x', 'y')
    row_spec = P(None, 'y', 'x')
    in_specs = (P('dp', 'x'), P('dp'), cache_spec, cache_spec, P(None, 'x'), P(None, 'x'), P(), P(), col_spec, col_spec, col_spec, row_spec, col_spec, col_spec, row_spec)
    out_specs = (P('dp', 'x'), cache_spec, cache_spec)

    def device_step(hidden, positions, k_cache, v_cache, g_attn, g_mlp, q_gain, k_gain, w_q, w_k, w_v, w_o, w_gate, w_up, w_down):
        model_dim = hidden.shape[1] * group_size
        layers, local, cache_len, n_kv, _ = k_cache.shape
        my_pos = lax.dynamic_slice_in_dim(positions, lax.axis_index('x') * local, local)
        half = HEAD_DIM // 2
        inv_freq = np.power(ROPE_BASE, -2.0 * np.arange(half) / HEAD_DIM).astype(np.float32)
        angles = my_pos.astype(F32)[:, None] * jnp.asarray(np.concatenate([inv_freq, inv_freq]))[None, :]
        sign = jnp.asarray(np.repeat(np.array([-1.0, 1.0], np.float32), half))
        cos_tab, sin_tab = jnp.cos(angles), jnp.sin(angles) * sign[None, :]
        cos_tab, sin_tab, my_pos, hidden = lax.optimization_barrier((cos_tab, sin_tab, my_pos, hidden))
        k_rows = k_cache.reshape(layers, local, cache_len * n_kv, HEAD_DIM)
        v_rows = v_cache.reshape(layers, local, cache_len * n_kv, HEAD_DIM)
        attn_tabs = (cos_tab, sin_tab, q_gain, k_gain, k_rows, v_rows)
        caches = {'k_rows': k_rows, 'v_rows': v_rows}
        qkv, pref = chain_call(False, True, 0, 0, 8, 16, model_dim, hidden, g_attn=g_attn, wq=w_q, wk=w_k, wv=w_v, **caches)
        k_new, v_new, attn, _ = attn_call(0, my_pos, qkv, *attn_tabs, pref, None)
        hidden, qkv, pref = chain_call(True, True, 0, 1, 5, 40, model_dim, hidden, attn, g_mlp, w_o, w_gate, w_up, w_down, g_attn, w_q, w_k, w_v, **caches)
        k_new, v_new, attn, _ = attn_call(1, my_pos, qkv, *attn_tabs, pref, (k_new, v_new))
        (hidden,) = chain_call(True, False, 1, 2, 0, 46, model_dim, hidden, attn, g_mlp, w_o, w_gate, w_up, w_down)
        return hidden, k_new.reshape(k_cache.shape), v_new.reshape(v_cache.shape)

    return jax.shard_map(device_step, mesh=mesh, in_specs=in_specs, out_specs=out_specs, check_vma=False)
```

```python
import functools

import jax
import jax.numpy as jnp
import numpy as np
from jax import lax
from jax.experimental import pallas as pl
from jax.experimental.pallas import tpu as pltpu
from jax.sharding import PartitionSpec as P

HEAD_DIM = 128
NORM_EPS = 1e-6
ROPE_BASE = 1000000.0
MESH = pl.DeviceIdType.MESH
BF16 = jnp.bfloat16
F32 = jnp.float32

CW = 256
IW = 2 * CW
O2, O3, O4, O5 = 2, 8, 14, 16
E1, E2, E3, E4 = 6, 12, 8, 14
QKV_LAG = 2
HEAD_GROUPS = 2
RING = 8
SB = 8
AHEAD = 2
NBUF = 3
MASK = (0, 2, 1, 3)
POS = (0, 2, 1, 3)
HALVES = ((0, 2), (1, 3))


def in_hbm(x):
    return pltpu.with_memory_space_constraint(x, pltpu.HBM)


def groups(head):
    return HEAD_GROUPS if head else 1


def dot(a, b):
    return jnp.dot(a, b, preferred_element_type=F32)


def chain_kernel(head, tail, layer, n_pref, model_dim, *refs):
    NM = groups(head)
    it = iter(refs)
    hid_in = next(it)
    if head:
        attn_in, g_mlp_in = next(it), next(it)
        wo_in, wg_in, wu_in, wd_in = (next(it).at[layer] for _ in range(4))
    if tail:
        tail_layer = layer + 1 if head else layer
        g_attn_in = next(it)
        wq_in, wk_in, wv_in, k_in, v_in = (next(it).at[tail_layer] for _ in range(5))
    if head:
        hid_out = next(it)
    if tail:
        qkv_out, pref_out = next(it), next(it)
    h_buf, n_buf, stat_buf, keep_buf, own_buf, dsend, drecv, xsend, xrecv = (next(it) for _ in range(9))
    gain_buf, gain_sem = next(it), next(it)
    h_sem, st_ss, st_rs, d_ss, d_rs, x_ss, x_rs = (next(it) for _ in range(7))
    if head:
        attn_all, wo_buf, wgu_buf, wd_buf, acc_buf, act_all, y_send, y_recv = (next(it) for _ in range(8))
        ag_ss, ag_rs, y_ss, y_rs, act_ss, act_rs, wo_sem, wgu_sem, wd_sem, o_sem, a_sem = (next(it) for _ in range(11))
    if tail:
        wqkv_buf, wqkv_sem, pref_sem = (next(it) for _ in range(3))

    me = lax.axis_index('x')
    yy = lax.axis_index('y')
    chip, core = lax.div(me, 2), lax.rem(me, 2)
    d1 = chip * 2 + (1 - core)
    d2 = (1 - chip) * 2 + core
    d3 = (1 - chip) * 2 + (1 - core)
    quarter = (me, d2, d1, d3)
    R = h_buf.shape[1] // 4
    M = 4 * R
    n_ffn = act_all.shape[0] // NM if head else 0
    n_mlp = n_ffn * NM
    n_qkv = 6
    ring = dsend.shape[0]
    n_items = drecv.shape[0]

    def after_ring(s, action):
        if isinstance(s, int):
            if s >= ring:
                action()
        else:
            pl.when(s >= ring)(action)

    barrier = pltpu.get_barrier_semaphore()
    for peer in ({'x': d1}, {'x': d2}, {'x': d3}, {'y': 1 - yy}):
        pl.semaphore_signal(barrier, inc=1, device_id=peer, device_id_type=MESH)

    def remote(src, dst, ss, rs, peer):
        return pltpu.make_async_remote_copy(src_ref=src, dst_ref=dst, send_sem=ss, recv_sem=rs, device_id=peer, device_id_type=MESH)

    def attn_own(m):
        return pltpu.make_async_copy(attn_in.at[pl.ds(m * R, R)], attn_all.at[m, pl.ds(0, R)], a_sem.at[m])
    if head:
        for m in range(NM):
            attn_own(m).start()

    def hid_copy(m, k):
        row = pl.multiple_of(quarter[k] * (NM * R) + m * R, R)
        return pltpu.make_async_copy(hid_in.at[pl.ds(row, R)], h_buf.at[m, pl.ds(k * R, R)], h_sem.at[m, k])

    for m in range(NM):
        for k in range(4):
            hid_copy(m, k).start()
    gain_copies = []
    if head:
        gain_copies.append(pltpu.make_async_copy(g_mlp_in, gain_buf.at[0], gain_sem.at[0]))
    if tail:
        gain_copies.append(pltpu.make_async_copy(g_attn_in, gain_buf.at[1], gain_sem.at[1]))
    for cp in gain_copies:
        cp.start()

    def wgu_copy(j):
        off = pl.multiple_of(j * CW, CW)
        return (pltpu.make_async_copy(wg_in.at[:, pl.ds(off, CW)], wgu_buf.at[j, :, pl.ds(0, CW)], wgu_sem.at[0, j]),
                pltpu.make_async_copy(wu_in.at[:, pl.ds(off, CW)], wgu_buf.at[j, :, pl.ds(CW, CW)], wgu_sem.at[1, j]))

    if head:
        wo_copy = pltpu.make_async_copy(wo_in, wo_buf, wo_sem)
        wd_copy = pltpu.make_async_copy(wd_in, wd_buf, wd_sem)
    if tail:
        wqkv_copies = [pltpu.make_async_copy(wq_in.at[:, pl.ds(j * IW, IW)], wqkv_buf.at[j], wqkv_sem.at[j]) for j in range(4)]
        wqkv_copies += [pltpu.make_async_copy(w, wqkv_buf.at[j], wqkv_sem.at[j]) for j, w in ((4, wk_in), (5, wv_in))]
    def start_wgu(j, c):
        for cp in wgu_copy(j):
            cp.start()
        return c
    if head:
        wo_copy.start()
    else:
        for cp in wqkv_copies:
            cp.start()

    def pref_copy(blk, c):
        seqs = pl.ds(blk * SB, SB)
        return pltpu.make_async_copy((k_in, v_in)[c].at[seqs], pref_out.at[blk, c], pref_sem.at[blk, c])
    def pref_start():
        for blk in range(n_pref):
            for c in (0, 1):
                pref_copy(blk, c).start()

    def diag():
        return lax.broadcasted_iota(jnp.int32, (R, 128), 0) == lax.broadcasted_iota(jnp.int32, (R, 128), 1)

    def stat_send(kind, m, a):
        peer = (None, d1, d2, d3)[a]
        return remote(stat_buf.at[kind, m, 0], stat_buf.at[kind, m, a], st_ss.at[kind, m, a - 1], st_rs.at[kind, m, a - 1], {'x': peer})

    def stats_start(kind, m):
        for k in range(4):
            hv = h_buf[m, pl.ds(k * R, R), :].astype(F32)
            row_sum = jnp.sum(hv * hv, axis=1, keepdims=True)
            stat_buf[kind, m, 0, pl.ds(k, 1), :] = jnp.sum(jnp.where(diag(), row_sum, 0.0), axis=0, keepdims=True)
        for a in (1, 2, 3):
            stat_send(kind, m, a).start()

    def norm(kind, m, gain):
        for a in (1, 2, 3):
            stat_send(kind, m, a).wait()
        gain_row = gain.astype(F32)
        for k in range(4):
            total = stat_buf[kind, m, 0, pl.ds(k, 1), :]
            for a in (1, 2, 3):
                total = total + stat_buf[kind, m, a, pl.ds(POS[MASK[k] ^ a], 1), :]
            col = jnp.sum(jnp.where(diag(), total, 0.0), axis=1, keepdims=True)
            hv = h_buf[m, pl.ds(k * R, R), :].astype(F32)
            n_buf[m, pl.ds(k * R, R), :] = (hv * lax.rsqrt(col / model_dim + NORM_EPS) * gain_row).astype(BF16)

    def d_copy(s):
        return remote(dsend.at[lax.rem(s, ring)], drecv.at[s], d_ss.at[s], d_rs.at[s], {'x': d1})

    def x_copy(s):
        return remote(xsend.at[lax.rem(s, ring)], xrecv.at[s], x_ss.at[s], x_rs.at[s], {'x': d2})

    def stage1_math(s, m, w):
        part = dot(n_buf[m], w)
        keep_buf[lax.rem(s, keep_buf.shape[0])] = part[:2 * R]
        dsend[lax.rem(s, ring)] = part[2 * R:].astype(BF16)

    def stage1(s, m, w):
        after_ring(s, lambda: d_copy(s - ring).wait_send())
        stage1_math(s, m, w)
        d_copy(s).start()

    def stage2_wait(s):
        d_copy(s).wait_recv()
        after_ring(s, lambda: x_copy(s - ring).wait_send())

    def stage2_math(s):
        slot = lax.rem(s, keep_buf.shape[0])
        xsend[lax.rem(s, ring)] = (keep_buf[slot, pl.ds(R, R), :] + drecv[s, pl.ds(R, R), :].astype(F32)).astype(BF16)
        own_buf[lax.rem(s, own_buf.shape[0])] = keep_buf[slot, pl.ds(0, R), :] + drecv[s, pl.ds(0, R), :].astype(F32)

    def stage2(s):
        stage2_wait(s)
        stage2_math(s)
        x_copy(s).start()

    def stage3_sum(s):
        return (own_buf[lax.rem(s, own_buf.shape[0])] + xrecv[s].astype(F32)).astype(BF16)

    def stage3(s):
        x_copy(s).wait_recv()
        return stage3_sum(s)

    def gather_copies(buf, i, ss, rs):
        own, other = buf.at[i, pl.ds(0, R)], buf.at[i, pl.ds(R, R)]
        return (lambda: remote(own, buf.at[i, pl.ds(2 * R, R)], ss.at[0, i], rs.at[0, i], {'x': d1}),
                lambda: remote(own, buf.at[i, pl.ds(R, R)], ss.at[1, i], rs.at[1, i], {'x': d2}),
                lambda: remote(other, buf.at[i, pl.ds(3 * R, R)], ss.at[2, i], rs.at[2, i], {'x': d1}))

    def attn_copies(m):
        return gather_copies(attn_all, m, ag_ss, ag_rs)

    def y_copy(kind, m, half):
        rows = pl.ds(half * 2 * R, 2 * R)
        return remote(y_send.at[kind, m, rows], y_recv.at[kind, m, rows], y_ss.at[kind, m, half], y_rs.at[kind, m, half], {'y': 1 - yy})

    def attn_half(m, half):
        rows = jnp.concatenate([attn_all[m, pl.ds(k * R, R), :] for k in HALVES[half]], axis=0)
        y_send[0, m, pl.ds(half * 2 * R, 2 * R), :] = dot(rows, wo_buf[...]).astype(BF16)
        y_copy(0, m, half).start()

    def attn_finish(m):
        for half in (0, 1):
            y_copy(0, m, half).wait()
            for i, k in enumerate(HALVES[half]):
                here, there = pl.ds(k * R, R), pl.ds((half * 2 + i) * R, R)
                total = (y_send[0, m, there, :].astype(F32) + y_recv[0, m, there, :].astype(F32)).astype(BF16)
                h_buf[m, here, :] = (h_buf[m, here, :].astype(F32) + total.astype(F32)).astype(BF16)

    def mlp_start(m):
        y_send[1, m] = acc_buf[m].astype(BF16)
        for half in (0, 1):
            y_copy(1, m, half).start()

    def mlp_finish(m):
        for half in (0, 1):
            y_copy(1, m, half).wait()
            rows = pl.ds(half * 2 * R, 2 * R)
            total = (y_send[1, m, rows, :].astype(F32) + y_recv[1, m, rows, :].astype(F32)).astype(BF16)
            h_buf[m, rows, :] = (h_buf[m, rows, :].astype(F32) + total.astype(F32)).astype(BF16)

    def act_copies(t):
        return gather_copies(act_all, t, act_ss, act_rs)

    def out_copy(m, k):
        row = pl.multiple_of(quarter[k] * (NM * R) + m * R, R)
        return pltpu.make_async_copy(h_buf.at[m, pl.ds(k * R, R)], hid_out.at[pl.ds(row, R)], o_sem.at[m, k])

    def mid_ready(m):
        attn_finish(m)
        stats_start(0, m)

    def layer_done(m):
        mlp_finish(m)
        if tail:
            stats_start(1, m)
        for k in range(4):
            out_copy(m, k).start()

    def split(t):
        return (0, t) if NM == 1 else (lax.div(t, n_ffn), lax.rem(t, n_ffn))

    def mlp_iter(t, steady):
        def stage(first, action):
            if steady:
                action()
            else:
                pl.when((t >= first) & (t < n_mlp + first))(action)

        def relay_on():
            _, to_chip, relay = act_copies(t - O4)
            to_chip().wait_recv()
            relay().start()

        def act_ready():
            to_core, _, relay = act_copies(t - O5)
            to_core().wait_recv()
            relay().wait_recv()

        @pl.when(t < n_ffn)
        def _():
            for cp in wgu_copy(t):
                cp.wait()
        stage(O4, relay_on)
        stage(O2, lambda: stage2_wait(t - O2))
        stage(O3, lambda: x_copy(t - O3).wait_recv())
        stage(O5, act_ready)
        stage(0, lambda: after_ring(t, lambda: d_copy(t - ring).wait_send()))

        def activate():
            s = t - O3
            full = stage3_sum(s)
            gate, up = full[:, :CW].astype(F32), full[:, CW:].astype(F32)
            act_all[s, pl.ds(0, R), :] = (jax.nn.silu(gate) * up).astype(BF16)

        def product():
            m, j = split(t)
            stage1_math(t, m, wgu_buf[j])

        def down():
            s = t - O5
            m, j = split(s)
            acc_buf[m] += dot(act_all[s], wd_buf[pl.ds(pl.multiple_of(j * CW, CW), CW), :])

        def send_act():
            to_core, to_chip, _ = act_copies(t - O3)
            to_chip().start()
            to_core().start()

        stage(O2, lambda: stage2_math(t - O2))
        stage(O3, activate)
        stage(0, product)
        stage(O5, down)
        stage(O2, lambda: x_copy(t - O2).start())
        stage(O3, send_act)
        stage(0, lambda: d_copy(t).start())

    pl.semaphore_wait(barrier, 4)
    for cp in gain_copies:
        cp.wait()

    if head:
        for m in range(NM):
            attn_own(m).wait()
            to_core, to_chip, _ = attn_copies(m)
            to_chip().start()
            to_core().start()
            acc_buf[m] = jnp.zeros(acc_buf.shape[1:], F32)
        for m in range(NM):
            for k in range(4):
                hid_copy(m, k).wait()
        wo_copy.wait()
        lax.fori_loop(0, n_ffn, start_wgu, 0)
        wd_copy.start()
        if tail:
            for cp in wqkv_copies:
                cp.start()
        for m in range(NM):
            attn_copies(m)[0]().wait_recv()
            attn_half(m, 0)
        for m in range(NM):
            _, to_chip, relay = attn_copies(m)
            to_chip().wait_recv()
            relay().start()
            relay().wait_recv()
            attn_half(m, 1)
        mid_ready(0)
        norm(0, 0, gain_buf[0, pl.ds(layer, 1), :])
        if tail:
            pref_start()
        events = {}

        def at(t, action, *operands):
            events.setdefault(t, []).append(functools.partial(action, *operands))
        for m in range(1, NM):
            at((m - 1) * n_ffn + E1, mid_ready, m)
            at((m - 1) * n_ffn + E2, lambda m: norm(0, m, gain_buf[0, pl.ds(layer, 1), :]), m)
        for m in range(NM - 1):
            done = (m + 1) * n_ffn - 1 + O5
            at(done, mlp_start, m)
            at(min(done + E3, n_mlp + O5 - 2), layer_done, m)
            if tail:
                at(min(done + E4, n_mlp + O5 - 1), lambda m: norm(1, m, gain_buf[1, pl.ds(tail_layer, 1), :]), m)

        def body(steady, t, c):
            mlp_iter(t, steady)
            for when, actions in events.items():
                @pl.when(t == when)
                def _(actions=actions):
                    for action in actions:
                        action()
            return c
        lax.fori_loop(0, O5, functools.partial(body, False), 0)
        wd_copy.wait()
        lax.fori_loop(O5, n_mlp, functools.partial(body, True), 0)
        lax.fori_loop(n_mlp, n_mlp + O5, functools.partial(body, False), 0)
        mlp_start(NM - 1)
        if not tail:
            layer_done(NM - 1)
    else:
        for m in range(NM):
            for k in range(4):
                hid_copy(m, k).wait()
            stats_start(1, m)

    if tail:
        for cp in wqkv_copies:
            cp.wait()
        if not head:
            pref_start()

        def qkv_send(m):
            first = n_mlp + m * n_qkv
            for t in range(n_qkv + QKV_LAG):
                if t < n_qkv:
                    stage1(first + t, m, wqkv_buf[t])
                if t >= QKV_LAG:
                    stage2(first + t - QKV_LAG)

        def qkv_take(m):
            for j in range(n_qkv):
                qkv_out[j, pl.ds(m * R, R), :] = stage3(n_mlp + m * n_qkv + j)

        last = NM - 1
        for m in range(last):
            qkv_send(m)
        if head:
            layer_done(last)
        for m in range(last):
            qkv_take(m)
        norm(1, last, gain_buf[1, pl.ds(tail_layer, 1), :])
        qkv_send(last)
        qkv_take(last)

    if tail:
        for blk in range(n_pref):
            for c in (0, 1):
                pref_copy(blk, c).wait()

    def drain(s, c):
        d_copy(s).wait_send()
        x_copy(s).wait_send()
        return c
    lax.fori_loop(max(n_items - ring, 0), n_items, drain, 0)
    if head:
        def drain_act(s, c):
            for cp in act_copies(s):
                cp().wait_send()
            return c
        lax.fori_loop(0, n_mlp, drain_act, 0)
        for m in range(NM):
            for cp in attn_copies(m):
                cp().wait_send()
            for k in range(4):
                out_copy(m, k).wait()


def chain_call(head, tail, layer, cid, n_pref, vmem_mib, model_dim, hidden, attn=None, g_mlp=None, wo=None, wg=None, wu=None, wd=None, g_attn=None, wq=None, wk=None, wv=None, k_rows=None, v_rows=None):
    batch, feat = hidden.shape
    NM = groups(head)
    M = batch // NM
    R = M // 4
    vmem = pl.BlockSpec(memory_space=pltpu.VMEM)
    hbm = pl.BlockSpec(memory_space=pltpu.HBM)
    args, in_specs = [in_hbm(hidden)], [hbm]
    out_shape, out_specs = [], []
    n_items = 0
    if head:
        args += [in_hbm(attn), in_hbm(g_mlp), in_hbm(wo), in_hbm(wg), in_hbm(wu), in_hbm(wd)]
        in_specs += [hbm] * 6
        out_shape.append(jax.ShapeDtypeStruct(hidden.shape, hidden.dtype))
        out_specs.append(hbm)
        n_ffn = wg.shape[2] // CW
        n_items += n_ffn * NM
    if tail:
        args += [in_hbm(g_attn), in_hbm(wq), in_hbm(wk), in_hbm(wv), in_hbm(k_rows), in_hbm(v_rows)]
        in_specs += [hbm] * 6
        out_shape.append(jax.ShapeDtypeStruct((6, batch // 4, IW), BF16))
        out_specs.append(vmem)
        out_shape.append(pltpu.VMEM((n_pref, 2, SB) + k_rows.shape[2:], BF16))
        out_specs.append(vmem)
        n_items += 6 * NM
    dma = pltpu.SemaphoreType.DMA
    scratch = [
        pltpu.VMEM((NM, M, feat), BF16), pltpu.VMEM((NM, M, feat), BF16), pltpu.VMEM((2, NM, 4, 8, 128), F32),
        pltpu.VMEM((max(O2, QKV_LAG) + 1, 2 * R, IW), F32), pltpu.VMEM((max(O3 - O2 + 1, 6), R, IW), F32),
        pltpu.VMEM((RING, 2 * R, IW), BF16), pltpu.VMEM((n_items, 2 * R, IW), BF16),
        pltpu.VMEM((RING, R, IW), BF16), pltpu.VMEM((n_items, R, IW), BF16),
        pltpu.VMEM((2,) + (g_mlp if head else g_attn).shape, BF16), dma((2,)),
        dma((NM, 4)), dma((2, NM, 3)), dma((2, NM, 3)), dma((n_items,)), dma((n_items,)), dma((n_items,)), dma((n_items,))]
    if head:
        scratch += [
            pltpu.VMEM((NM, M, attn.shape[1]), BF16), pltpu.VMEM(wo.shape[1:], BF16), pltpu.VMEM((n_ffn, feat, IW), BF16),
            pltpu.VMEM(wd.shape[1:], BF16), pltpu.VMEM((NM, M, feat), F32), pltpu.VMEM((n_ffn * NM, M, CW), BF16),
            pltpu.VMEM((2, NM, M, feat), BF16), pltpu.VMEM((2, NM, M, feat), BF16),
            dma((3, NM)), dma((3, NM)), dma((2, NM, 2)), dma((2, NM, 2)), dma((3, n_ffn * NM)), dma((3, n_ffn * NM)),
            dma, dma((2, n_ffn)), dma, dma((NM, 4)), dma((NM,))]
    if tail:
        scratch += [pltpu.VMEM((6, feat, IW), BF16), dma((6,)), dma((n_pref, 2))]
    return pl.pallas_call(
        functools.partial(chain_kernel, head, tail, layer, n_pref, model_dim),
        out_shape=out_shape, in_specs=in_specs, out_specs=out_specs, scratch_shapes=scratch,
        name=f'chain_{int(head)}{int(tail)}',
        compiler_params=pltpu.CompilerParams(collective_id=cid, has_side_effects=True, vmem_limit_bytes=vmem_mib * 1024 * 1024),
    )(*args)


def attn_kernel(layer, n_pref, pos_hbm, qkv_hbm, cos_hbm, sin_hbm, qg_hbm, kg_hbm, k_hbm, v_hbm, *refs):
    k_out, v_out, o_ref, pref, kv_slots, q_buf, kv_buf, o_buf, s_buf, p_buf, qkv_ref, tabs_ref, pos_ref, gain_ref, o_vmem, in_sem, out_sem, small_sem = refs[-18:]
    small = (pltpu.make_async_copy(qkv_hbm, qkv_ref, small_sem.at[0]), pltpu.make_async_copy(cos_hbm, tabs_ref.at[0], small_sem.at[1]), pltpu.make_async_copy(sin_hbm, tabs_ref.at[1], small_sem.at[5]),
             pltpu.make_async_copy(pos_hbm, pos_ref, small_sem.at[2]),
             pltpu.make_async_copy(qg_hbm, gain_ref.at[0], small_sem.at[3]), pltpu.make_async_copy(kg_hbm, gain_ref.at[1], small_sem.at[4]))
    for cp in small:
        cp.start()
    local = o_ref.shape[0]
    n_q = q_buf.shape[0] // local
    n_kv = kv_buf.shape[1] // local
    n_rows = k_hbm.shape[2]
    group = n_q // n_kv
    per_chunk = qkv_ref.shape[2] // HEAD_DIM
    n_blocks = local // SB

    def held(blk, early):
        return pref.at[blk] if early else kv_slots.at[lax.rem(blk - n_pref, NBUF)]

    def run(blk, early, out, wait):
        seqs = pl.ds(blk * SB, SB)
        for c in (0, 1):
            here = held(blk, early).at[c]
            if out:
                cp = pltpu.make_async_copy(here, (k_out, v_out)[c].at[layer, seqs], out_sem.at[blk, c])
            else:
                cp = pltpu.make_async_copy((k_hbm, v_hbm)[c].at[layer, seqs], here, in_sem.at[blk, c])
            cp.wait() if wait else cp.start()

    for blk in range(n_pref, min(n_pref + NBUF, n_blocks)):
        run(blk, False, False, False)

    def head_of(idx):
        return qkv_ref[idx // per_chunk, :, pl.ds((idx % per_chunk) * HEAD_DIM, HEAD_DIM)].astype(F32)

    for cp in small:
        cp.wait()
    cos_tab, sin_tab = tabs_ref[0], tabs_ref[1]
    gains = [gain_ref[i, pl.ds(layer, 1), :].astype(F32) for i in (0, 1)]

    def norm_rope(vals, gain):
        normed = vals * lax.rsqrt(jnp.mean(vals * vals, axis=-1, keepdims=True) + NORM_EPS) * gain
        return (normed * cos_tab + pltpu.roll(normed, HEAD_DIM // 2, 1) * sin_tab).astype(BF16).astype(F32)
    for h in range(n_kv):
        kv_buf[0, pl.ds(h * local, local), :] = norm_rope(head_of(n_q + h), gains[1])
        kv_buf[1, pl.ds(h * local, local), :] = head_of(n_q + n_kv + h)

    row_ids = lax.broadcasted_iota(jnp.int32, (16, HEAD_DIM), 0)
    lane_ids = lax.broadcasted_iota(jnp.int32, (n_q, n_rows), 1)
    head_hit = lax.rem(lane_ids, n_kv) == lax.div(lax.broadcasted_iota(jnp.int32, (n_q, n_rows), 0), group)
    lane_of = jnp.where(head_hit, lane_ids, n_rows)

    def patch(blk, early):
        ref = held(blk, early)
        for i in range(SB):
            b = blk * SB + i
            row = pos_ref[b] * n_kv
            base = pl.multiple_of(lax.div(row, 16) * 16, 16)
            hit = lax.div(row_ids, n_kv) == lax.div(row - base, n_kv)
            for c in (0, 1):
                new = kv_buf[c, pl.ds(b, n_kv, stride=local), :]
                new = jnp.concatenate([new] * (16 // n_kv), axis=0)
                old = ref[c, i, pl.ds(base, 16), :]
                ref[c, i, pl.ds(base, 16), :] = jnp.where(hit, new, old.astype(F32)).astype(BF16)

    for blk in range(min(AHEAD, n_pref)):
        patch(blk, True)
    for h in range(n_q):
        q_buf[pl.ds(h * local, local), :] = norm_rope(head_of(h), gains[0])
    for blk in range(min(AHEAD, n_pref)):
        run(blk, True, True, False)

    def block_step(blk, early, nxt, nxt_early):
        ref = held(blk, early)
        if nxt is not None:
            if not nxt_early:
                run(nxt, False, False, True)
            patch(nxt, nxt_early)
        for i in range(SB):
            q = q_buf[pl.ds(blk * SB + i, n_q, stride=local), :].astype(BF16)
            s_buf[i] = lax.dot_general(q, ref[0, i], (((1,), (1,)), ((), ())), preferred_element_type=F32)
        if nxt is not None:
            run(nxt, nxt_early, True, False)
        for i in range(SB):
            row = pos_ref[blk * SB + i] * n_kv
            scores = jnp.where(lane_of < row + n_kv, s_buf[i] * (HEAD_DIM ** -0.5), -1e30)
            e = jnp.exp(scores - jnp.max(scores, axis=-1, keepdims=True))
            p_buf[i] = (e / jnp.sum(e, axis=-1, keepdims=True)).astype(BF16)
        for i in range(SB):
            o_buf[pl.ds(blk * SB + i, n_q, stride=local), :] = dot(p_buf[i], ref[1, i])

    def early_step(blk, carry):
        block_step(blk, True, blk + AHEAD, True)
        return carry
    lax.fori_loop(0, n_pref - AHEAD, early_step, 0)
    for blk in range(n_pref - AHEAD, n_blocks):
        nxt = blk + AHEAD if blk + AHEAD < n_blocks else None
        block_step(blk, blk < n_pref, nxt, False)

    for h in range(n_q):
        o_vmem[:, pl.ds(h * HEAD_DIM, HEAD_DIM)] = o_buf[pl.ds(h * local, local), :].astype(BF16)
    o_copy = pltpu.make_async_copy(o_vmem, o_ref, small_sem.at[6])
    o_copy.start()
    o_copy.wait()
    for blk in range(n_pref):
        run(blk, True, True, True)
    for blk in range(max(n_blocks - NBUF, n_pref), n_blocks):
        run(blk, False, True, True)


def attn_call(layer, pos, qkv, cos_tab, sin_tab, q_gain, k_gain, k_cache, v_cache, pref, prev):
    layers, local, n_rows, _ = k_cache.shape
    n_kv = 4
    n_q = 16
    vmem = pl.BlockSpec(memory_space=pltpu.VMEM)
    hbm = pl.BlockSpec(memory_space=pltpu.HBM)
    args = [in_hbm(pos), qkv if layer == 0 else in_hbm(qkv), in_hbm(cos_tab), in_hbm(sin_tab), in_hbm(q_gain), in_hbm(k_gain), in_hbm(k_cache), in_hbm(v_cache), pltpu.with_memory_space_constraint(pref, pltpu.VMEM)]
    in_specs = [hbm] * 8 + [vmem]
    aliases = {8: 3}
    n_pref, n_blocks = pref.shape[0], local // SB
    if prev is not None:
        args += list(prev)
        in_specs += [hbm] * 2
        aliases.update({9: 0, 10: 1})
    return pl.pallas_call(
        functools.partial(attn_kernel, layer, n_pref),
        out_shape=[jax.ShapeDtypeStruct(k_cache.shape, BF16)] * 2 + [pltpu.HBM((local, n_q * HEAD_DIM), BF16), jax.ShapeDtypeStruct(pref.shape, BF16)],
        in_specs=in_specs,
        out_specs=[hbm, hbm, hbm, vmem],
        scratch_shapes=[pltpu.VMEM((min(NBUF, max(n_blocks - n_pref, 1)) if n_pref < n_blocks else 1, 2, SB if n_pref < n_blocks else 1, n_rows, HEAD_DIM), BF16),
                        pltpu.VMEM((n_q * local, HEAD_DIM), F32), pltpu.VMEM((2, n_kv * local, HEAD_DIM), F32), pltpu.VMEM((n_q * local, HEAD_DIM), F32),
                        pltpu.VMEM((SB, n_q, n_rows), F32), pltpu.VMEM((SB, n_q, n_rows), BF16),
                        pltpu.VMEM(qkv.shape, BF16), pltpu.VMEM((2,) + cos_tab.shape, F32), pltpu.SMEM(pos.shape, jnp.int32), pltpu.VMEM((2,) + q_gain.shape, BF16), pltpu.VMEM((local, n_q * HEAD_DIM), BF16),
                        pltpu.SemaphoreType.DMA((n_blocks, 2)), pltpu.SemaphoreType.DMA((n_blocks, 2)), pltpu.SemaphoreType.DMA((7,))],
        input_output_aliases=aliases, name=f'attn_{layer}',
        compiler_params=pltpu.CompilerParams(vmem_limit_bytes=(20 if layer == 0 else 22) * 1024 * 1024),
    )(*args)


def solution(mesh):
    group_size = mesh.shape['x']
    cache_spec = P(None, ('dp', 'x'), None, 'y', None)
    col_spec = P(None, 'x', 'y')
    row_spec = P(None, 'y', 'x')
    in_specs = (P('dp', 'x'), P('dp'), cache_spec, cache_spec, P(None, 'x'), P(None, 'x'), P(), P(), col_spec, col_spec, col_spec, row_spec, col_spec, col_spec, row_spec)
    out_specs = (P('dp', 'x'), cache_spec, cache_spec)

    def device_step(hidden, positions, k_cache, v_cache, g_attn, g_mlp, q_gain, k_gain, w_q, w_k, w_v, w_o, w_gate, w_up, w_down):
        model_dim = hidden.shape[1] * group_size
        layers, local, cache_len, n_kv, _ = k_cache.shape
        my_pos = lax.dynamic_slice_in_dim(positions, lax.axis_index('x') * local, local)
        half = HEAD_DIM // 2
        inv_freq = np.power(ROPE_BASE, -2.0 * np.arange(half) / HEAD_DIM).astype(np.float32)
        angles = my_pos.astype(F32)[:, None] * jnp.asarray(np.concatenate([inv_freq, inv_freq]))[None, :]
        sign = jnp.asarray(np.repeat(np.array([-1.0, 1.0], np.float32), half))
        cos_tab, sin_tab = jnp.cos(angles), jnp.sin(angles) * sign[None, :]
        cos_tab, sin_tab, my_pos, hidden = lax.optimization_barrier((cos_tab, sin_tab, my_pos, hidden))
        k_rows = k_cache.reshape(layers, local, cache_len * n_kv, HEAD_DIM)
        v_rows = v_cache.reshape(layers, local, cache_len * n_kv, HEAD_DIM)
        attn_tabs = (cos_tab, sin_tab, q_gain, k_gain, k_rows, v_rows)
        caches = {'k_rows': k_rows, 'v_rows': v_rows}
        qkv, pref = chain_call(False, True, 0, 0, 8, 16, model_dim, hidden, g_attn=g_attn, wq=w_q, wk=w_k, wv=w_v, **caches)
        k_new, v_new, attn, _ = attn_call(0, my_pos, qkv, *attn_tabs, pref, None)
        hidden, qkv, pref = chain_call(True, True, 0, 1, 5, 40, model_dim, hidden, attn, g_mlp, w_o, w_gate, w_up, w_down, g_attn, w_q, w_k, w_v, **caches)
        k_new, v_new, attn, _ = attn_call(1, my_pos, qkv, *attn_tabs, pref, (k_new, v_new))
        (hidden,) = chain_call(True, False, 1, 2, 0, 46, model_dim, hidden, attn, g_mlp, w_o, w_gate, w_up, w_down)
        return hidden, k_new.reshape(k_cache.shape), v_new.reshape(v_cache.shape)

    return jax.shard_map(device_step, mesh=mesh, in_specs=in_specs, out_specs=out_specs, check_vma=False)
```
